512 devices in a mesh: groups: 2 (over y), pts: 32 (over z), cb: 8 (over x, core).
Axes of the slice: x: 4, y: 2, z: 32, core: 2. Of those that a mesh axis runs over, the one named last changes fastest.
The devices are a block of a 4x8x32 slice.
Arguments:
- points: bfloat16 [131072, 768], P(('groups', 'pts')), parts along dimension 0, may hold values from -60 to 60
- code_one: int32 [131072], P(('groups', 'pts')), parts along dimension 0, may hold values from 0 to 2047
- code_two: int32 [131072], P(('groups', 'pts')), parts along dimension 0, may hold values from 0 to 2047
- cent_one: bfloat16 [4096, 768], P(('groups', 'cb')), parts along dimension 0, may hold values from -6 to 6
- cent_two: bfloat16 [4096, 768], P(('groups', 'cb')), parts along dimension 0, may hold values from -6 to 6
Outputs:
- new_one: bfloat16 [4096, 768], P(('groups', 'cb')), parts along dimension 0
- new_two: bfloat16 [4096, 768], P(('groups', 'cb')), parts along dimension 0
- distortion: float32 [4], P('groups'), parts along dimension 0
The draws below stay inside these ranges and needn't reach their ends.
There are 2 independent parts, one for each index of `groups`. The reference program is written for one: setup_inputs(seed, part) draws one part's arguments, and reference() takes and returns one part's arrays. A program takes and returns all parts, laid end to end along the dimension named above; each array names one. Nothing has to cross between parts.
All inputs are finite; a program needn't handle non-finite values.
Results may differ from the reference program's by a relative error of at most 0.0014.
Values may be sent and summed in bfloat16 or wider, within the bound.
A program may use at most 64 MiB of HBM per device.

```python
import math
import jax
import jax.numpy as jnp
from jax import lax

D = 768
K = 2048
POINTS = 65536


def centre_table(key):
    values = jax.random.normal(jax.random.fold_in(key, 11), (K, D), jnp.float32)
    return jnp.clip(values, -6.0, 6.0).astype(jnp.bfloat16)


def draw_cent_one(key, part):
    return centre_table(key)


def draw_points(key, part):
    centres = centre_table(key).astype(jnp.float32)
    picks = jax.random.randint(jax.random.fold_in(key, 12), (POINTS,), 0, K)
    chosen = jnp.take(centres, picks, axis=0)
    key_jit = jax.random.fold_in(jax.random.fold_in(key, 13), 0)
    key_base = jax.random.fold_in(jax.random.fold_in(key, 13), 1)
    key_cols = jax.random.fold_in(jax.random.fold_in(key, 13), 3)
    rowpos = jnp.arange(POINTS, dtype=jnp.float32) / POINTS
    trend = jnp.power(3.0, rowpos)
    jitter = jnp.exp(jax.random.uniform(key_jit, (POINTS,), jnp.float32, 0.0, math.log(4.0)))
    colscale = jnp.exp(jax.random.uniform(key_cols, (D,), jnp.float32, math.log(0.5), math.log(2.0)))
    base = jax.random.normal(key_base, (POINTS, D), jnp.float32)
    noise = 0.15 * base * (trend * jitter)[:, None] * colscale[None, :]
    return jnp.clip(chosen + noise, -60.0, 60.0).astype(jnp.bfloat16)


def plant(result, own_key, smallest, high):
    shape = result.shape
    place = [jax.random.randint(jax.random.fold_in(own_key, axis), (), 0, shape[axis]) for axis in range(len(shape))]
    result = result.at[tuple(place)].set(smallest)
    longest = shape.index(max(shape))
    place[longest] = (place[longest] + 1) % shape[longest]
    return result.at[tuple(place)].set(high)


def levels(stream_key, shape, cuts, smallest, top_value):
    def one(axis_at, parts):
        steps = jax.random.uniform(jax.random.fold_in(jax.random.fold_in(stream_key, 6), axis_at), (parts,), jnp.float32, smallest / len(cuts), top_value / len(cuts))
        return jnp.repeat(jnp.exp(steps), shape[axis_at] // parts).reshape((-1,) + (1,) * (len(shape) - axis_at - 1))

    level = one(*cuts[0])
    for cut in cuts[1:]:
        level = level * one(*cut)
    return level


def normal_values(key, dims, scale, limit, cuts=(), kind=jnp.bfloat16):
    level = levels(key, dims, cuts, -0.22, 0.18) if cuts else 1.0
    result = jax.random.normal(key, dims, jnp.float32) * scale * level
    return jnp.minimum(jnp.maximum(result, -limit), limit).astype(kind)


def setup_inputs(seed: int = 0, part: int = 0) -> dict:
    keys = jax.random.split(jax.random.key(seed), 6)
    part_keys = jax.random.split(jax.random.fold_in(keys[5], part), 6)
    return {
        "points": draw_points(jax.random.fold_in(jax.random.fold_in(keys[5], part), 71), part),
        "code_one": plant(jax.random.randint(part_keys[1], (POINTS,), 0, K), jax.random.fold_in(part_keys[1], 1), 0, K - 1).astype(jnp.int32),
        "code_two": plant(jax.random.randint(part_keys[2], (POINTS,), 0, K), jax.random.fold_in(part_keys[2], 1), 0, K - 1).astype(jnp.int32),
        "cent_one": draw_cent_one(jax.random.fold_in(jax.random.fold_in(keys[5], part), 71), part),
        "cent_two": normal_values(part_keys[4], (K, D), 1.0, 6.0, ((0, 8),)),
    }


def nearest_total(data, cents):
    csq = jnp.sum(jnp.square(cents.astype(jnp.float32)), axis=1)
    block = math.gcd(POINTS, 4096)
    blocks = data.reshape(POINTS // block, block, D)

    def one_block(rows_in):
        sq = jnp.sum(jnp.square(rows_in.astype(jnp.float32)), axis=1)
        cross = lax.dot_general(rows_in, cents, (((1,), (1,)), ((), ())), preferred_element_type=jnp.float32)
        dist = sq[:, None] - 2.0 * cross + csq[None, :]
        return jnp.min(dist, axis=1)

    mins = lax.map(one_block, blocks)
    return jnp.sum(mins)


def update(data, codes, cents):
    sums = jax.ops.segment_sum(data.astype(jnp.float32), codes, num_segments=K)
    counts = jax.ops.segment_sum(jnp.ones((POINTS,), jnp.float32), codes, num_segments=K)
    return ((sums + cents.astype(jnp.float32)) / (counts + 1.0)[:, None]).astype(jnp.bfloat16)


def reference(points, code_one, code_two, cent_one, cent_two):
    new_one = update(points, code_one, cent_one)
    looked = jnp.take(new_one, code_one, axis=0)
    residual = (points.astype(jnp.float32) - looked.astype(jnp.float32)).astype(jnp.bfloat16)
    new_two = update(residual, code_two, cent_two)
    first = nearest_total(points, cent_one)
    second = nearest_total(residual, cent_two)
    distortion = jnp.stack([first, second]) / jnp.float32(POINTS * D)
    return new_one, new_two, distortion
```

```python
import functools

import jax
import jax.numpy as jnp
from jax import lax
from jax.experimental import pallas as pl
from jax.experimental.pallas import tpu as pltpu
from jax.sharding import PartitionSpec as P

MESH = pl.DeviceIdType.MESH
F32 = jnp.float32
BF16 = jnp.bfloat16
LANES = 128
HALF = 64
WIN = 4
NEAR = (-2, -1, 1)


def far_first(n):
    order = [n // 2]
    for k in range(n // 2 - 1, 0, -1):
        order += [k, n - k]
    return order


def iota(shape, dim):
    return lax.broadcasted_iota(jnp.int32, shape, dim)


def kernel(nz, nx, pts, code1, code2, cent1, cent2, new1, new2, dist, v, sem):
    z = lax.axis_index("pts")
    cb = lax.axis_index("cb")
    x = cb // 2
    c = cb - 2 * x
    h = x - 2 * (x // 2)
    q = z // WIN
    cl = z - WIN * q
    par = cl - 2 * (cl // 2)
    e = cl // 2
    nq = nz // WIN
    s = 1 - 2 * c
    rows = cent1.shape[0]
    npts = pts.shape[0]
    own = npts // (2 * nx)
    g = 2 * rows // nz
    ch = 3 * g
    FAR = far_first(nq)

    def zed(step):
        return lax.rem(z + step + nz, nz)

    def to_z(t):
        return {"pts": t}

    def to_x(t):
        return {"cb": 2 * t + c}

    sib = {"cb": 2 * x + 1 - c}

    def send(src, dst, ss, rs, where):
        pltpu.make_async_remote_copy(
            src_ref=src, dst_ref=dst, send_sem=ss, recv_sem=rs, device_id=where, device_id_type=MESH
        ).start()

    def wait(ref, sm):
        pltpu.make_async_copy(ref, ref, sm).wait()

    def xed(i):
        return lax.rem(x + i, nx)

    barrier = pltpu.get_barrier_semaphore()
    for step in (-2, -1, 1, 2):
        pl.semaphore_signal(barrier, inc=1, device_id=to_z(zed(step)), device_id_type=MESH)
    for o in range(1, nq):
        pl.semaphore_signal(barrier, inc=1, device_id=to_z(zed(WIN * o)), device_id_type=MESH)
    for i in range(1, nx):
        pl.semaphore_signal(barrier, inc=1, device_id=to_x(xed(i)), device_id_type=MESH)
    pl.semaphore_signal(barrier, inc=1, device_id=sib, device_id_type=MESH)

    tile_a = x + (x + 1) // 2
    tile_b = 1 + 3 * (x // 2)
    col_a = pl.ds(pl.multiple_of(tile_a * LANES, LANES), LANES)
    col_b = pl.ds(pl.multiple_of(tile_b * LANES, LANES), LANES)
    loads = [
        pltpu.make_async_copy(pts.at[:, col_a], v["P"].at[:, 0:LANES], sem["ld"].at[0]),
        pltpu.make_async_copy(pts.at[:, col_b], v["P"].at[:, LANES : 2 * LANES], sem["ld"].at[1]),
        pltpu.make_async_copy(cent1, v["C1"].at[cb], sem["ld"].at[2]),
        pltpu.make_async_copy(cent2, v["C2"].at[cb], sem["ld"].at[3]),
        pltpu.make_async_copy(pts.at[pl.ds(pl.multiple_of(cb * own, own), own), :], v["R1"], sem["ld"].at[4]),
    ]
    for ld in loads:
        ld.start()
    loads[0].wait()
    loads[1].wait()

    blk = 256
    hm_b = iota((blk, LANES), 1) // HALF == h
    hm_g = iota((g, LANES), 1) // HALF == h

    @pl.loop(0, npts // blk)
    def _(i):
        sl = pl.ds(pl.multiple_of(i * blk, blk), blk)
        v["W"][sl, 0:LANES] = v["P"][sl, 0:LANES]
        b = v["P"][sl, LANES : 2 * LANES].astype(F32)
        v["W"][sl, LANES : 2 * LANES] = jnp.where(hm_b, b, 1.0).astype(BF16)

    m16 = (iota((nq, g, LANES), 2) & (g - 1)) == iota((nq, g, LANES), 1)

    def class_of(i):
        t = zed(s * (i - 2 + (i // 2) * (5 - 2 * i)))
        return t, t // WIN, lax.rem(t, WIN)

    def class_sums(i, code, w, S, Sc):
        _, _, ct = class_of(i)
        pt = lax.rem(ct, 2)
        et = ct // 2
        n = 2 * nq * g
        r = iota((n, 1), 0)
        hl = r // (nq * g)
        rq = (r // g) & (nq - 1)
        lab = rows * (2 * (2 * pt + hl) + c) + g * (2 * rq + et) + (r & (g - 1))
        oh = jnp.where(lab == code[...], 1.0, 0.0).astype(BF16)
        out = jnp.dot(oh, w[...], preferred_element_type=F32)
        lo, hi = out[: nq * g], out[nq * g :]
        S[ct, :, 0:g, :] = lo[:, :LANES].reshape(nq, g, LANES)
        S[ct, :, g : 2 * g, :] = hi[:, :LANES].reshape(nq, g, LANES)
        lb = lo[:, LANES:]
        hb = pltpu.roll(hi[:, LANES:], HALF, 1)
        hm = iota(lb.shape, 1) // HALF == h
        S[ct, :, 2 * g :, :] = jnp.where(hm, lb, hb).reshape(nq, g, LANES)
        cnt = jnp.where(hm, hb, lb).reshape(nq, g, LANES)
        Sc[ct] = jnp.sum(jnp.where(m16, cnt, 0.0), axis=1, keepdims=True)

    def class_sends(i, S, Sc, X1, X1c, k):
        t, qt, ct = class_of(i)
        for o in FAR + [0]:
            qd = lax.rem(qt + o, nq)
            send(S.at[ct, qd], X1.at[i, qd], sem["s1"].at[k], sem["r1"].at[k, qd], to_z(t))
        send(Sc.at[ct], X1c.at[i], sem["s1c"].at[k], sem["r1c"].at[k], to_z(t))

    def far_sums(S, Sc, X1, X1c, T, Tc, X2, X2c, k):
        wait(X1c, sem["r1c"].at[k])
        Tc[...] = Sc[cl] + X1c[0] + X1c[1] + X1c[2]
        for o in FAR:
            qd = lax.rem(q + o, nq)
            t = zed(WIN * o)
            wait(X1.at[:, 0], sem["r1"].at[k, qd])
            T[qd] = S[cl, qd] + X1[0, qd] + X1[1, qd] + X1[2, qd]
            send(T.at[qd], X2.at[o - 1], sem["s2"].at[k], sem["r2"].at[k], to_z(t))
            send(Tc.at[qd], X2c.at[o - 1], sem["s2c"].at[k], sem["r2c"].at[k], to_z(t))
        wait(X1.at[:, 0], sem["r1"].at[k, q])
        T[q] = S[cl, q] + X1[0, q] + X1[1, q] + X1[2, q]

    def finish(T, Tc, X2, X2c, C, N, k):
        wait(X2c, sem["r2c"].at[k])
        cnt = Tc[q]
        for o in range(nq - 1):
            cnt = cnt + X2c[o]
        wait(X2, sem["r2"].at[k])
        tot = T[q]
        for o in range(nq - 1):
            tot = tot + X2[o]
        full = jnp.broadcast_to(cnt, (g, LANES))
        diag = (iota((g, LANES), 1) & (HALF - 1)) == iota((g, LANES), 0)
        lo_n = jnp.sum(jnp.where(diag & jnp.logical_not(hm_g), full, 0.0), axis=1, keepdims=True) + 1.0
        hi_n = jnp.sum(jnp.where(diag & hm_g, full, 0.0), axis=1, keepdims=True) + 1.0
        sl = pl.ds(pl.multiple_of(g * (z // 2), g), g)
        at_lo = 2 * (2 * par) + c
        at_hi = 2 * (2 * par + 1) + c
        a_lo = C[at_lo, sl, col_a].astype(F32)
        a_hi = C[at_hi, sl, col_a].astype(F32)
        b_lo = C[at_lo, sl, col_b].astype(F32)
        b_hi = pltpu.roll(C[at_hi, sl, col_b].astype(F32), HALF, 1)
        ci = 2 * par + e
        N[c, ci, q, 0:g, :] = ((tot[0:g] + a_lo) / lo_n).astype(BF16)
        N[c, ci, q, g : 2 * g, :] = ((tot[g : 2 * g] + a_hi) / hi_n).astype(BF16)
        N[c, ci, q, 2 * g :, :] = (
            (tot[2 * g :] + jnp.where(hm_g, b_lo, b_hi)) / jnp.where(hm_g, lo_n, hi_n)
        ).astype(BF16)

    def cidx(t):
        ct = lax.rem(t, WIN)
        return 2 * lax.rem(ct, 2) + ct // 2

    def gather(N, k, twin):
        ci = 2 * par + e

        def near_sends(qs):
            for i in range(3):
                send(N.at[c, ci, qs], N.at[c, ci, qs], sem["sl"].at[k], sem["rl"].at[k, i], to_z(zed(s * NEAR[i])))

        for o in FAR:
            send(N.at[c, ci, q], N.at[c, ci, q], sem["sf"].at[k], sem["rf"].at[k, o - 1], to_z(zed(WIN * o)))
        near_sends(q)
        for o in FAR[::-1]:
            qs = lax.rem(q - o + nq, nq)
            wait(N.at[c, ci, qs], sem["rf"].at[k, o - 1])
            near_sends(qs)
        if twin:
            send(N.at[c, ci], N.at[c, ci], sem["st"].at[0], sem["rt"].at[0], sib)
        for i in (2, 1, 0):
            cs = cidx(zed(-s * NEAR[i]))
            wait(N.at[c, cs], sem["rl"].at[k, i])
            if twin:
                send(N.at[c, cs], N.at[c, cs], sem["st"].at[0], sem["rt"].at[0], sib)

    def out_parts(N, t):
        pair = pl.ds(2 * (t // 2), 2)
        rs = pl.ds(pl.multiple_of(g * lax.rem(t, 2), g), g)
        return N.at[c, pair, :, rs, :], N.at[c, pair, :, pl.ds(2 * g, g), :]

    def out_sends(N, OA, OB, k):
        for i in range(1, nx):
            t = xed(i)
            a, b = out_parts(N, t)
            send(a, OA.at[x], sem["so"].at[k, 0], sem["ro"].at[k, 0], to_x(t))
            send(b, OB.at[x], sem["so"].at[k, 1], sem["ro"].at[k, 1], to_x(t))
        a, b = out_parts(N, x)
        pltpu.make_async_copy(a, OA.at[x], sem["lo"].at[k, 0]).start()
        pltpu.make_async_copy(b, OB.at[x], sem["lo"].at[k, 1]).start()

    left = iota((g, LANES), 1) < HALF

    def out_rows(OA, OB, out, k):
        wait(OA.at[0], sem["lo"].at[k, 0])
        wait(OB.at[0], sem["lo"].at[k, 1])
        wait(OA.at[pl.ds(0, nx - 1)], sem["ro"].at[k, 0])
        wait(OB.at[pl.ds(0, nx - 1)], sem["ro"].at[k, 1])
        for ee in range(2):
            for qq in range(nq):
                r0 = g * (2 * qq + ee)
                for xx in range(nx):
                    ta = xx + (xx + 1) // 2
                    out[r0 : r0 + g, ta * LANES : (ta + 1) * LANES] = OA[xx, ee, qq]
                for y in range(nx // 2):
                    two = []
                    for xx in (2 * y, 2 * y + 1):
                        b = OB[xx, ee, qq].astype(F32)
                        two.append(jnp.where(h == 1, pltpu.roll(b, HALF, 1), b))
                    tb = 1 + 3 * y
                    out[r0 : r0 + g, tb * LANES : (tb + 1) * LANES] = jnp.where(left, two[0], two[1]).astype(BF16)

    def nearest(C, R):
        def body(k, m):
            ck = C[k]
            cross = lax.dot_general(ck, R[...], (((1,), (1,)), ((), ())), preferred_element_type=F32)
            cf = ck.astype(F32)
            csq = jnp.sum(cf * cf, axis=1, keepdims=True)
            d = csq - 2.0 * cross
            return jnp.minimum(m, jnp.min(d.reshape(rows // 8, 8, own), axis=0))

        m = lax.fori_loop(0, 2 * nx, body, jnp.full((8, own), jnp.inf, F32))
        mins = jnp.min(m, axis=0, keepdims=True)
        r = R[...].astype(F32)
        psq = jnp.sum(jnp.sum(r * r, axis=0, keepdims=True), axis=1, keepdims=True)
        return jnp.sum(mins, axis=1, keepdims=True) + psq

    @pl.loop(0, WIN)
    def _(i):
        class_sums(i, code1, v["W"], v["S1"], v["Sc1"])

    loads[2].wait()
    loads[3].wait()
    loads[4].wait()
    pl.semaphore_wait(barrier, 4 + (nq - 1) + (nx - 1) + 1)

    for i in range(3):
        class_sends(i, v["S1"], v["Sc1"], v["X11"], v["X1c1"], 0)
    for k, C in enumerate((v["C1"], v["C2"])):
        for i in range(1, nx):
            send(C.at[cb], C.at[cb], sem["sc"].at[k], sem["rc"].at[k], to_x(xed(i)))
        send(C.at[cb], C.at[cb], sem["sct"].at[k], sem["rct"].at[k], sib)

    for b in range(npts // LANES):
        row = code1[0:1, b * LANES : (b + 1) * LANES].astype(F32)
        v["CT"][b * LANES : (b + 1) * LANES, :] = jnp.transpose(jnp.broadcast_to(row, (LANES, LANES)))

    def twin_cents(C, k):
        wait(C.at[pl.ds(0, nx - 1)], sem["rc"].at[k])
        for i in range(1, nx):
            at = 2 * xed(i) + c
            send(C.at[at], C.at[at], sem["sct"].at[k], sem["rct"].at[k], sib)

    far_sums(v["S1"], v["Sc1"], v["X11"], v["X1c1"], v["T1"], v["Tc1"], v["X21"], v["X2c1"], 0)
    twin_cents(v["C1"], 0)
    finish(v["T1"], v["Tc1"], v["X21"], v["X2c1"], v["C1"], v["N1"], 0)
    gather(v["N1"], 0, True)
    out_sends(v["N1"], v["OA1"], v["OB1"], 0)
    wait(v["N1"].at[0], sem["rt"].at[0])

    kb = nq * g
    for cc in range(2):
        for k in range(WIN):
            base = (cc * WIN + k) * 2 * kb
            n = v["N1"][cc, k]
            v["L"][base : base + kb, 0:LANES] = n[:, 0:g, :].reshape(kb, LANES)
            v["L"][base + kb : base + 2 * kb, 0:LANES] = n[:, g : 2 * g, :].reshape(kb, LANES)
            b = n[:, 2 * g :, :].reshape(kb, LANES)
            v["L"][base : base + kb, LANES : 2 * LANES] = b
            v["L"][base + kb : base + 2 * kb, LANES : 2 * LANES] = pltpu.roll(b.astype(F32), HALF, 1).astype(BF16)

    @pl.loop(0, npts // blk)
    def _(i):
        sl = pl.ds(pl.multiple_of(i * blk, blk), blk)
        codes = v["CT"][sl, :]
        parts = []
        lane = iota((1, LANES), 1)
        for j in range(2 * nx * rows // LANES):
            r = lane + j * LANES
            cc = r // (WIN * 2 * kb)
            k = (r // (2 * kb)) & (WIN - 1)
            hl = (r // kb) & 1
            rq = (r // g) & (nq - 1)
            lab = rows * (2 * (2 * (k // 2) + hl) + cc) + g * (2 * rq + (k & 1)) + (r & (g - 1))
            parts.append(jnp.where(codes == lab.astype(F32), 1.0, 0.0).astype(BF16))
        oh = jnp.concatenate(parts, axis=1)
        looked = jnp.dot(oh, v["L"][...], preferred_element_type=F32)
        res = v["P"][sl, :].astype(F32) - looked
        v["W2"][sl, 0:LANES] = res[:, 0:LANES].astype(BF16)
        v["W2"][sl, LANES : 2 * LANES] = jnp.where(hm_b, res[:, LANES:], 1.0).astype(BF16)

    @pl.loop(0, WIN)
    def _(i):
        class_sums(i, code2, v["W2"], v["S2"], v["Sc2"])

        @pl.when(i < 3)
        def _():
            class_sends(i, v["S2"], v["Sc2"], v["X12"], v["X1c2"], 1)

    for i in range(1, nx):
        t = xed(i)
        sl = pl.ds(pl.multiple_of(own * (2 * t + c), own), own)
        send(v["W2"].at[sl, :], v["RR"].at[x], sem["srr"], sem["rrr"], to_x(t))
    sl = pl.ds(pl.multiple_of(own * cb, own), own)
    mine = pltpu.make_async_copy(v["W2"].at[sl, :], v["RR"].at[x], sem["ld"].at[5])
    mine.start()
    far_sums(v["S2"], v["Sc2"], v["X12"], v["X1c2"], v["T2"], v["Tc2"], v["X22"], v["X2c2"], 1)
    twin_cents(v["C2"], 1)
    out_rows(v["OA1"], v["OB1"], new1, 0)

    wait(v["C1"].at[pl.ds(0, nx)], sem["rct"].at[0])
    near_one = nearest(v["C1"], v["R1"])
    mine.wait()
    wait(v["RR"].at[pl.ds(0, nx - 1)], sem["rrr"])
    for xx in range(nx):
        ta = xx + (xx + 1) // 2
        v["R2"][:, ta * LANES : (ta + 1) * LANES] = v["RR"][xx, :, 0:LANES]
    left_own = iota((own, LANES), 1) < HALF
    for y in range(nx // 2):
        tb = 1 + 3 * y
        v["R2"][:, tb * LANES : (tb + 1) * LANES] = jnp.where(
            left_own,
            v["RR"][2 * y, :, LANES:].astype(F32),
            v["RR"][2 * y + 1, :, LANES:].astype(F32),
        ).astype(BF16)
    wait(v["C2"].at[pl.ds(0, nx)], sem["rct"].at[1])
    near_two = nearest(v["C2"], v["R2"])
    lane = iota((1, LANES), 1)
    v["D0"][c] = jnp.where(lane == 0, near_one, jnp.where(lane == 1, near_two, 0.0))
    send(v["D0"].at[c], v["D0"].at[c], sem["sd"].at[0], sem["rd"].at[0], sib)

    finish(v["T2"], v["Tc2"], v["X22"], v["X2c2"], v["C2"], v["N2"], 1)

    wait(v["D0"].at[0], sem["rd"].at[0])
    v["D1"][x] = v["D0"][0] + v["D0"][1]
    for i in range(1, nx):
        send(v["D1"].at[x], v["D1"].at[x], sem["sd"].at[1], sem["rd"].at[1], to_x(xed(i)))

    gather(v["N2"], 1, False)
    out_sends(v["N2"], v["OA2"], v["OB2"], 1)

    wait(v["D1"].at[pl.ds(0, nx - 1)], sem["rd"].at[1])
    tot = v["D1"][0]
    for i in range(1, nx):
        tot = tot + v["D1"][i]
    v["D2"][cl, q] = tot
    for o in FAR:
        send(v["D2"].at[cl, q], v["D2"].at[cl, q], sem["sd"].at[2], sem["rd"].at[2], to_z(zed(WIN * o)))

    out_rows(v["OA2"], v["OB2"], new2, 1)

    wait(v["D2"].at[0, pl.ds(0, nq - 1)], sem["rd"].at[2])
    for i in range(3):
        send(v["D2"].at[cl], v["D2"].at[cl], sem["sd"].at[3], sem["rd"].at[3], to_z(zed(s * NEAR[i])))
    wait(v["D2"].at[pl.ds(0, 3)], sem["rd"].at[3])
    tot = v["D2"][0, 0]
    for i in range(1, nz):
        tot = tot + v["D2"][i // nq, i % nq]
    dist[...] = tot / jnp.float32(npts * nz * pts.shape[1])

    for k in range(2):
        wait(v["X11"], sem["s1"].at[k])
        wait(v["X1c1"], sem["s1c"].at[k])
        wait(v["X21"], sem["s2"].at[k])
        wait(v["X2c1"], sem["s2c"].at[k])
        wait(v["N1"].at[0, 0, pl.ds(0, nq - 1)], sem["sf"].at[k])
        wait(v["N1"].at[0, pl.ds(0, 3)], sem["sl"].at[k])
        wait(v["OA1"].at[pl.ds(0, nx - 1)], sem["so"].at[k, 0])
        wait(v["OB1"].at[pl.ds(0, nx - 1)], sem["so"].at[k, 1])
        wait(v["C1"].at[pl.ds(0, nx - 1)], sem["sc"].at[k])
        wait(v["C1"].at[pl.ds(0, nx)], sem["sct"].at[k])
    wait(v["N1"].at[0], sem["st"].at[0])
    wait(v["RR"].at[pl.ds(0, nx - 1)], sem["srr"])
    wait(v["D0"].at[0], sem["sd"].at[0])
    wait(v["D1"].at[pl.ds(0, nx - 1)], sem["sd"].at[1])
    wait(v["D2"].at[0, pl.ds(0, nq - 1)], sem["sd"].at[2])
    wait(v["D2"].at[pl.ds(0, 3)], sem["sd"].at[3])


def solution(mesh):
    nz = mesh.shape["pts"]
    nx = mesh.shape["cb"] // 2
    nq = nz // WIN

    def local(points, code_one, code_two, cent_one, cent_two):
        npts, width = points.shape
        rows = cent_one.shape[0]
        own = npts // (2 * nx)
        g = 2 * rows // nz
        ch = 3 * g
        vm = pltpu.VMEM
        v = {
            "P": vm((npts, 2 * LANES), BF16),
            "W": vm((npts, 2 * LANES), BF16),
            "W2": vm((npts, 2 * LANES), BF16),
            "CT": vm((npts, LANES), F32),
            "L": vm((2 * nx * rows, 2 * LANES), BF16),
            "R1": vm((own, width), BF16),
            "R2": vm((own, width), BF16),
            "RR": vm((nx, own, 2 * LANES), BF16),
            "D0": vm((2, 1, LANES), F32),
            "D1": vm((nx, 1, LANES), F32),
            "D2": vm((WIN, nq, 1, LANES), F32),
        }
        for k in ("1", "2"):
            v["C" + k] = vm((2 * nx, rows, width), BF16)
            v["S" + k] = vm((WIN, nq, ch, LANES), F32)
            v["Sc" + k] = vm((WIN, nq, 1, LANES), F32)
            v["X1" + k] = vm((3, nq, ch, LANES), F32)
            v["X1c" + k] = vm((3, nq, 1, LANES), F32)
            v["T" + k] = vm((nq, ch, LANES), F32)
            v["Tc" + k] = vm((nq, 1, LANES), F32)
            v["X2" + k] = vm((nq - 1, ch, LANES), F32)
            v["X2c" + k] = vm((nq - 1, 1, LANES), F32)
            v["N" + k] = vm((2, WIN, nq, ch, LANES), BF16)
            v["OA" + k] = vm((nx, 2, nq, g, LANES), BF16)
            v["OB" + k] = vm((nx, 2, nq, g, LANES), BF16)
        dma = pltpu.SemaphoreType.DMA
        sem = {
            "ld": dma((6,)),
            "s1": dma((2,)), "r1": dma((2, nq)), "s1c": dma((2,)), "r1c": dma((2,)),
            "s2": dma((2,)), "r2": dma((2,)), "s2c": dma((2,)), "r2c": dma((2,)),
            "sf": dma((2,)), "rf": dma((2, nq - 1)), "sl": dma((2,)), "rl": dma((2, 3)),
            "st": dma((1,)), "rt": dma((1,)),
            "so": dma((2, 2)), "ro": dma((2, 2)), "lo": dma((2, 2)),
            "sc": dma((2,)), "rc": dma((2,)), "sct": dma((2,)), "rct": dma((2,)),
            "srr": dma(()), "rrr": dma(()),
            "sd": dma((4,)), "rd": dma((4,)),
        }
        hbm = pl.BlockSpec(memory_space=pl.ANY)
        vmem = pl.BlockSpec(memory_space=pltpu.VMEM)
        new_one, new_two, dist = pl.pallas_call(
            functools.partial(kernel, nz, nx),
            out_shape=(
                jax.ShapeDtypeStruct((rows, width), BF16),
                jax.ShapeDtypeStruct((rows, width), BF16),
                jax.ShapeDtypeStruct((1, LANES), F32),
            ),
            in_specs=[hbm, vmem, vmem, hbm, hbm],
            out_specs=(vmem, vmem, vmem),
            scratch_shapes=[v, sem],
            compiler_params=pltpu.CompilerParams(
                collective_id=0, has_side_effects=True, vmem_limit_bytes=60 * 1024 * 1024
            ),
        )(points, code_one.reshape(1, npts), code_two.reshape(1, npts), cent_one, cent_two)
        return new_one, new_two, dist[0, :2]

    cents = P(("groups", "cb"), None)
    return jax.shard_map(
        local,
        mesh=mesh,
        in_specs=(P(("groups", "pts"), None), P(("groups", "pts")), P(("groups", "pts")), cents, cents),
        out_specs=(cents, cents, P("groups")),
        check_vma=False,
    )
```

```python
import functools

import jax
import jax.numpy as jnp
from jax import lax
from jax.experimental import pallas as pl
from jax.experimental.pallas import tpu as pltpu
from jax.sharding import PartitionSpec as P

MESH = pl.DeviceIdType.MESH
F32 = jnp.float32
BF16 = jnp.bfloat16
LANES = 128
HALF = 64
WIN = 4
NEAR = (-2, -1, 1)


TREE = (4, 3, -3, 1, -1, 2, -2)


def iota(shape, dim):
    return lax.broadcasted_iota(jnp.int32, shape, dim)


def kernel(nz, nx, pts, code1, code2, cent1, cent2, new1, new2, dist, v, sem):
    z = lax.axis_index("pts")
    cb = lax.axis_index("cb")
    x = cb // 2
    c = cb - 2 * x
    h = x - 2 * (x // 2)
    q = z // WIN
    cl = z - WIN * q
    par = cl - 2 * (cl // 2)
    e = cl // 2
    nq = nz // WIN
    s = 1 - 2 * c
    rows = cent1.shape[0]
    npts = pts.shape[0]
    own = npts // (2 * nx)
    g = 2 * rows // nz
    ch = 3 * g

    def qm(d):
        return lax.rem(q + d * s + 2 * nq, nq)

    def zq(d):
        return lax.rem(z + WIN * d * s + 2 * nz, nz)

    def zed(step):
        return lax.rem(z + step + nz, nz)

    def to_z(t):
        return {"pts": t}

    def to_x(t):
        return {"cb": 2 * t + c}

    sib = {"cb": 2 * x + 1 - c}

    def send(src, dst, ss, rs, where):
        pltpu.make_async_remote_copy(
            src_ref=src, dst_ref=dst, send_sem=ss, recv_sem=rs, device_id=where, device_id_type=MESH
        ).start()

    def wait(ref, sm):
        pltpu.make_async_copy(ref, ref, sm).wait()

    def xed(i):
        return lax.rem(x + i, nx)

    barrier = pltpu.get_barrier_semaphore()
    for step in (-2, -1, 1, 2):
        pl.semaphore_signal(barrier, inc=1, device_id=to_z(zed(step)), device_id_type=MESH)
    for o in range(1, nq):
        pl.semaphore_signal(barrier, inc=1, device_id=to_z(zed(WIN * o)), device_id_type=MESH)
    for i in range(1, nx):
        pl.semaphore_signal(barrier, inc=1, device_id=to_x(xed(i)), device_id_type=MESH)
    pl.semaphore_signal(barrier, inc=1, device_id=sib, device_id_type=MESH)

    tile_a = x + (x + 1) // 2
    tile_b = 1 + 3 * (x // 2)
    col_a = pl.ds(pl.multiple_of(tile_a * LANES, LANES), LANES)
    col_b = pl.ds(pl.multiple_of(tile_b * LANES, LANES), LANES)
    loads = [
        pltpu.make_async_copy(pts.at[:, col_a], v["P"].at[:, 0:LANES], sem["ld"].at[0]),
        pltpu.make_async_copy(pts.at[:, col_b], v["P"].at[:, LANES : 2 * LANES], sem["ld"].at[1]),
        pltpu.make_async_copy(cent1, v["C1"].at[cb], sem["ld"].at[2]),
        pltpu.make_async_copy(cent2, v["C2"].at[cb], sem["ld"].at[3]),
        pltpu.make_async_copy(pts.at[pl.ds(pl.multiple_of(cb * own, own), own), :], v["R1"], sem["ld"].at[4]),
    ]
    for ld in loads:
        ld.start()
    loads[0].wait()
    loads[1].wait()

    blk = 256
    hm_b = iota((blk, LANES), 1) // HALF == h
    hm_g = iota((g, LANES), 1) // HALF == h

    @pl.loop(0, npts // blk)
    def _(i):
        sl = pl.ds(pl.multiple_of(i * blk, blk), blk)
        v["W"][sl, 0:LANES] = v["P"][sl, 0:LANES]
        b = v["P"][sl, LANES : 2 * LANES].astype(F32)
        v["W"][sl, LANES : 2 * LANES] = jnp.where(hm_b, b, 1.0).astype(BF16)

    m16 = (iota((nq, g, LANES), 2) & (g - 1)) == iota((nq, g, LANES), 1)

    def class_of(i):
        t = zed(s * (i - 2 + (i // 2) * (5 - 2 * i)))
        return t, t // WIN, lax.rem(t, WIN)

    def class_sums(i, code, w, S, Sc):
        _, _, ct = class_of(i)
        pt = lax.rem(ct, 2)
        et = ct // 2
        n = 2 * nq * g
        r = iota((n, 1), 0)
        hl = r // (nq * g)
        rq = (r // g) & (nq - 1)
        lab = rows * (2 * (2 * pt + hl) + c) + g * (2 * rq + et) + (r & (g - 1))
        oh = jnp.where(lab == code[...], 1.0, 0.0).astype(BF16)
        out = jnp.dot(oh, w[...], preferred_element_type=F32)
        lo, hi = out[: nq * g], out[nq * g :]
        S[ct, :, 0:g, :] = lo[:, :LANES].reshape(nq, g, LANES)
        S[ct, :, g : 2 * g, :] = hi[:, :LANES].reshape(nq, g, LANES)
        lb = lo[:, LANES:]
        hb = pltpu.roll(hi[:, LANES:], HALF, 1)
        hm = iota(lb.shape, 1) // HALF == h
        S[ct, :, 2 * g :, :] = jnp.where(hm, lb, hb).reshape(nq, g, LANES)
        cnt = jnp.where(hm, hb, lb).reshape(nq, g, LANES)
        Sc[ct] = jnp.sum(jnp.where(m16, cnt, 0.0), axis=1, keepdims=True)

    def class_sends(i, S, Sc, X1, X1c, k):
        t, qt, ct = class_of(i)
        send(Sc.at[ct], X1c.at[i], sem["s1c"].at[k], sem["r1c"].at[k], to_z(t))
        for d in TREE + (0,):
            qd = lax.rem(qt + d * s + 2 * nq, nq)
            send(S.at[ct, qd], X1.at[i, qd], sem["s1"].at[k], sem["r1"].at[k, qd], to_z(t))

    def far_sums(S, Sc, X1, X1c, T, Tc, XM, X2, X2c, k):
        for d in TREE + (0,):
            qd = qm(d)
            wait(X1.at[:, 0], sem["r1"].at[k, qd])
            t = S[cl, qd] + X1[0, qd] + X1[1, qd] + X1[2, qd]
            if d == 2:
                wait(XM.at[0], sem["rm"].at[k, 0])
                wait(XM.at[1], sem["rm"].at[k, 1])
                t = t + XM[0] + XM[1]
            if d == -2:
                wait(XM.at[2], sem["rm"].at[k, 2])
                t = t + XM[2]
            T[qd] = t
            if d == 4:
                send(T.at[qd], XM.at[0], sem["s2"].at[k], sem["rm"].at[k, 0], to_z(zq(2)))
                wait(X1c, sem["r1c"].at[k])
                Tc[...] = Sc[cl] + X1c[0] + X1c[1] + X1c[2]
                for o in range(1, nq):
                    qo = lax.rem(q + o, nq)
                    send(Tc.at[qo], X2c.at[o - 1], sem["s2c"].at[k], sem["r2c"].at[k], to_z(zed(WIN * o)))
            elif d == 3:
                send(T.at[qd], XM.at[1], sem["s2"].at[k], sem["rm"].at[k, 1], to_z(zq(1)))
            elif d == -3:
                send(T.at[qd], XM.at[2], sem["s2"].at[k], sem["rm"].at[k, 2], to_z(zq(-1)))
            elif d != 0:
                at = (1, -1, 2, -2).index(d)
                send(T.at[qd], X2.at[at], sem["s2"].at[k], sem["r2"].at[k], to_z(zq(d)))

    def finish(T, Tc, X2, X2c, C, k):
        wait(X2c, sem["r2c"].at[k])
        cnt = Tc[q]
        for o in range(nq - 1):
            cnt = cnt + X2c[o]
        wait(X2, sem["r2"].at[k])
        tot = T[q] + X2[0] + X2[1] + X2[2] + X2[3]
        full = jnp.broadcast_to(cnt, (g, LANES))
        diag = (iota((g, LANES), 1) & (HALF - 1)) == iota((g, LANES), 0)
        lo_n = jnp.sum(jnp.where(diag & jnp.logical_not(hm_g), full, 0.0), axis=1, keepdims=True) + 1.0
        hi_n = jnp.sum(jnp.where(diag & hm_g, full, 0.0), axis=1, keepdims=True) + 1.0
        sl = pl.ds(pl.multiple_of(g * (z // 2), g), g)
        at_lo = 2 * (2 * par) + c
        at_hi = 2 * (2 * par + 1) + c
        a_lo = C[at_lo, sl, col_a].astype(F32)
        a_hi = C[at_hi, sl, col_a].astype(F32)
        b_lo = C[at_lo, sl, col_b].astype(F32)
        b_hi = pltpu.roll(C[at_hi, sl, col_b].astype(F32), HALF, 1)
        new_lo = ((tot[0:g] + a_lo) / lo_n).astype(BF16)
        new_hi = ((tot[g : 2 * g] + a_hi) / hi_n).astype(BF16)
        new_b = ((tot[2 * g :] + jnp.where(hm_g, b_lo, b_hi)) / jnp.where(hm_g, lo_n, hi_n)).astype(BF16)
        return new_lo, new_hi, new_b

    def cidx(t):
        ct = lax.rem(t, WIN)
        return 2 * lax.rem(ct, 2) + ct // 2

    def tree(at, k, near_sends):
        slots = (1, -1, 2, -2, 3, -3, 4)

        def far_send(ref, d, to):
            send(ref, ref, sem["sf"].at[k], sem["rf"].at[k, slots.index(d)], to_z(zq(to)))

        for d in (2, -2, 1, -1):
            far_send(at(q), d, d)
        near_sends(q)
        for d in slots:
            qs = qm(-d)
            wait(at(qs), sem["rf"].at[k, slots.index(d)])
            if d == 2:
                far_send(at(qs), 4, 2)
                far_send(at(qs), 3, 1)
            if d == -2:
                far_send(at(qs), -3, -1)
            near_sends(qs)

    def gather(N):
        ci = 2 * par + e

        def near_sends(qs):
            for i in range(3):
                send(N.at[c, ci, qs], N.at[c, ci, qs], sem["sl"].at[0], sem["rl"].at[0, i], to_z(zed(s * NEAR[i])))

        tree(lambda qs: N.at[c, ci, qs], 0, near_sends)
        send(N.at[c, ci], N.at[c, ci], sem["st"].at[0], sem["rt"].at[0], sib)
        for i in (2, 1, 0):
            cs = cidx(zed(-s * NEAR[i]))
            wait(N.at[c, cs], sem["rl"].at[0, i])
            send(N.at[c, cs], N.at[c, cs], sem["st"].at[0], sem["rt"].at[0], sib)

    def gather_rows(O):
        def near_sends(qs):
            at = O.at[2 * qs + e]
            for i, step in enumerate((1, -1, 2 * s)):
                send(at, at, sem["sl"].at[1], sem["rl"].at[1, i], to_z(zed(step)))

        tree(lambda qs: O.at[2 * qs + e], 1, near_sends)

    def out_parts(N, t):
        pair = pl.ds(2 * (t // 2), 2)
        rs = pl.ds(pl.multiple_of(g * lax.rem(t, 2), g), g)
        return N.at[c, pair, :, rs, :], N.at[c, pair, :, pl.ds(2 * g, g), :]

    def out_sends(N, OA, OB):
        for i in range(1, nx):
            t = xed(i)
            a, b = out_parts(N, t)
            send(a, OA.at[x], sem["so"].at[0], sem["ro"].at[0], to_x(t))
            send(b, OB.at[x], sem["so"].at[1], sem["ro"].at[1], to_x(t))
        a, b = out_parts(N, x)
        pltpu.make_async_copy(a, OA.at[x], sem["lo"].at[0]).start()
        pltpu.make_async_copy(b, OB.at[x], sem["lo"].at[1]).start()

    left = iota((g, LANES), 1) < HALF

    def out_rows(OA, OB, out):
        wait(OA.at[0], sem["lo"].at[0])
        wait(OB.at[0], sem["lo"].at[1])
        wait(OA.at[pl.ds(0, nx - 1)], sem["ro"].at[0])
        wait(OB.at[pl.ds(0, nx - 1)], sem["ro"].at[1])
        for ee in range(2):
            for qq in range(nq):
                r0 = g * (2 * qq + ee)
                for xx in range(nx):
                    ta = xx + (xx + 1) // 2
                    out[r0 : r0 + g, ta * LANES : (ta + 1) * LANES] = OA[xx, ee, qq]
                for y in range(nx // 2):
                    two = []
                    for xx in (2 * y, 2 * y + 1):
                        b = OB[xx, ee, qq].astype(F32)
                        two.append(jnp.where(h == 1, pltpu.roll(b, HALF, 1), b))
                    tb = 1 + 3 * y
                    out[r0 : r0 + g, tb * LANES : (tb + 1) * LANES] = jnp.where(left, two[0], two[1]).astype(BF16)

    def nearest(C, R):
        def body(k, m):
            ck = C[k]
            cross = lax.dot_general(ck, R[...], (((1,), (1,)), ((), ())), preferred_element_type=F32)
            cf = ck.astype(F32)
            csq = jnp.sum(cf * cf, axis=1, keepdims=True)
            d = csq - 2.0 * cross
            return jnp.minimum(m, jnp.min(d.reshape(rows // 8, 8, own), axis=0))

        m = lax.fori_loop(0, 2 * nx, body, jnp.full((8, own), jnp.inf, F32))
        mins = jnp.min(m, axis=0, keepdims=True)
        r = R[...].astype(F32)
        psq = jnp.sum(jnp.sum(r * r, axis=0, keepdims=True), axis=1, keepdims=True)
        return jnp.sum(mins, axis=1, keepdims=True) + psq

    @pl.loop(0, WIN)
    def _(i):
        class_sums(i, code1, v["W"], v["S1"], v["Sc1"])

    loads[2].wait()
    loads[3].wait()
    loads[4].wait()
    pl.semaphore_wait(barrier, 4 + (nq - 1) + (nx - 1) + 1)

    for i in range(3):
        class_sends(i, v["S1"], v["Sc1"], v["X11"], v["X1c1"], 0)
    for k, C in enumerate((v["C1"], v["C2"])):
        for i in range(1, nx):
            send(C.at[cb], C.at[cb], sem["sc"].at[k], sem["rc"].at[k], to_x(xed(i)))
        send(C.at[cb], C.at[cb], sem["sct"].at[k], sem["rct"].at[k], sib)

    for b in range(npts // LANES):
        row = code1[0:1, b * LANES : (b + 1) * LANES].astype(F32)
        v["CT"][b * LANES : (b + 1) * LANES, :] = jnp.transpose(jnp.broadcast_to(row, (LANES, LANES)))

    def twin_cents(C, k):
        wait(C.at[pl.ds(0, nx - 1)], sem["rc"].at[k])
        for i in range(1, nx):
            at = 2 * xed(i) + c
            send(C.at[at], C.at[at], sem["sct"].at[k], sem["rct"].at[k], sib)

    far_sums(v["S1"], v["Sc1"], v["X11"], v["X1c1"], v["T1"], v["Tc1"], v["XM1"], v["X21"], v["X2c1"], 0)
    twin_cents(v["C1"], 0)
    new_lo, new_hi, new_b = finish(v["T1"], v["Tc1"], v["X21"], v["X2c1"], v["C1"], 0)
    v["N1"][c, 2 * par + e, q, 0:g, :] = new_lo
    v["N1"][c, 2 * par + e, q, g : 2 * g, :] = new_hi
    v["N1"][c, 2 * par + e, q, 2 * g :, :] = new_b
    gather(v["N1"])
    twin_cents(v["C2"], 1)
    out_sends(v["N1"], v["OA1"], v["OB1"])
    wait(v["N1"].at[0], sem["rt"].at[0])

    kb = nq * g
    for cc in range(2):
        for k in range(WIN):
            base = (cc * WIN + k) * 2 * kb
            n = v["N1"][cc, k]
            v["L"][base : base + kb, 0:LANES] = n[:, 0:g, :].reshape(kb, LANES)
            v["L"][base + kb : base + 2 * kb, 0:LANES] = n[:, g : 2 * g, :].reshape(kb, LANES)
            b = n[:, 2 * g :, :].reshape(kb, LANES)
            v["L"][base : base + kb, LANES : 2 * LANES] = b
            v["L"][base + kb : base + 2 * kb, LANES : 2 * LANES] = pltpu.roll(b.astype(F32), HALF, 1).astype(BF16)

    @pl.loop(0, npts // blk)
    def _(i):
        sl = pl.ds(pl.multiple_of(i * blk, blk), blk)
        codes = v["CT"][sl, :]
        parts = []
        lane = iota((1, LANES), 1)
        for j in range(2 * nx * rows // LANES):
            r = lane + j * LANES
            cc = r // (WIN * 2 * kb)
            k = (r // (2 * kb)) & (WIN - 1)
            hl = (r // kb) & 1
            rq = (r // g) & (nq - 1)
            lab = rows * (2 * (2 * (k // 2) + hl) + cc) + g * (2 * rq + (k & 1)) + (r & (g - 1))
            parts.append(jnp.where(codes == lab.astype(F32), 1.0, 0.0).astype(BF16))
        oh = jnp.concatenate(parts, axis=1)
        looked = jnp.dot(oh, v["L"][...], preferred_element_type=F32)
        res = v["P"][sl, :].astype(F32) - looked
        v["W2"][sl, 0:LANES] = res[:, 0:LANES].astype(BF16)
        v["W2"][sl, LANES : 2 * LANES] = jnp.where(hm_b, res[:, LANES:], 1.0).astype(BF16)

    @pl.loop(0, WIN)
    def _(i):
        class_sums(i, code2, v["W2"], v["S2"], v["Sc2"])

        @pl.when(i < 3)
        def _():
            class_sends(i, v["S2"], v["Sc2"], v["X12"], v["X1c2"], 1)

    for i in range(1, nx):
        t = xed(i)
        sl = pl.ds(pl.multiple_of(own * (2 * t + c), own), own)
        send(v["W2"].at[sl, :], v["RR"].at[x], sem["srr"], sem["rrr"], to_x(t))
    sl = pl.ds(pl.multiple_of(own * cb, own), own)
    mine = pltpu.make_async_copy(v["W2"].at[sl, :], v["RR"].at[x], sem["ld"].at[5])
    mine.start()
    far_sums(v["S2"], v["Sc2"], v["X12"], v["X1c2"], v["T2"], v["Tc2"], v["XM2"], v["X22"], v["X2c2"], 1)
    out_rows(v["OA1"], v["OB1"], v["NW"])
    put_one = pltpu.make_async_copy(v["NW"], new1, sem["ld"].at[6])
    put_one.start()

    wait(v["C1"].at[pl.ds(0, nx)], sem["rct"].at[0])
    near_one = nearest(v["C1"], v["R1"])
    mine.wait()
    wait(v["RR"].at[pl.ds(0, nx - 1)], sem["rrr"])
    for xx in range(nx):
        ta = xx + (xx + 1) // 2
        v["R2"][:, ta * LANES : (ta + 1) * LANES] = v["RR"][xx, :, 0:LANES]
    left_own = iota((own, LANES), 1) < HALF
    for y in range(nx // 2):
        tb = 1 + 3 * y
        v["R2"][:, tb * LANES : (tb + 1) * LANES] = jnp.where(
            left_own,
            v["RR"][2 * y, :, LANES:].astype(F32),
            v["RR"][2 * y + 1, :, LANES:].astype(F32),
        ).astype(BF16)
    wait(v["C2"].at[pl.ds(0, nx)], sem["rct"].at[1])
    near_two = nearest(v["C2"], v["R2"])
    lane = iota((1, LANES), 1)
    v["D0"][c] = jnp.where(lane == 0, near_one, jnp.where(lane == 1, near_two, 0.0))
    send(v["D0"].at[c], v["D0"].at[c], sem["sd"].at[0], sem["rd"].at[0], sib)

    wait(v["D0"].at[0], sem["rd"].at[0])
    v["D1"][x] = v["D0"][0] + v["D0"][1]
    for i in range(1, nx):
        send(v["D1"].at[x], v["D1"].at[x], sem["sd"].at[1], sem["rd"].at[1], to_x(xed(i)))
    wait(v["D1"].at[pl.ds(0, nx - 1)], sem["rd"].at[1])
    tot = v["D1"][0]
    for i in range(1, nx):
        tot = tot + v["D1"][i]
    v["D2"][cl, q] = tot
    for o in range(1, nq):
        send(v["D2"].at[cl, q], v["D2"].at[cl, q], sem["sd"].at[2], sem["rd"].at[2], to_z(zed(WIN * o)))

    new_lo, new_hi, new_b = finish(v["T2"], v["Tc2"], v["X22"], v["X2c2"], v["C2"], 1)
    v["NC"][0:g, :] = new_lo
    v["NC"][g : 2 * g, :] = new_b
    v["NC"][2 * g :, :] = new_hi
    role = x // 2 == par
    for hl in range(2):
        t = 2 * par + hl
        src = v["NC"].at[pl.ds(g * hl, 2 * g), :]

        @pl.when(t != x)
        def _():
            send(src, v["Y"].at[x], sem["sy"], sem["ry"], to_x(t))

        @pl.when(t == x)
        def _():
            pltpu.make_async_copy(src, v["Y"].at[x], sem["ly"]).start()

    def pass_dist():
        wait(v["D2"].at[0, pl.ds(0, nq - 1)], sem["rd"].at[2])
        for i in range(3):
            send(v["D2"].at[cl], v["D2"].at[cl], sem["sd"].at[3], sem["rd"].at[3], to_z(zed(s * NEAR[i])))

    @pl.when(role)
    def _():
        wait(v["Y"].at[pl.ds(0, nx - 1)], sem["ry"])
        wait(v["Y"].at[0], sem["ly"])
        mine = 2 * q + e
        for y in range(nx // 2):
            two = []
            for xx in (2 * y, 2 * y + 1):
                top = v["Y"][xx, 0:g, :].astype(F32)
                low = v["Y"][xx, g : 2 * g, :].astype(F32)
                ta = xx + (xx + 1) // 2
                v["O"][mine, :, ta * LANES : (ta + 1) * LANES] = jnp.where(h == 1, low, top).astype(BF16)
                two.append(jnp.where(h == 1, pltpu.roll(top, HALF, 1), low))
            tb = 1 + 3 * y
            v["O"][mine, :, tb * LANES : (tb + 1) * LANES] = jnp.where(left, two[0], two[1]).astype(BF16)
        gather_rows(v["O"])
        pass_dist()
        wait(v["O"].at[pl.ds(0, nq)], sem["rl"].at[1, 2])

    @pl.when(jnp.logical_not(role))
    def _():
        pass_dist()
        wait(v["O"].at[pl.ds(0, nq)], sem["rl"].at[1, 0])
        wait(v["O"].at[pl.ds(0, nq)], sem["rl"].at[1, 1])

    put_two = pltpu.make_async_copy(v["O"], new2, sem["ld"].at[7])
    put_two.start()

    wait(v["D2"].at[pl.ds(0, 3)], sem["rd"].at[3])
    tot = v["D2"][0, 0]
    for i in range(1, nz):
        tot = tot + v["D2"][i // nq, i % nq]
    dist[...] = tot / jnp.float32(npts * nz * pts.shape[1])

    for k in range(2):
        wait(v["X11"], sem["s1"].at[k])
        wait(v["X1c1"], sem["s1c"].at[k])
        wait(v["X11"].at[0, pl.ds(0, nq - 1)], sem["s2"].at[k])
        wait(v["X2c1"], sem["s2c"].at[k])
        wait(v["C1"].at[pl.ds(0, nx - 1)], sem["sc"].at[k])
        wait(v["C1"].at[pl.ds(0, nx)], sem["sct"].at[k])
    wait(v["N1"].at[0, 0, pl.ds(0, nq - 1)], sem["sf"].at[0])
    wait(v["N1"].at[0, pl.ds(0, 3)], sem["sl"].at[0])
    wait(v["OA1"].at[pl.ds(0, nx - 1)], sem["so"].at[0])
    wait(v["OB1"].at[pl.ds(0, nx - 1)], sem["so"].at[1])
    wait(v["N1"].at[0], sem["st"].at[0])
    wait(v["RR"].at[pl.ds(0, nx - 1)], sem["srr"])
    wait(v["D0"].at[0], sem["sd"].at[0])
    wait(v["D1"].at[pl.ds(0, nx - 1)], sem["sd"].at[1])
    wait(v["D2"].at[0, pl.ds(0, nq - 1)], sem["sd"].at[2])
    wait(v["D2"].at[pl.ds(0, 3)], sem["sd"].at[3])

    @pl.when(role)
    def _():
        wait(v["O"].at[pl.ds(0, nq - 1)], sem["sf"].at[1])
        wait(v["X11"], sem["sl"].at[1])
        wait(v["Y"].at[0], sem["sy"])

    @pl.when(jnp.logical_not(role))
    def _():
        wait(v["Y"].at[pl.ds(0, 2)], sem["sy"])

    put_one.wait()
    put_two.wait()


def solution(mesh):
    nz = mesh.shape["pts"]
    nx = mesh.shape["cb"] // 2
    nq = nz // WIN

    def local(points, code_one, code_two, cent_one, cent_two):
        npts, width = points.shape
        rows = cent_one.shape[0]
        own = npts // (2 * nx)
        g = 2 * rows // nz
        ch = 3 * g
        vm = pltpu.VMEM
        v = {
            "P": vm((npts, 2 * LANES), BF16),
            "W": vm((npts, 2 * LANES), BF16),
            "W2": vm((npts, 2 * LANES), BF16),
            "CT": vm((npts, LANES), F32),
            "L": vm((2 * nx * rows, 2 * LANES), BF16),
            "R1": vm((own, width), BF16),
            "R2": vm((own, width), BF16),
            "RR": vm((nx, own, 2 * LANES), BF16),
            "D0": vm((2, 1, LANES), F32),
            "D1": vm((nx, 1, LANES), F32),
            "D2": vm((WIN, nq, 1, LANES), F32),
        }
        v["N1"] = vm((2, WIN, nq, ch, LANES), BF16)
        v["OA1"] = vm((nx, 2, nq, g, LANES), BF16)
        v["OB1"] = vm((nx, 2, nq, g, LANES), BF16)
        v["NW"] = vm((rows, width), BF16)
        v["NC"] = vm((ch, LANES), BF16)
        v["Y"] = vm((nx, 2 * g, LANES), BF16)
        v["O"] = vm((2 * nq, g, width), BF16)
        for k in ("1", "2"):
            v["C" + k] = vm((2 * nx, rows, width), BF16)
            v["S" + k] = vm((WIN, nq, ch, LANES), F32)
            v["Sc" + k] = vm((WIN, nq, 1, LANES), F32)
            v["X1" + k] = vm((3, nq, ch, LANES), F32)
            v["X1c" + k] = vm((3, nq, 1, LANES), F32)
            v["T" + k] = vm((nq, ch, LANES), F32)
            v["Tc" + k] = vm((nq, 1, LANES), F32)
            v["XM" + k] = vm((3, ch, LANES), F32)
            v["X2" + k] = vm((4, ch, LANES), F32)
            v["X2c" + k] = vm((nq - 1, 1, LANES), F32)
        dma = pltpu.SemaphoreType.DMA
        sem = {
            "ld": dma((8,)),
            "s1": dma((2,)), "r1": dma((2, nq)), "s1c": dma((2,)), "r1c": dma((2,)),
            "rm": dma((2, 3)), "s2": dma((2,)), "r2": dma((2,)), "s2c": dma((2,)), "r2c": dma((2,)),
            "sf": dma((2,)), "rf": dma((2, nq - 1)), "sl": dma((2,)), "rl": dma((2, 3)),
            "st": dma((1,)), "rt": dma((1,)),
            "so": dma((2,)), "ro": dma((2,)), "lo": dma((2,)),
            "sy": dma(()), "ry": dma(()), "ly": dma(()),
            "sc": dma((2,)), "rc": dma((2,)), "sct": dma((2,)), "rct": dma((2,)),
            "srr": dma(()), "rrr": dma(()),
            "sd": dma((4,)), "rd": dma((4,)),
        }
        hbm = pl.BlockSpec(memory_space=pl.ANY)
        vmem = pl.BlockSpec(memory_space=pltpu.VMEM)
        new_one, new_two, dist = pl.pallas_call(
            functools.partial(kernel, nz, nx),
            out_shape=(
                jax.ShapeDtypeStruct((rows, width), BF16),
                jax.ShapeDtypeStruct((2 * nq, g, width), BF16),
                jax.ShapeDtypeStruct((1, LANES), F32),
            ),
            in_specs=[hbm, vmem, vmem, hbm, hbm],
            out_specs=(hbm, hbm, vmem),
            scratch_shapes=[v, sem],
            compiler_params=pltpu.CompilerParams(
                collective_id=0, has_side_effects=True, vmem_limit_bytes=60 * 1024 * 1024
            ),
        )(points, code_one.reshape(1, npts), code_two.reshape(1, npts), cent_one, cent_two)
        return new_one, new_two.reshape(rows, width), dist[0, :2]

    cents = P(("groups", "cb"), None)
    return jax.shard_map(
        local,
        mesh=mesh,
        in_specs=(P(("groups", "pts"), None), P(("groups", "pts")), P(("groups", "pts")), cents, cents),
        out_specs=(cents, cents, P("groups")),
        check_vma=False,
    )
```

```python
import functools

import jax
import jax.numpy as jnp
from jax import lax
from jax.experimental import pallas as pl
from jax.experimental.pallas import tpu as pltpu
from jax.sharding import PartitionSpec as P

MESH = pl.DeviceIdType.MESH
F32 = jnp.float32
BF16 = jnp.bfloat16
LANES = 128
HALF = 64
WIN = 4
NEAR = (-2, -1, 1)


TREE = (4, 3, -3, 1, -1, 2, -2)


def iota(shape, dim):
    return lax.broadcasted_iota(jnp.int32, shape, dim)


def kernel(nz, nx, pts, code1, code2, cent1, cent2, new1, new2, dist, v, sem):
    z = lax.axis_index("pts")
    cb = lax.axis_index("cb")
    x = cb // 2
    c = cb - 2 * x
    h = x - 2 * (x // 2)
    q = z // WIN
    cl = z - WIN * q
    par = cl - 2 * (cl // 2)
    e = cl // 2
    nq = nz // WIN
    s = 1 - 2 * c
    rows = cent1.shape[0]
    npts = pts.shape[0]
    chip = npts // nx
    g = 2 * rows // nz

    def qm(d):
        return lax.rem(q + d * s + 2 * nq, nq)

    def zq(d):
        return lax.rem(z + WIN * d * s + 2 * nz, nz)

    def zed(step):
        return lax.rem(z + step + nz, nz)

    def to_z(t):
        return {"pts": t}

    def to_x(t):
        return {"cb": 2 * t + c}

    sib = {"cb": 2 * x + 1 - c}

    def send(src, dst, ss, rs, where):
        pltpu.make_async_remote_copy(
            src_ref=src, dst_ref=dst, send_sem=ss, recv_sem=rs, device_id=where, device_id_type=MESH
        ).start()

    def wait(ref, sm):
        pltpu.make_async_copy(ref, ref, sm).wait()

    def xed(i):
        return lax.rem(x + i, nx)

    barrier = pltpu.get_barrier_semaphore()
    for step in (-2, -1, 1, 2):
        pl.semaphore_signal(barrier, inc=1, device_id=to_z(zed(step)), device_id_type=MESH)
    for o in range(1, nq):
        pl.semaphore_signal(barrier, inc=1, device_id=to_z(zed(WIN * o)), device_id_type=MESH)
    for i in range(1, nx):
        pl.semaphore_signal(barrier, inc=1, device_id=to_x(xed(i)), device_id_type=MESH)
    pl.semaphore_signal(barrier, inc=1, device_id=sib, device_id_type=MESH)

    tile_a = x + (x + 1) // 2
    tile_b = 1 + 3 * (x // 2)
    col_a = pl.ds(pl.multiple_of(tile_a * LANES, LANES), LANES)
    col_b = pl.ds(pl.multiple_of(tile_b * LANES, LANES), LANES)
    loads = [
        pltpu.make_async_copy(pts.at[:, col_a], v["P"].at[:, 0:LANES], sem["ld"].at[0]),
        pltpu.make_async_copy(pts.at[:, col_b], v["P"].at[:, LANES : 2 * LANES], sem["ld"].at[1]),
        pltpu.make_async_copy(cent1, v["C1"].at[x], sem["ld"].at[2]),
        pltpu.make_async_copy(cent2, v["C2"].at[x], sem["ld"].at[3]),
        pltpu.make_async_copy(pts.at[pl.ds(pl.multiple_of(x * chip, chip), chip), :], v["R1"], sem["ld"].at[4]),
    ]
    for ld in loads:
        ld.start()
    loads[0].wait()
    loads[1].wait()

    blk = 256
    hm_b = iota((blk, LANES), 1) // HALF == h
    hm_g = iota((g, LANES), 1) // HALF == h

    @pl.loop(0, npts // blk)
    def _(i):
        sl = pl.ds(pl.multiple_of(i * blk, blk), blk)
        v["W"][sl, 0:LANES] = v["P"][sl, 0:LANES]
        b = v["P"][sl, LANES : 2 * LANES].astype(F32)
        v["W"][sl, LANES : 2 * LANES] = jnp.where(hm_b, b, 1.0).astype(BF16)

    m16 = (iota((nq, g, LANES), 2) & (g - 1)) == iota((nq, g, LANES), 1)

    def class_of(i):
        t = zed(s * (i - 2 + (i // 2) * (5 - 2 * i)))
        return t, t // WIN, lax.rem(t, WIN)

    def class_sums(i, code, w, S, Sc):
        _, _, ct = class_of(i)
        pt = lax.rem(ct, 2)
        et = ct // 2
        n = 2 * nq * g
        r = iota((n, 1), 0)
        hl = r // (nq * g)
        rq = (r // g) & (nq - 1)
        lab = rows * (2 * (2 * pt + hl) + c) + g * (2 * rq + et) + (r & (g - 1))
        oh = jnp.where(lab == code[...], 1.0, 0.0).astype(BF16)
        out = jnp.dot(oh, w[...], preferred_element_type=F32)
        lo, hi = out[: nq * g], out[nq * g :]
        S[ct, :, 0:g, :] = lo[:, :LANES].reshape(nq, g, LANES)
        S[ct, :, g : 2 * g, :] = hi[:, :LANES].reshape(nq, g, LANES)
        lb = lo[:, LANES:]
        hb = pltpu.roll(hi[:, LANES:], HALF, 1)
        hm = iota(lb.shape, 1) // HALF == h
        S[ct, :, 2 * g :, :] = jnp.where(hm, lb, hb).reshape(nq, g, LANES)
        cnt = jnp.where(hm, hb, lb).reshape(nq, g, LANES)
        Sc[ct] = jnp.sum(jnp.where(m16, cnt, 0.0), axis=1, keepdims=True)

    def class_sends(i, S, Sc, X1, X1c, k):
        t, qt, ct = class_of(i)
        send(Sc.at[ct], X1c.at[i], sem["s1c"].at[k], sem["r1c"].at[k], to_z(t))
        for d in TREE + (0,):
            qd = lax.rem(qt + d * s + 2 * nq, nq)
            send(S.at[ct, qd], X1.at[i, qd], sem["s1"].at[k], sem["r1"].at[k, qd], to_z(t))

    def far_sums(S, Sc, X1, X1c, T, Tc, XM, X2, X2c, k):
        for d in TREE + (0,):
            qd = qm(d)
            wait(X1.at[:, 0], sem["r1"].at[k, qd])
            t = S[cl, qd] + X1[0, qd] + X1[1, qd] + X1[2, qd]
            if d == 2:
                wait(XM.at[0], sem["rm"].at[k, 0])
                wait(XM.at[1], sem["rm"].at[k, 1])
                t = t + XM[0] + XM[1]
            if d == -2:
                wait(XM.at[2], sem["rm"].at[k, 2])
                t = t + XM[2]
            T[qd] = t
            if d == 4:
                send(T.at[qd], XM.at[0], sem["s2"].at[k], sem["rm"].at[k, 0], to_z(zq(2)))
                wait(X1c, sem["r1c"].at[k])
                Tc[...] = Sc[cl] + X1c[0] + X1c[1] + X1c[2]
                for o in range(1, nq):
                    qo = lax.rem(q + o, nq)
                    send(Tc.at[qo], X2c.at[o - 1], sem["s2c"].at[k], sem["r2c"].at[k], to_z(zed(WIN * o)))
            elif d == 3:
                send(T.at[qd], XM.at[1], sem["s2"].at[k], sem["rm"].at[k, 1], to_z(zq(1)))
            elif d == -3:
                send(T.at[qd], XM.at[2], sem["s2"].at[k], sem["rm"].at[k, 2], to_z(zq(-1)))
            elif d != 0:
                at = (1, -1, 2, -2).index(d)
                send(T.at[qd], X2.at[at], sem["s2"].at[k], sem["r2"].at[k], to_z(zq(d)))

    def finish(T, Tc, X2, X2c, C, k):
        wait(X2c, sem["r2c"].at[k])
        cnt = Tc[q]
        for o in range(nq - 1):
            cnt = cnt + X2c[o]
        wait(X2, sem["r2"].at[k])
        tot = T[q] + X2[0] + X2[1] + X2[2] + X2[3]
        full = jnp.broadcast_to(cnt, (g, LANES))
        diag = (iota((g, LANES), 1) & (HALF - 1)) == iota((g, LANES), 0)
        lo_n = jnp.sum(jnp.where(diag & jnp.logical_not(hm_g), full, 0.0), axis=1, keepdims=True) + 1.0
        hi_n = jnp.sum(jnp.where(diag & hm_g, full, 0.0), axis=1, keepdims=True) + 1.0
        sl = pl.ds(pl.multiple_of(g * (z // 2), g), g)
        at_lo = 2 * par
        at_hi = 2 * par + 1
        a_lo = C[at_lo, sl, col_a].astype(F32)
        a_hi = C[at_hi, sl, col_a].astype(F32)
        b_lo = C[at_lo, sl, col_b].astype(F32)
        b_hi = pltpu.roll(C[at_hi, sl, col_b].astype(F32), HALF, 1)
        new_lo = ((tot[0:g] + a_lo) / lo_n).astype(BF16)
        new_hi = ((tot[g : 2 * g] + a_hi) / hi_n).astype(BF16)
        new_b = ((tot[2 * g :] + jnp.where(hm_g, b_lo, b_hi)) / jnp.where(hm_g, lo_n, hi_n)).astype(BF16)
        return new_lo, new_hi, new_b

    def cidx(t):
        ct = lax.rem(t, WIN)
        return 2 * lax.rem(ct, 2) + ct // 2

    def tree(at, k, near_sends):
        slots = (1, -1, 2, -2, 3, -3, 4)

        def far_send(ref, d, to):
            send(ref, ref, sem["sf"].at[k], sem["rf"].at[k, slots.index(d)], to_z(zq(to)))

        for d in (2, -2, 1, -1):
            far_send(at(q), d, d)
        near_sends(q)
        for d in slots:
            qs = qm(-d)
            wait(at(qs), sem["rf"].at[k, slots.index(d)])
            if d == 2:
                far_send(at(qs), 4, 2)
                far_send(at(qs), 3, 1)
            if d == -2:
                far_send(at(qs), -3, -1)
            near_sends(qs)

    def gather(N):
        ci = 2 * par + e

        def near_sends(qs):
            for i in range(3):
                send(N.at[c, ci, qs], N.at[c, ci, qs], sem["sl"].at[0], sem["rl"].at[0, i], to_z(zed(s * NEAR[i])))

        tree(lambda qs: N.at[c, ci, qs], 0, near_sends)
        send(N.at[c, ci], N.at[c, ci], sem["st"].at[0], sem["rt"].at[0], sib)
        for i in (2, 1, 0):
            cs = cidx(zed(-s * NEAR[i]))
            wait(N.at[c, cs], sem["rl"].at[0, i])
            send(N.at[c, cs], N.at[c, cs], sem["st"].at[0], sem["rt"].at[0], sib)

    def gather_rows(O):
        def near_sends(qs):
            at = O.at[2 * qs + e]
            for i, step in enumerate((1, -1, 2 * s)):
                send(at, at, sem["sl"].at[1], sem["rl"].at[1, i], to_z(zed(step)))

        tree(lambda qs: O.at[2 * qs + e], 1, near_sends)

    def out_parts(N, t):
        pair = pl.ds(2 * (t // 2), 2)
        rs = pl.ds(pl.multiple_of(g * lax.rem(t, 2), g), g)
        return N.at[c, pair, :, rs, :], N.at[c, pair, :, pl.ds(2 * g, g), :]

    def out_sends(N, OA, OB):
        for i in range(1, nx):
            t = xed(i)
            a, b = out_parts(N, t)
            send(a, OA.at[x], sem["so"].at[0], sem["ro"].at[0], to_x(t))
            send(b, OB.at[x], sem["so"].at[1], sem["ro"].at[1], to_x(t))
        a, b = out_parts(N, x)
        pltpu.make_async_copy(a, OA.at[x], sem["lo"].at[0]).start()
        pltpu.make_async_copy(b, OB.at[x], sem["lo"].at[1]).start()

    left = iota((g, LANES), 1) < HALF

    def out_rows(OA, OB, out):
        wait(OA.at[0], sem["lo"].at[0])
        wait(OB.at[0], sem["lo"].at[1])
        wait(OA.at[pl.ds(0, nx - 1)], sem["ro"].at[0])
        wait(OB.at[pl.ds(0, nx - 1)], sem["ro"].at[1])
        for ee in range(2):
            for qq in range(nq):
                r0 = g * (2 * qq + ee)
                for xx in range(nx):
                    ta = xx + (xx + 1) // 2
                    out[r0 : r0 + g, ta * LANES : (ta + 1) * LANES] = OA[xx, ee, qq]
                for y in range(nx // 2):
                    two = []
                    for xx in (2 * y, 2 * y + 1):
                        b = OB[xx, ee, qq].astype(F32)
                        two.append(jnp.where(h == 1, pltpu.roll(b, HALF, 1), b))
                    tb = 1 + 3 * y
                    out[r0 : r0 + g, tb * LANES : (tb + 1) * LANES] = jnp.where(left, two[0], two[1]).astype(BF16)

    def nearest(C, R):
        def body(k, m):
            ck = C[k]
            cross = lax.dot_general(ck, R[...], (((1,), (1,)), ((), ())), preferred_element_type=F32)
            cf = ck.astype(F32)
            csq = jnp.sum(cf * cf, axis=1, keepdims=True)
            d = csq - 2.0 * cross
            return jnp.minimum(m, jnp.min(d.reshape(rows // 8, 8, chip), axis=0))

        m = lax.fori_loop(0, nx, body, jnp.full((8, chip), jnp.inf, F32))
        r = R[...].astype(F32)
        psq = jnp.sum(jnp.sum(r * r, axis=0, keepdims=True), axis=1, keepdims=True)
        return jnp.min(m, axis=0, keepdims=True), psq

    @pl.loop(0, WIN)
    def _(i):
        class_sums(i, code1, v["W"], v["S1"], v["Sc1"])

    loads[2].wait()
    loads[3].wait()
    loads[4].wait()
    pl.semaphore_wait(barrier, 4 + (nq - 1) + (nx - 1) + 1)

    for i in range(3):
        class_sends(i, v["S1"], v["Sc1"], v["X11"], v["X1c1"], 0)
    for k, C in enumerate((v["C1"], v["C2"])):
        for i in range(1, nx):
            send(C.at[x], C.at[x], sem["sc"].at[k], sem["rc"].at[k], to_x(xed(i)))

    for b in range(npts // LANES):
        row = code1[0:1, b * LANES : (b + 1) * LANES].astype(F32)
        v["CT"][b * LANES : (b + 1) * LANES, :] = jnp.transpose(jnp.broadcast_to(row, (LANES, LANES)))

    far_sums(v["S1"], v["Sc1"], v["X11"], v["X1c1"], v["T1"], v["Tc1"], v["XM1"], v["X21"], v["X2c1"], 0)
    wait(v["C1"].at[pl.ds(0, nx - 1)], sem["rc"].at[0])
    mins_one, psq_one = nearest(v["C1"], v["R1"])
    v["D0"][c, 0] = mins_one
    new_lo, new_hi, new_b = finish(v["T1"], v["Tc1"], v["X21"], v["X2c1"], v["C1"], 0)
    v["N1"][c, 2 * par + e, q, 0:g, :] = new_lo
    v["N1"][c, 2 * par + e, q, g : 2 * g, :] = new_hi
    v["N1"][c, 2 * par + e, q, 2 * g :, :] = new_b
    gather(v["N1"])
    out_sends(v["N1"], v["OA1"], v["OB1"])
    wait(v["N1"].at[0], sem["rt"].at[0])

    kb = nq * g
    for cc in range(2):
        for k in range(WIN):
            base = (cc * WIN + k) * 2 * kb
            n = v["N1"][cc, k]
            v["L"][base : base + kb, 0:LANES] = n[:, 0:g, :].reshape(kb, LANES)
            v["L"][base + kb : base + 2 * kb, 0:LANES] = n[:, g : 2 * g, :].reshape(kb, LANES)
            b = n[:, 2 * g :, :].reshape(kb, LANES)
            v["L"][base : base + kb, LANES : 2 * LANES] = b
            v["L"][base + kb : base + 2 * kb, LANES : 2 * LANES] = pltpu.roll(b.astype(F32), HALF, 1).astype(BF16)

    @pl.loop(0, npts // blk)
    def _(i):
        sl = pl.ds(pl.multiple_of(i * blk, blk), blk)
        codes = v["CT"][sl, :]
        parts = []
        lane = iota((1, LANES), 1)
        for j in range(2 * nx * rows // LANES):
            r = lane + j * LANES
            cc = r // (WIN * 2 * kb)
            k = (r // (2 * kb)) & (WIN - 1)
            hl = (r // kb) & 1
            rq = (r // g) & (nq - 1)
            lab = rows * (2 * (2 * (k // 2) + hl) + cc) + g * (2 * rq + (k & 1)) + (r & (g - 1))
            parts.append(jnp.where(codes == lab.astype(F32), 1.0, 0.0).astype(BF16))
        oh = jnp.concatenate(parts, axis=1)
        looked = jnp.dot(oh, v["L"][...], preferred_element_type=F32)
        res = v["P"][sl, :].astype(F32) - looked
        v["W2"][sl, 0:LANES] = res[:, 0:LANES].astype(BF16)
        v["W2"][sl, LANES : 2 * LANES] = jnp.where(hm_b, res[:, LANES:], 1.0).astype(BF16)

    @pl.loop(0, WIN)
    def _(i):
        class_sums(i, code2, v["W2"], v["S2"], v["Sc2"])

        @pl.when(i < 3)
        def _():
            class_sends(i, v["S2"], v["Sc2"], v["X12"], v["X1c2"], 1)

    for i in range(1, nx):
        t = xed(i)
        sl = pl.ds(pl.multiple_of(chip * t, chip), chip)
        send(v["W2"].at[sl, :], v["RR"].at[x], sem["srr"], sem["rrr"], to_x(t))
    sl = pl.ds(pl.multiple_of(chip * x, chip), chip)
    mine = pltpu.make_async_copy(v["W2"].at[sl, :], v["RR"].at[x], sem["ld"].at[5])
    mine.start()
    far_sums(v["S2"], v["Sc2"], v["X12"], v["X1c2"], v["T2"], v["Tc2"], v["XM2"], v["X22"], v["X2c2"], 1)
    out_rows(v["OA1"], v["OB1"], v["NW"])
    put_one = pltpu.make_async_copy(v["NW"], new1, sem["ld"].at[6])
    put_one.start()

    mine.wait()
    wait(v["RR"].at[pl.ds(0, nx - 1)], sem["rrr"])
    for xx in range(nx):
        ta = xx + (xx + 1) // 2
        v["R2"][:, ta * LANES : (ta + 1) * LANES] = v["RR"][xx, :, 0:LANES]
    left_own = iota((chip, LANES), 1) < HALF
    for y in range(nx // 2):
        tb = 1 + 3 * y
        v["R2"][:, tb * LANES : (tb + 1) * LANES] = jnp.where(
            left_own,
            v["RR"][2 * y, :, LANES:].astype(F32),
            v["RR"][2 * y + 1, :, LANES:].astype(F32),
        ).astype(BF16)
    wait(v["C2"].at[pl.ds(0, nx - 1)], sem["rc"].at[1])
    mins_two, psq_two = nearest(v["C2"], v["R2"])
    v["D0"][c, 1] = mins_two
    send(v["D0"].at[c], v["D0"].at[c], sem["sd"].at[0], sem["rd"].at[0], sib)
    wait(v["D0"].at[0], sem["rd"].at[0])
    lane = iota((1, LANES), 1)
    tot_one = jnp.sum(jnp.minimum(v["D0"][0, 0], v["D0"][1, 0]), axis=1, keepdims=True) + psq_one
    tot_two = jnp.sum(jnp.minimum(v["D0"][0, 1], v["D0"][1, 1]), axis=1, keepdims=True) + psq_two
    v["D1"][x] = jnp.where(lane == 0, tot_one, jnp.where(lane == 1, tot_two, 0.0))
    for i in range(1, nx):
        send(v["D1"].at[x], v["D1"].at[x], sem["sd"].at[1], sem["rd"].at[1], to_x(xed(i)))

    new_lo, new_hi, new_b = finish(v["T2"], v["Tc2"], v["X22"], v["X2c2"], v["C2"], 1)
    v["NC"][0:g, :] = new_lo
    v["NC"][g : 2 * g, :] = new_b
    v["NC"][2 * g :, :] = new_hi
    role = x // 2 == par
    for hl in range(2):
        t = 2 * par + hl
        src = v["NC"].at[pl.ds(g * hl, 2 * g), :]

        @pl.when(t != x)
        def _():
            send(src, v["Y"].at[x], sem["sy"], sem["ry"], to_x(t))

        @pl.when(t == x)
        def _():
            pltpu.make_async_copy(src, v["Y"].at[x], sem["ly"]).start()

    wait(v["D1"].at[pl.ds(0, nx - 1)], sem["rd"].at[1])
    tot = v["D1"][0]
    for i in range(1, nx):
        tot = tot + v["D1"][i]
    v["D2"][cl, q] = tot
    for o in range(1, nq):
        send(v["D2"].at[cl, q], v["D2"].at[cl, q], sem["sd"].at[2], sem["rd"].at[2], to_z(zed(WIN * o)))

    def pass_dist():
        wait(v["D2"].at[0, pl.ds(0, nq - 1)], sem["rd"].at[2])
        for i in range(3):
            send(v["D2"].at[cl], v["D2"].at[cl], sem["sd"].at[3], sem["rd"].at[3], to_z(zed(s * NEAR[i])))

    @pl.when(role)
    def _():
        wait(v["Y"].at[pl.ds(0, nx - 1)], sem["ry"])
        wait(v["Y"].at[0], sem["ly"])
        mine = 2 * q + e
        for y in range(nx // 2):
            two = []
            for xx in (2 * y, 2 * y + 1):
                top = v["Y"][xx, 0:g, :].astype(F32)
                low = v["Y"][xx, g : 2 * g, :].astype(F32)
                ta = xx + (xx + 1) // 2
                v["O"][mine, :, ta * LANES : (ta + 1) * LANES] = jnp.where(h == 1, low, top).astype(BF16)
                two.append(jnp.where(h == 1, pltpu.roll(top, HALF, 1), low))
            tb = 1 + 3 * y
            v["O"][mine, :, tb * LANES : (tb + 1) * LANES] = jnp.where(left, two[0], two[1]).astype(BF16)
        gather_rows(v["O"])
        pass_dist()
        wait(v["O"].at[pl.ds(0, nq)], sem["rl"].at[1, 2])

    @pl.when(jnp.logical_not(role))
    def _():
        pass_dist()
        wait(v["O"].at[pl.ds(0, nq)], sem["rl"].at[1, 0])
        wait(v["O"].at[pl.ds(0, nq)], sem["rl"].at[1, 1])

    put_two = pltpu.make_async_copy(v["O"], new2, sem["ld"].at[7])
    put_two.start()

    wait(v["D2"].at[pl.ds(0, 3)], sem["rd"].at[3])
    tot = v["D2"][0, 0]
    for i in range(1, nz):
        tot = tot + v["D2"][i // nq, i % nq]
    dist[...] = tot / jnp.float32(npts * nz * pts.shape[1])

    for k in range(2):
        wait(v["X11"], sem["s1"].at[k])
        wait(v["X1c1"], sem["s1c"].at[k])
        wait(v["X11"].at[0, pl.ds(0, nq - 1)], sem["s2"].at[k])
        wait(v["X2c1"], sem["s2c"].at[k])
        wait(v["C1"].at[pl.ds(0, nx - 1)], sem["sc"].at[k])
    wait(v["N1"].at[0, 0, pl.ds(0, nq - 1)], sem["sf"].at[0])
    wait(v["N1"].at[0, pl.ds(0, 3)], sem["sl"].at[0])
    wait(v["OA1"].at[pl.ds(0, nx - 1)], sem["so"].at[0])
    wait(v["OB1"].at[pl.ds(0, nx - 1)], sem["so"].at[1])
    wait(v["N1"].at[0], sem["st"].at[0])
    wait(v["RR"].at[pl.ds(0, nx - 1)], sem["srr"])
    wait(v["D0"].at[0], sem["sd"].at[0])
    wait(v["D1"].at[pl.ds(0, nx - 1)], sem["sd"].at[1])
    wait(v["D2"].at[0, pl.ds(0, nq - 1)], sem["sd"].at[2])
    wait(v["D2"].at[pl.ds(0, 3)], sem["sd"].at[3])

    @pl.when(role)
    def _():
        wait(v["O"].at[pl.ds(0, nq - 1)], sem["sf"].at[1])
        wait(v["X11"], sem["sl"].at[1])
        wait(v["Y"].at[0], sem["sy"])

    @pl.when(jnp.logical_not(role))
    def _():
        wait(v["Y"].at[pl.ds(0, 2)], sem["sy"])

    put_one.wait()
    put_two.wait()


def solution(mesh):
    nz = mesh.shape["pts"]
    nx = mesh.shape["cb"] // 2
    nq = nz // WIN

    def local(points, code_one, code_two, cent_one, cent_two):
        npts, width = points.shape
        rows = cent_one.shape[0]
        chip = npts // nx
        g = 2 * rows // nz
        ch = 3 * g
        vm = pltpu.VMEM
        v = {
            "P": vm((npts, 2 * LANES), BF16),
            "W": vm((npts, 2 * LANES), BF16),
            "W2": vm((npts, 2 * LANES), BF16),
            "CT": vm((npts, LANES), F32),
            "L": vm((2 * nx * rows, 2 * LANES), BF16),
            "R1": vm((chip, width), BF16),
            "R2": vm((chip, width), BF16),
            "RR": vm((nx, chip, 2 * LANES), BF16),
            "D0": vm((2, 2, 1, chip), F32),
            "D1": vm((nx, 1, LANES), F32),
            "D2": vm((WIN, nq, 1, LANES), F32),
        }
        v["N1"] = vm((2, WIN, nq, ch, LANES), BF16)
        v["OA1"] = vm((nx, 2, nq, g, LANES), BF16)
        v["OB1"] = vm((nx, 2, nq, g, LANES), BF16)
        v["NW"] = vm((rows, width), BF16)
        v["NC"] = vm((ch, LANES), BF16)
        v["Y"] = vm((nx, 2 * g, LANES), BF16)
        v["O"] = vm((2 * nq, g, width), BF16)
        for k in ("1", "2"):
            v["C" + k] = vm((nx, rows, width), BF16)
            v["S" + k] = vm((WIN, nq, ch, LANES), F32)
            v["Sc" + k] = vm((WIN, nq, 1, LANES), F32)
            v["X1" + k] = vm((3, nq, ch, LANES), F32)
            v["X1c" + k] = vm((3, nq, 1, LANES), F32)
            v["T" + k] = vm((nq, ch, LANES), F32)
            v["Tc" + k] = vm((nq, 1, LANES), F32)
            v["XM" + k] = vm((3, ch, LANES), F32)
            v["X2" + k] = vm((4, ch, LANES), F32)
            v["X2c" + k] = vm((nq - 1, 1, LANES), F32)
        dma = pltpu.SemaphoreType.DMA
        sem = {
            "ld": dma((8,)),
            "s1": dma((2,)), "r1": dma((2, nq)), "s1c": dma((2,)), "r1c": dma((2,)),
            "rm": dma((2, 3)), "s2": dma((2,)), "r2": dma((2,)), "s2c": dma((2,)), "r2c": dma((2,)),
            "sf": dma((2,)), "rf": dma((2, nq - 1)), "sl": dma((2,)), "rl": dma((2, 3)),
            "st": dma((1,)), "rt": dma((1,)),
            "so": dma((2,)), "ro": dma((2,)), "lo": dma((2,)),
            "sy": dma(()), "ry": dma(()), "ly": dma(()),
            "sc": dma((2,)), "rc": dma((2,)),
            "srr": dma(()), "rrr": dma(()),
            "sd": dma((4,)), "rd": dma((4,)),
        }
        hbm = pl.BlockSpec(memory_space=pl.ANY)
        vmem = pl.BlockSpec(memory_space=pltpu.VMEM)
        far = pl.BlockSpec(memory_space=pltpu.HBM)
        new_one, new_two, dist = pl.pallas_call(
            functools.partial(kernel, nz, nx),
            out_shape=(
                jax.ShapeDtypeStruct((rows, width), BF16),
                jax.ShapeDtypeStruct((2 * nq, g, width), BF16),
                jax.ShapeDtypeStruct((1, LANES), F32),
            ),
            in_specs=[far, vmem, vmem, far, far],
            out_specs=(hbm, hbm, vmem),
            scratch_shapes=[v, sem],
            compiler_params=pltpu.CompilerParams(
                collective_id=0, has_side_effects=True, vmem_limit_bytes=53 * 1024 * 1024
            ),
        )(points, code_one.reshape(1, npts), code_two.reshape(1, npts), cent_one, cent_two)
        return new_one, new_two.reshape(rows, width), dist[0, :2]

    cents = P(("groups", "cb"), None)
    return jax.shard_map(
        local,
        mesh=mesh,
        in_specs=(P(("groups", "pts"), None), P(("groups", "pts")), P(("groups", "pts")), cents, cents),
        out_specs=(cents, cents, P("groups")),
        check_vma=False,
    )
```

```python
import functools

import jax
import jax.numpy as jnp
from jax import lax
from jax.experimental import pallas as pl
from jax.experimental.pallas import tpu as pltpu
from jax.sharding import PartitionSpec as P

MESH = pl.DeviceIdType.MESH
F32 = jnp.float32
BF16 = jnp.bfloat16
LANES = 128
HALF = 64
WIN = 4
NEAR = (-2, -1, 1)


TREE = (4, 3, -3, 1, -1, 2, -2)


def iota(shape, dim):
    return lax.broadcasted_iota(jnp.int32, shape, dim)


def kernel(nz, nx, pts, code1, code2, cent1, cent2, new1, new2, dist, v, sem):
    z = lax.axis_index("pts")
    cb = lax.axis_index("cb")
    x = cb // 2
    c = cb - 2 * x
    h = x - 2 * (x // 2)
    q = z // WIN
    cl = z - WIN * q
    par = cl - 2 * (cl // 2)
    e = cl // 2
    nq = nz // WIN
    s = 1 - 2 * c
    rows = cent1.shape[0]
    npts = pts.shape[0]
    chip = npts // nx
    g = 2 * rows // nz

    def qm(d):
        return lax.rem(q + d * s + 2 * nq, nq)

    def zq(d):
        return lax.rem(z + WIN * d * s + 2 * nz, nz)

    def zed(step):
        return lax.rem(z + step + nz, nz)

    def to_z(t):
        return {"pts": t}

    def to_x(t):
        return {"cb": 2 * t + c}

    sib = {"cb": 2 * x + 1 - c}

    def send(src, dst, ss, rs, where):
        pltpu.make_async_remote_copy(
            src_ref=src, dst_ref=dst, send_sem=ss, recv_sem=rs, device_id=where, device_id_type=MESH
        ).start()

    def wait(ref, sm):
        pltpu.make_async_copy(ref, ref, sm).wait()

    def xed(i):
        return lax.rem(x + i, nx)

    barrier = pltpu.get_barrier_semaphore()
    for step in (-2, -1, 1, 2):
        pl.semaphore_signal(barrier, inc=1, device_id=to_z(zed(step)), device_id_type=MESH)
    for o in range(1, nq):
        pl.semaphore_signal(barrier, inc=1, device_id=to_z(zed(WIN * o)), device_id_type=MESH)
    for i in range(1, nx):
        pl.semaphore_signal(barrier, inc=1, device_id=to_x(xed(i)), device_id_type=MESH)
    pl.semaphore_signal(barrier, inc=1, device_id=sib, device_id_type=MESH)

    tile_a = x + (x + 1) // 2
    tile_b = 1 + 3 * (x // 2)
    col_a = pl.ds(pl.multiple_of(tile_a * LANES, LANES), LANES)
    col_b = pl.ds(pl.multiple_of(tile_b * LANES, LANES), LANES)
    loads = [
        pltpu.make_async_copy(pts.at[:, col_a], v["P"].at[:, 0:LANES], sem["ld"].at[0]),
        pltpu.make_async_copy(pts.at[:, col_b], v["P"].at[:, LANES : 2 * LANES], sem["ld"].at[1]),
        pltpu.make_async_copy(cent1, v["C1"].at[x], sem["ld"].at[2]),
        pltpu.make_async_copy(cent2, v["C2"].at[x], sem["ld"].at[3]),
        pltpu.make_async_copy(pts.at[pl.ds(pl.multiple_of(x * chip, chip), chip), :], v["R1"], sem["ld"].at[4]),
    ]
    for ld in loads:
        ld.start()
    loads[0].wait()
    loads[1].wait()

    blk = 256
    hm_b = iota((blk, LANES), 1) // HALF == h
    hm_g = iota((g, LANES), 1) // HALF == h

    @pl.loop(0, npts // blk)
    def _(i):
        sl = pl.ds(pl.multiple_of(i * blk, blk), blk)
        v["W"][sl, 0:LANES] = v["P"][sl, 0:LANES]
        b = v["P"][sl, LANES : 2 * LANES].astype(F32)
        v["W"][sl, LANES : 2 * LANES] = jnp.where(hm_b, b, 1.0).astype(BF16)

    m16 = (iota((nq, g, LANES), 2) & (g - 1)) == iota((nq, g, LANES), 1)

    def class_of(i):
        t = zed(s * (i - 2 + (i // 2) * (5 - 2 * i)))
        return t, t // WIN, lax.rem(t, WIN)

    def class_sums(i, code, w, S, Sc):
        _, _, ct = class_of(i)
        pt = lax.rem(ct, 2)
        et = ct // 2
        n = 2 * nq * g
        r = iota((n, 1), 0)
        hl = r // (nq * g)
        rq = (r // g) & (nq - 1)
        lab = rows * (2 * (2 * pt + hl) + c) + g * (2 * rq + et) + (r & (g - 1))
        oh = jnp.where(lab == code[...], 1.0, 0.0).astype(BF16)
        out = jnp.dot(oh, w[...], preferred_element_type=F32)
        lo, hi = out[: nq * g], out[nq * g :]
        S[ct, :, 0:g, :] = lo[:, :LANES].reshape(nq, g, LANES)
        S[ct, :, g : 2 * g, :] = hi[:, :LANES].reshape(nq, g, LANES)
        lb = lo[:, LANES:]
        hb = pltpu.roll(hi[:, LANES:], HALF, 1)
        hm = iota(lb.shape, 1) // HALF == h
        S[ct, :, 2 * g :, :] = jnp.where(hm, lb, hb).reshape(nq, g, LANES)
        cnt = jnp.where(hm, hb, lb).reshape(nq, g, LANES)
        Sc[ct] = jnp.sum(jnp.where(m16, cnt, 0.0), axis=1, keepdims=True)

    def class_sends(i, S, Sc, X1, X1c, k):
        t, qt, ct = class_of(i)
        send(Sc.at[ct], X1c.at[i], sem["s1c"].at[k], sem["r1c"].at[k], to_z(t))
        for d in TREE + (0,):
            qd = lax.rem(qt + d * s + 2 * nq, nq)
            send(S.at[ct, qd], X1.at[i, qd], sem["s1"].at[k], sem["r1"].at[k, qd], to_z(t))

    def far_sums(S, Sc, X1, X1c, T, Tc, XM, X2, X2c, k):
        for d in TREE + (0,):
            qd = qm(d)
            wait(X1.at[:, 0], sem["r1"].at[k, qd])
            t = S[cl, qd] + X1[0, qd] + X1[1, qd] + X1[2, qd]
            if d == 2:
                wait(XM.at[0], sem["rm"].at[k, 0])
                wait(XM.at[1], sem["rm"].at[k, 1])
                t = t + XM[0] + XM[1]
            if d == -2:
                wait(XM.at[2], sem["rm"].at[k, 2])
                t = t + XM[2]
            T[qd] = t
            if d == 4:
                send(T.at[qd], XM.at[0], sem["s2"].at[k], sem["rm"].at[k, 0], to_z(zq(2)))
                wait(X1c, sem["r1c"].at[k])
                Tc[...] = Sc[cl] + X1c[0] + X1c[1] + X1c[2]
                for o in range(1, nq):
                    qo = lax.rem(q + o, nq)
                    send(Tc.at[qo], X2c.at[o - 1], sem["s2c"].at[k], sem["r2c"].at[k], to_z(zed(WIN * o)))
            elif d == 3:
                send(T.at[qd], XM.at[1], sem["s2"].at[k], sem["rm"].at[k, 1], to_z(zq(1)))
            elif d == -3:
                send(T.at[qd], XM.at[2], sem["s2"].at[k], sem["rm"].at[k, 2], to_z(zq(-1)))
            elif d != 0:
                at = (1, -1, 2, -2).index(d)
                send(T.at[qd], X2.at[at], sem["s2"].at[k], sem["r2"].at[k], to_z(zq(d)))

    def finish(T, Tc, X2, X2c, C, k):
        wait(X2c, sem["r2c"].at[k])
        cnt = Tc[q]
        for o in range(nq - 1):
            cnt = cnt + X2c[o]
        wait(X2, sem["r2"].at[k])
        tot = T[q] + X2[0] + X2[1] + X2[2] + X2[3]
        full = jnp.broadcast_to(cnt, (g, LANES))
        diag = (iota((g, LANES), 1) & (HALF - 1)) == iota((g, LANES), 0)
        lo_n = jnp.sum(jnp.where(diag & jnp.logical_not(hm_g), full, 0.0), axis=1, keepdims=True) + 1.0
        hi_n = jnp.sum(jnp.where(diag & hm_g, full, 0.0), axis=1, keepdims=True) + 1.0
        sl = pl.ds(pl.multiple_of(g * (z // 2), g), g)
        at_lo = 2 * par
        at_hi = 2 * par + 1
        a_lo = C[at_lo, sl, col_a].astype(F32)
        a_hi = C[at_hi, sl, col_a].astype(F32)
        b_lo = C[at_lo, sl, col_b].astype(F32)
        b_hi = pltpu.roll(C[at_hi, sl, col_b].astype(F32), HALF, 1)
        new_lo = ((tot[0:g] + a_lo) / lo_n).astype(BF16)
        new_hi = ((tot[g : 2 * g] + a_hi) / hi_n).astype(BF16)
        new_b = ((tot[2 * g :] + jnp.where(hm_g, b_lo, b_hi)) / jnp.where(hm_g, lo_n, hi_n)).astype(BF16)
        return new_lo, new_hi, new_b

    def cidx(t):
        ct = lax.rem(t, WIN)
        return 2 * lax.rem(ct, 2) + ct // 2

    def far_gather(at, k, near_sends):
        slots = (1, -1, 2, -2, 3, -3, 4)

        def far_send(ref, d, to):
            send(ref, ref, sem["sf"].at[k], sem["rf"].at[k, slots.index(d)], to_z(zq(to)))

        for d in slots[::-1]:
            far_send(at(q), d, d)
        near_sends(q)
        for d in slots:
            qs = qm(-d)
            wait(at(qs), sem["rf"].at[k, slots.index(d)])
            near_sends(qs)

    def gather(N):
        ci = 2 * par + e

        def near_sends(qs):
            for i in range(3):
                send(N.at[c, ci, qs], N.at[c, ci, qs], sem["sl"].at[0], sem["rl"].at[0, i], to_z(zed(s * NEAR[i])))

        far_gather(lambda qs: N.at[c, ci, qs], 0, near_sends)
        send(N.at[c, ci], N.at[c, ci], sem["st"].at[0], sem["rt"].at[0], sib)
        for i in (2, 1, 0):
            cs = cidx(zed(-s * NEAR[i]))
            wait(N.at[c, cs], sem["rl"].at[0, i])
            send(N.at[c, cs], N.at[c, cs], sem["st"].at[0], sem["rt"].at[0], sib)

    def gather_rows(O):
        def near_sends(qs):
            at = O.at[2 * qs + e]
            for i, step in enumerate((1, -1, 2 * s)):
                send(at, at, sem["sl"].at[1], sem["rl"].at[1, i], to_z(zed(step)))

        far_gather(lambda qs: O.at[2 * qs + e], 1, near_sends)

    def out_parts(N, t):
        pair = pl.ds(2 * (t // 2), 2)
        rs = pl.ds(pl.multiple_of(g * lax.rem(t, 2), g), g)
        return N.at[c, pair, :, rs, :], N.at[c, pair, :, pl.ds(2 * g, g), :]

    def out_sends(N, OA, OB):
        for i in range(1, nx):
            t = xed(i)
            a, b = out_parts(N, t)
            send(a, OA.at[x], sem["so"].at[0], sem["ro"].at[0], to_x(t))
            send(b, OB.at[x], sem["so"].at[1], sem["ro"].at[1], to_x(t))
        a, b = out_parts(N, x)
        pltpu.make_async_copy(a, OA.at[x], sem["lo"].at[0]).start()
        pltpu.make_async_copy(b, OB.at[x], sem["lo"].at[1]).start()

    left = iota((g, LANES), 1) < HALF

    def out_rows(OA, OB, out):
        wait(OA.at[0], sem["lo"].at[0])
        wait(OB.at[0], sem["lo"].at[1])
        wait(OA.at[pl.ds(0, nx - 1)], sem["ro"].at[0])
        wait(OB.at[pl.ds(0, nx - 1)], sem["ro"].at[1])
        for ee in range(2):
            for qq in range(nq):
                r0 = g * (2 * qq + ee)
                for xx in range(nx):
                    ta = xx + (xx + 1) // 2
                    out[r0 : r0 + g, ta * LANES : (ta + 1) * LANES] = OA[xx, ee, qq]
                for y in range(nx // 2):
                    two = []
                    for xx in (2 * y, 2 * y + 1):
                        b = OB[xx, ee, qq].astype(F32)
                        two.append(jnp.where(h == 1, pltpu.roll(b, HALF, 1), b))
                    tb = 1 + 3 * y
                    out[r0 : r0 + g, tb * LANES : (tb + 1) * LANES] = jnp.where(left, two[0], two[1]).astype(BF16)

    def nearest(C, R):
        def body(k, m):
            ck = C[k]
            cross = lax.dot_general(ck, R[...], (((1,), (1,)), ((), ())), preferred_element_type=F32)
            cf = ck.astype(F32)
            csq = jnp.sum(cf * cf, axis=1, keepdims=True)
            d = csq - 2.0 * cross
            return jnp.minimum(m, jnp.min(d.reshape(rows // 8, 8, chip), axis=0))

        m = lax.fori_loop(0, nx, body, jnp.full((8, chip), jnp.inf, F32))
        r = R[...].astype(F32)
        psq = jnp.sum(jnp.sum(r * r, axis=0, keepdims=True), axis=1, keepdims=True)
        return jnp.min(m, axis=0, keepdims=True), psq

    @pl.loop(0, WIN)
    def _(i):
        class_sums(i, code1, v["W"], v["S1"], v["Sc1"])

    loads[2].wait()
    loads[3].wait()
    loads[4].wait()
    pl.semaphore_wait(barrier, 4 + (nq - 1) + (nx - 1) + 1)

    for i in range(3):
        class_sends(i, v["S1"], v["Sc1"], v["X11"], v["X1c1"], 0)
    for k, C in enumerate((v["C1"], v["C2"])):
        for i in range(1, nx):
            send(C.at[x], C.at[x], sem["sc"].at[k], sem["rc"].at[k], to_x(xed(i)))

    for b in range(npts // LANES):
        row = code1[0:1, b * LANES : (b + 1) * LANES].astype(F32)
        v["CT"][b * LANES : (b + 1) * LANES, :] = jnp.transpose(jnp.broadcast_to(row, (LANES, LANES)))

    far_sums(v["S1"], v["Sc1"], v["X11"], v["X1c1"], v["T1"], v["Tc1"], v["XM1"], v["X21"], v["X2c1"], 0)
    wait(v["C1"].at[pl.ds(0, nx - 1)], sem["rc"].at[0])
    mins_one, psq_one = nearest(v["C1"], v["R1"])
    v["D0"][c, 0] = mins_one
    new_lo, new_hi, new_b = finish(v["T1"], v["Tc1"], v["X21"], v["X2c1"], v["C1"], 0)
    v["N1"][c, 2 * par + e, q, 0:g, :] = new_lo
    v["N1"][c, 2 * par + e, q, g : 2 * g, :] = new_hi
    v["N1"][c, 2 * par + e, q, 2 * g :, :] = new_b
    gather(v["N1"])
    out_sends(v["N1"], v["OA1"], v["OB1"])
    wait(v["N1"].at[0], sem["rt"].at[0])

    kb = nq * g
    for cc in range(2):
        for k in range(WIN):
            base = (cc * WIN + k) * 2 * kb
            n = v["N1"][cc, k]
            v["L"][base : base + kb, 0:LANES] = n[:, 0:g, :].reshape(kb, LANES)
            v["L"][base + kb : base + 2 * kb, 0:LANES] = n[:, g : 2 * g, :].reshape(kb, LANES)
            b = n[:, 2 * g :, :].reshape(kb, LANES)
            v["L"][base : base + kb, LANES : 2 * LANES] = b
            v["L"][base + kb : base + 2 * kb, LANES : 2 * LANES] = pltpu.roll(b.astype(F32), HALF, 1).astype(BF16)

    @pl.loop(0, npts // blk)
    def _(i):
        sl = pl.ds(pl.multiple_of(i * blk, blk), blk)
        codes = v["CT"][sl, :]
        parts = []
        lane = iota((1, LANES), 1)
        for j in range(2 * nx * rows // LANES):
            r = lane + j * LANES
            cc = r // (WIN * 2 * kb)
            k = (r // (2 * kb)) & (WIN - 1)
            hl = (r // kb) & 1
            rq = (r // g) & (nq - 1)
            lab = rows * (2 * (2 * (k // 2) + hl) + cc) + g * (2 * rq + (k & 1)) + (r & (g - 1))
            parts.append(jnp.where(codes == lab.astype(F32), 1.0, 0.0).astype(BF16))
        oh = jnp.concatenate(parts, axis=1)
        looked = jnp.dot(oh, v["L"][...], preferred_element_type=F32)
        res = v["P"][sl, :].astype(F32) - looked
        v["W2"][sl, 0:LANES] = res[:, 0:LANES].astype(BF16)
        v["W2"][sl, LANES : 2 * LANES] = jnp.where(hm_b, res[:, LANES:], 1.0).astype(BF16)

    @pl.loop(0, WIN)
    def _(i):
        class_sums(i, code2, v["W2"], v["S2"], v["Sc2"])

        @pl.when(i < 3)
        def _():
            class_sends(i, v["S2"], v["Sc2"], v["X12"], v["X1c2"], 1)

    for i in range(1, nx):
        t = xed(i)
        sl = pl.ds(pl.multiple_of(chip * t, chip), chip)
        send(v["W2"].at[sl, :], v["RR"].at[x], sem["srr"], sem["rrr"], to_x(t))
    sl = pl.ds(pl.multiple_of(chip * x, chip), chip)
    mine = pltpu.make_async_copy(v["W2"].at[sl, :], v["RR"].at[x], sem["ld"].at[5])
    mine.start()
    far_sums(v["S2"], v["Sc2"], v["X12"], v["X1c2"], v["T2"], v["Tc2"], v["XM2"], v["X22"], v["X2c2"], 1)
    out_rows(v["OA1"], v["OB1"], v["NW"])
    put_one = pltpu.make_async_copy(v["NW"], new1, sem["ld"].at[6])
    put_one.start()

    mine.wait()
    wait(v["RR"].at[pl.ds(0, nx - 1)], sem["rrr"])
    for xx in range(nx):
        ta = xx + (xx + 1) // 2
        v["R2"][:, ta * LANES : (ta + 1) * LANES] = v["RR"][xx, :, 0:LANES]
    left_own = iota((chip, LANES), 1) < HALF
    for y in range(nx // 2):
        tb = 1 + 3 * y
        v["R2"][:, tb * LANES : (tb + 1) * LANES] = jnp.where(
            left_own,
            v["RR"][2 * y, :, LANES:].astype(F32),
            v["RR"][2 * y + 1, :, LANES:].astype(F32),
        ).astype(BF16)
    wait(v["C2"].at[pl.ds(0, nx - 1)], sem["rc"].at[1])
    mins_two, psq_two = nearest(v["C2"], v["R2"])
    v["D0"][c, 1] = mins_two
    send(v["D0"].at[c], v["D0"].at[c], sem["sd"].at[0], sem["rd"].at[0], sib)
    wait(v["D0"].at[0], sem["rd"].at[0])
    lane = iota((1, LANES), 1)
    tot_one = jnp.sum(jnp.minimum(v["D0"][0, 0], v["D0"][1, 0]), axis=1, keepdims=True) + psq_one
    tot_two = jnp.sum(jnp.minimum(v["D0"][0, 1], v["D0"][1, 1]), axis=1, keepdims=True) + psq_two
    v["D1"][x] = jnp.where(lane == 0, tot_one, jnp.where(lane == 1, tot_two, 0.0))
    for i in range(1, nx):
        send(v["D1"].at[x], v["D1"].at[x], sem["sd"].at[1], sem["rd"].at[1], to_x(xed(i)))

    new_lo, new_hi, new_b = finish(v["T2"], v["Tc2"], v["X22"], v["X2c2"], v["C2"], 1)
    v["NC"][0:g, :] = new_lo
    v["NC"][g : 2 * g, :] = new_b
    v["NC"][2 * g :, :] = new_hi
    role = x // 2 == par
    for hl in range(2):
        t = 2 * par + hl
        src = v["NC"].at[pl.ds(g * hl, 2 * g), :]

        @pl.when(t != x)
        def _():
            send(src, v["Y"].at[x], sem["sy"], sem["ry"], to_x(t))

        @pl.when(t == x)
        def _():
            pltpu.make_async_copy(src, v["Y"].at[x], sem["ly"]).start()

    wait(v["D1"].at[pl.ds(0, nx - 1)], sem["rd"].at[1])
    tot = v["D1"][0]
    for i in range(1, nx):
        tot = tot + v["D1"][i]
    v["D2"][cl, q] = tot
    for o in range(1, nq):
        send(v["D2"].at[cl, q], v["D2"].at[cl, q], sem["sd"].at[2], sem["rd"].at[2], to_z(zed(WIN * o)))

    def pass_dist():
        wait(v["D2"].at[0, pl.ds(0, nq - 1)], sem["rd"].at[2])
        for i in range(3):
            send(v["D2"].at[cl], v["D2"].at[cl], sem["sd"].at[3], sem["rd"].at[3], to_z(zed(s * NEAR[i])))

    @pl.when(role)
    def _():
        wait(v["Y"].at[pl.ds(0, nx - 1)], sem["ry"])
        wait(v["Y"].at[0], sem["ly"])
        mine = 2 * q + e
        for y in range(nx // 2):
            two = []
            for xx in (2 * y, 2 * y + 1):
                top = v["Y"][xx, 0:g, :].astype(F32)
                low = v["Y"][xx, g : 2 * g, :].astype(F32)
                ta = xx + (xx + 1) // 2
                v["O"][mine, :, ta * LANES : (ta + 1) * LANES] = jnp.where(h == 1, low, top).astype(BF16)
                two.append(jnp.where(h == 1, pltpu.roll(top, HALF, 1), low))
            tb = 1 + 3 * y
            v["O"][mine, :, tb * LANES : (tb + 1) * LANES] = jnp.where(left, two[0], two[1]).astype(BF16)
        gather_rows(v["O"])
        pass_dist()
        wait(v["O"].at[pl.ds(0, nq)], sem["rl"].at[1, 2])

    @pl.when(jnp.logical_not(role))
    def _():
        pass_dist()
        wait(v["O"].at[pl.ds(0, nq)], sem["rl"].at[1, 0])
        wait(v["O"].at[pl.ds(0, nq)], sem["rl"].at[1, 1])

    put_two = pltpu.make_async_copy(v["O"], new2, sem["ld"].at[7])
    put_two.start()

    wait(v["D2"].at[pl.ds(0, 3)], sem["rd"].at[3])
    tot = v["D2"][0, 0]
    for i in range(1, nz):
        tot = tot + v["D2"][i // nq, i % nq]
    dist[...] = tot / jnp.float32(npts * nz * pts.shape[1])

    for k in range(2):
        wait(v["X11"], sem["s1"].at[k])
        wait(v["X1c1"], sem["s1c"].at[k])
        wait(v["X11"].at[0, pl.ds(0, nq - 1)], sem["s2"].at[k])
        wait(v["X2c1"], sem["s2c"].at[k])
        wait(v["C1"].at[pl.ds(0, nx - 1)], sem["sc"].at[k])
    wait(v["N1"].at[0, 0, pl.ds(0, nq - 1)], sem["sf"].at[0])
    wait(v["N1"].at[0, pl.ds(0, 3)], sem["sl"].at[0])
    wait(v["OA1"].at[pl.ds(0, nx - 1)], sem["so"].at[0])
    wait(v["OB1"].at[pl.ds(0, nx - 1)], sem["so"].at[1])
    wait(v["N1"].at[0], sem["st"].at[0])
    wait(v["RR"].at[pl.ds(0, nx - 1)], sem["srr"])
    wait(v["D0"].at[0], sem["sd"].at[0])
    wait(v["D1"].at[pl.ds(0, nx - 1)], sem["sd"].at[1])
    wait(v["D2"].at[0, pl.ds(0, nq - 1)], sem["sd"].at[2])
    wait(v["D2"].at[pl.ds(0, 3)], sem["sd"].at[3])

    @pl.when(role)
    def _():
        wait(v["O"].at[pl.ds(0, nq - 1)], sem["sf"].at[1])
        wait(v["X11"], sem["sl"].at[1])
        wait(v["Y"].at[0], sem["sy"])

    @pl.when(jnp.logical_not(role))
    def _():
        wait(v["Y"].at[pl.ds(0, 2)], sem["sy"])

    put_one.wait()
    put_two.wait()


def solution(mesh):
    nz = mesh.shape["pts"]
    nx = mesh.shape["cb"] // 2
    nq = nz // WIN

    def local(points, code_one, code_two, cent_one, cent_two):
        npts, width = points.shape
        rows = cent_one.shape[0]
        chip = npts // nx
        g = 2 * rows // nz
        ch = 3 * g
        vm = pltpu.VMEM
        v = {
            "P": vm((npts, 2 * LANES), BF16),
            "W": vm((npts, 2 * LANES), BF16),
            "W2": vm((npts, 2 * LANES), BF16),
            "CT": vm((npts, LANES), F32),
            "L": vm((2 * nx * rows, 2 * LANES), BF16),
            "R1": vm((chip, width), BF16),
            "R2": vm((chip, width), BF16),
            "RR": vm((nx, chip, 2 * LANES), BF16),
            "D0": vm((2, 2, 1, chip), F32),
            "D1": vm((nx, 1, LANES), F32),
            "D2": vm((WIN, nq, 1, LANES), F32),
        }
        v["N1"] = vm((2, WIN, nq, ch, LANES), BF16)
        v["OA1"] = vm((nx, 2, nq, g, LANES), BF16)
        v["OB1"] = vm((nx, 2, nq, g, LANES), BF16)
        v["NW"] = vm((rows, width), BF16)
        v["NC"] = vm((ch, LANES), BF16)
        v["Y"] = vm((nx, 2 * g, LANES), BF16)
        v["O"] = vm((2 * nq, g, width), BF16)
        for k in ("1", "2"):
            v["C" + k] = vm((nx, rows, width), BF16)
            v["S" + k] = vm((WIN, nq, ch, LANES), F32)
            v["Sc" + k] = vm((WIN, nq, 1, LANES), F32)
            v["X1" + k] = vm((3, nq, ch, LANES), F32)
            v["X1c" + k] = vm((3, nq, 1, LANES), F32)
            v["T" + k] = vm((nq, ch, LANES), F32)
            v["Tc" + k] = vm((nq, 1, LANES), F32)
            v["XM" + k] = vm((3, ch, LANES), F32)
            v["X2" + k] = vm((4, ch, LANES), F32)
            v["X2c" + k] = vm((nq - 1, 1, LANES), F32)
        dma = pltpu.SemaphoreType.DMA
        sem = {
            "ld": dma((8,)),
            "s1": dma((2,)), "r1": dma((2, nq)), "s1c": dma((2,)), "r1c": dma((2,)),
            "rm": dma((2, 3)), "s2": dma((2,)), "r2": dma((2,)), "s2c": dma((2,)), "r2c": dma((2,)),
            "sf": dma((2,)), "rf": dma((2, nq - 1)), "sl": dma((2,)), "rl": dma((2, 3)),
            "st": dma((1,)), "rt": dma((1,)),
            "so": dma((2,)), "ro": dma((2,)), "lo": dma((2,)),
            "sy": dma(()), "ry": dma(()), "ly": dma(()),
            "sc": dma((2,)), "rc": dma((2,)),
            "srr": dma(()), "rrr": dma(()),
            "sd": dma((4,)), "rd": dma((4,)),
        }
        hbm = pl.BlockSpec(memory_space=pl.ANY)
        vmem = pl.BlockSpec(memory_space=pltpu.VMEM)
        far = pl.BlockSpec(memory_space=pltpu.HBM)
        new_one, new_two, dist = pl.pallas_call(
            functools.partial(kernel, nz, nx),
            out_shape=(
                jax.ShapeDtypeStruct((rows, width), BF16),
                jax.ShapeDtypeStruct((2 * nq, g, width), BF16),
                jax.ShapeDtypeStruct((1, LANES), F32),
            ),
            in_specs=[far, vmem, vmem, far, far],
            out_specs=(hbm, hbm, vmem),
            scratch_shapes=[v, sem],
            compiler_params=pltpu.CompilerParams(
                collective_id=0, has_side_effects=True, vmem_limit_bytes=53 * 1024 * 1024
            ),
        )(points, code_one.reshape(1, npts), code_two.reshape(1, npts), cent_one, cent_two)
        return new_one, new_two.reshape(rows, width), dist[0, :2]

    cents = P(("groups", "cb"), None)
    return jax.shard_map(
        local,
        mesh=mesh,
        in_specs=(P(("groups", "pts"), None), P(("groups", "pts")), P(("groups", "pts")), cents, cents),
        out_specs=(cents, cents, P("groups")),
        check_vma=False,
    )
```

```python
import functools

import jax
import jax.numpy as jnp
from jax import lax
from jax.experimental import pallas as pl
from jax.experimental.pallas import tpu as pltpu
from jax.sharding import PartitionSpec as P

MESH = pl.DeviceIdType.MESH
F32 = jnp.float32
BF16 = jnp.bfloat16
LANES = 128
HALF = 64
WIN = 4
NEAR = (-2, -1, 1)


TREE = (4, 3, -3, 2, -2, 1, -1)


def iota(shape, dim):
    return lax.broadcasted_iota(jnp.int32, shape, dim)


def kernel(nz, nx, pts, code1, code2, cent1, cent2, new1, new2, dist, v, sem):
    z = lax.axis_index("pts")
    cb = lax.axis_index("cb")
    x = cb // 2
    c = cb - 2 * x
    h = x - 2 * (x // 2)
    q = z // WIN
    cl = z - WIN * q
    par = cl - 2 * (cl // 2)
    e = cl // 2
    nq = nz // WIN
    s = 1 - 2 * c
    rows = cent1.shape[0]
    npts = pts.shape[0]
    chip = npts // nx
    g = 2 * rows // nz

    def qm(d):
        return lax.rem(q + d * s + 2 * nq, nq)

    def zq(d):
        return lax.rem(z + WIN * d * s + 2 * nz, nz)

    def zed(step):
        return lax.rem(z + step + nz, nz)

    def to_z(t):
        return {"pts": t}

    def to_x(t):
        return {"cb": 2 * t + c}

    sib = {"cb": 2 * x + 1 - c}

    def send(src, dst, ss, rs, where):
        pltpu.make_async_remote_copy(
            src_ref=src, dst_ref=dst, send_sem=ss, recv_sem=rs, device_id=where, device_id_type=MESH
        ).start()

    def wait(ref, sm):
        pltpu.make_async_copy(ref, ref, sm).wait()

    def xed(i):
        return lax.rem(x + i, nx)

    barrier = pltpu.get_barrier_semaphore()
    for step in (-2, -1, 1, 2):
        pl.semaphore_signal(barrier, inc=1, device_id=to_z(zed(step)), device_id_type=MESH)
    for i in range(1, nx):
        pl.semaphore_signal(barrier, inc=1, device_id=to_x(xed(i)), device_id_type=MESH)
    pl.semaphore_signal(barrier, inc=1, device_id=sib, device_id_type=MESH)

    tile_a = x + (x + 1) // 2
    tile_b = 1 + 3 * (x // 2)
    col_a = pl.ds(pl.multiple_of(tile_a * LANES, LANES), LANES)
    col_b = pl.ds(pl.multiple_of(tile_b * LANES, LANES), LANES)
    loads = [
        pltpu.make_async_copy(pts.at[:, col_a], v["P"].at[:, 0:LANES], sem["ld"].at[0]),
        pltpu.make_async_copy(pts.at[:, col_b], v["P"].at[:, LANES : 2 * LANES], sem["ld"].at[1]),
        pltpu.make_async_copy(cent1, v["C1"].at[x], sem["ld"].at[2]),
        pltpu.make_async_copy(cent2, v["C2"].at[x], sem["ld"].at[3]),
        pltpu.make_async_copy(pts.at[pl.ds(pl.multiple_of(x * chip, chip), chip), :], v["R1"], sem["ld"].at[4]),
    ]
    for ld in loads:
        ld.start()
    loads[0].wait()
    loads[1].wait()

    blk = 256
    hm_b = iota((blk, LANES), 1) // HALF == h
    hm_g = iota((g, LANES), 1) // HALF == h

    @pl.loop(0, npts // blk)
    def _(i):
        sl = pl.ds(pl.multiple_of(i * blk, blk), blk)
        v["W"][sl, 0:LANES] = v["P"][sl, 0:LANES]
        b = v["P"][sl, LANES : 2 * LANES].astype(F32)
        v["W"][sl, LANES : 2 * LANES] = jnp.where(hm_b, b, 1.0).astype(BF16)

    m16 = (iota((nq, g, LANES), 2) & (g - 1)) == iota((nq, g, LANES), 1)

    def class_of(i):
        t = zed(s * (i - 2 + (i // 2) * (5 - 2 * i)))
        return t, t // WIN, lax.rem(t, WIN)

    def class_sums(i, code, w, S, Sc):
        _, _, ct = class_of(i)
        pt = lax.rem(ct, 2)
        et = ct // 2
        n = 2 * nq * g
        r = iota((n, 1), 0)
        hl = r // (nq * g)
        rq = (r // g) & (nq - 1)
        lab = rows * (2 * (2 * pt + hl) + c) + g * (2 * rq + et) + (r & (g - 1))
        oh = jnp.where(lab == code[...], 1.0, 0.0).astype(BF16)
        out = jnp.dot(oh, w[...], preferred_element_type=F32)
        lo, hi = out[: nq * g], out[nq * g :]
        S[ct, :, 0:g, :] = lo[:, :LANES].reshape(nq, g, LANES)
        S[ct, :, g : 2 * g, :] = hi[:, :LANES].reshape(nq, g, LANES)
        lb = lo[:, LANES:]
        hb = pltpu.roll(hi[:, LANES:], HALF, 1)
        hm = iota(lb.shape, 1) // HALF == h
        S[ct, :, 2 * g :, :] = jnp.where(hm, lb, hb).reshape(nq, g, LANES)
        cnt = jnp.where(hm, hb, lb).reshape(nq, g, LANES)
        Sc[ct] = jnp.sum(jnp.where(m16, cnt, 0.0), axis=1, keepdims=True)

    def class_sends(i, S, Sc, X1, X1c, k):
        t, qt, ct = class_of(i)
        send(Sc.at[ct], X1c.at[i], sem["s1c"].at[k], sem["r1c"].at[k], to_z(t))
        for d in TREE + (0,):
            qd = lax.rem(qt + d * s + 2 * nq, nq)
            send(S.at[ct, qd], X1.at[i, qd], sem["s1"].at[k], sem["r1"].at[k, qd], to_z(t))

    def far_sums(S, Sc, X1, X1c, T, Tc, XM, XMc, X2, X2c, k):
        wait(X1c, sem["r1c"].at[k])
        for d in TREE + (0,):
            qd = qm(d)
            wait(X1.at[:, 0], sem["r1"].at[k, qd])
            t = S[cl, qd] + X1[0, qd] + X1[1, qd] + X1[2, qd]
            n = Sc[cl, qd] + X1c[0, qd] + X1c[1, qd] + X1c[2, qd]
            for m in {2: (0, 1), -2: (2,)}.get(d, ()):
                wait(XM.at[m], sem["rm"].at[k, m])
                wait(XMc.at[m], sem["rmc"].at[k, m])
                t = t + XM[m]
                n = n + XMc[m]
            T[qd] = t
            Tc[qd] = n
            if d in (4, 3, -3):
                m = (4, 3, -3).index(d)
                to = to_z(zq((2, 1, -1)[m]))
                send(T.at[qd], XM.at[m], sem["s2"].at[k], sem["rm"].at[k, m], to)
                send(Tc.at[qd], XMc.at[m], sem["s2c"].at[k], sem["rmc"].at[k, m], to)
            elif d != 0:
                m = (1, -1, 2, -2).index(d)
                send(T.at[qd], X2.at[m], sem["s2"].at[k], sem["r2"].at[k], to_z(zq(d)))
                send(Tc.at[qd], X2c.at[m], sem["s2c"].at[k], sem["r2c"].at[k], to_z(zq(d)))

    def finish(T, Tc, X2, X2c, C, k):
        wait(X2c, sem["r2c"].at[k])
        cnt = Tc[q] + X2c[0] + X2c[1] + X2c[2] + X2c[3]
        wait(X2, sem["r2"].at[k])
        tot = T[q] + X2[0] + X2[1] + X2[2] + X2[3]
        full = jnp.broadcast_to(cnt, (g, LANES))
        diag = (iota((g, LANES), 1) & (HALF - 1)) == iota((g, LANES), 0)
        lo_n = jnp.sum(jnp.where(diag & jnp.logical_not(hm_g), full, 0.0), axis=1, keepdims=True) + 1.0
        hi_n = jnp.sum(jnp.where(diag & hm_g, full, 0.0), axis=1, keepdims=True) + 1.0
        sl = pl.ds(pl.multiple_of(g * (z // 2), g), g)
        at_lo = 2 * par
        at_hi = 2 * par + 1
        a_lo = C[at_lo, sl, col_a].astype(F32)
        a_hi = C[at_hi, sl, col_a].astype(F32)
        b_lo = C[at_lo, sl, col_b].astype(F32)
        b_hi = pltpu.roll(C[at_hi, sl, col_b].astype(F32), HALF, 1)
        new_lo = ((tot[0:g] + a_lo) / lo_n).astype(BF16)
        new_hi = ((tot[g : 2 * g] + a_hi) / hi_n).astype(BF16)
        new_b = ((tot[2 * g :] + jnp.where(hm_g, b_lo, b_hi)) / jnp.where(hm_g, lo_n, hi_n)).astype(BF16)
        return new_lo, new_hi, new_b

    def cidx(t):
        ct = lax.rem(t, WIN)
        return 2 * lax.rem(ct, 2) + ct // 2

    def far_gather(at, k, near_sends):
        slots = (1, -1, 2, -2, 3, -3, 4)

        def far_send(ref, d, to):
            send(ref, ref, sem["sf"].at[k], sem["rf"].at[k, slots.index(d)], to_z(zq(to)))

        for d in slots[5::-1]:
            far_send(at(q), d, d)
        near_sends(q)
        for d in slots:
            qs = qm(-d)
            wait(at(qs), sem["rf"].at[k, slots.index(d)])
            if d == 2:
                far_send(at(qs), 4, 2)
            near_sends(qs)

    def gather(N):
        ci = 2 * par + e

        def near_sends(qs):
            for i in range(3):
                send(N.at[c, ci, qs], N.at[c, ci, qs], sem["sl"].at[0], sem["rl"].at[0, i], to_z(zed(s * NEAR[i])))

        far_gather(lambda qs: N.at[c, ci, qs], 0, near_sends)
        send(N.at[c, ci], N.at[c, ci], sem["st"].at[0], sem["rt"].at[0], sib)
        for i in (2, 1, 0):
            cs = cidx(zed(-s * NEAR[i]))
            wait(N.at[c, cs], sem["rl"].at[0, i])
            send(N.at[c, cs], N.at[c, cs], sem["st"].at[0], sem["rt"].at[0], sib)

    def gather_rows(O):
        def near_sends(qs):
            at = O.at[2 * qs + e]
            for i, step in enumerate((1, -1, 2 * s)):
                send(at, at, sem["sl"].at[1], sem["rl"].at[1, i], to_z(zed(step)))

        far_gather(lambda qs: O.at[2 * qs + e], 1, near_sends)

    def out_parts(N, t):
        pair = pl.ds(2 * (t // 2), 2)
        rs = pl.ds(pl.multiple_of(g * lax.rem(t, 2), g), g)
        return N.at[c, pair, :, rs, :], N.at[c, pair, :, pl.ds(2 * g, g), :]

    def out_sends(N, OA, OB):
        for i in range(1, nx):
            t = xed(i)
            a, b = out_parts(N, t)
            send(a, OA.at[x], sem["so"].at[0], sem["ro"].at[0], to_x(t))
            send(b, OB.at[x], sem["so"].at[1], sem["ro"].at[1], to_x(t))
        a, b = out_parts(N, x)
        pltpu.make_async_copy(a, OA.at[x], sem["lo"].at[0]).start()
        pltpu.make_async_copy(b, OB.at[x], sem["lo"].at[1]).start()

    left = iota((g, LANES), 1) < HALF

    def out_rows(OA, OB, out):
        wait(OA.at[0], sem["lo"].at[0])
        wait(OB.at[0], sem["lo"].at[1])
        wait(OA.at[pl.ds(0, nx - 1)], sem["ro"].at[0])
        wait(OB.at[pl.ds(0, nx - 1)], sem["ro"].at[1])
        for ee in range(2):
            for qq in range(nq):
                r0 = g * (2 * qq + ee)
                for xx in range(nx):
                    ta = xx + (xx + 1) // 2
                    out[r0 : r0 + g, ta * LANES : (ta + 1) * LANES] = OA[xx, ee, qq]
                for y in range(nx // 2):
                    two = []
                    for xx in (2 * y, 2 * y + 1):
                        b = OB[xx, ee, qq].astype(F32)
                        two.append(jnp.where(h == 1, pltpu.roll(b, HALF, 1), b))
                    tb = 1 + 3 * y
                    out[r0 : r0 + g, tb * LANES : (tb + 1) * LANES] = jnp.where(left, two[0], two[1]).astype(BF16)

    def nearest(C, R):
        def body(k, m):
            ck = C[k]
            cross = lax.dot_general(ck, R[...], (((1,), (1,)), ((), ())), preferred_element_type=F32)
            cf = ck.astype(F32)
            csq = jnp.sum(cf * cf, axis=1, keepdims=True)
            d = csq - 2.0 * cross
            return jnp.minimum(m, jnp.min(d.reshape(rows // 8, 8, chip), axis=0))

        m = lax.fori_loop(0, nx, body, jnp.full((8, chip), jnp.inf, F32))
        r = R[...].astype(F32)
        psq = jnp.sum(jnp.sum(r * r, axis=0, keepdims=True), axis=1, keepdims=True)
        return jnp.min(m, axis=0, keepdims=True), psq

    @pl.loop(0, WIN)
    def _(i):
        class_sums(i, code1, v["W"], v["S1"], v["Sc1"])

    loads[2].wait()
    loads[3].wait()
    loads[4].wait()
    pl.semaphore_wait(barrier, 4 + (nx - 1) + 1)

    def tell(k, step):
        pl.semaphore_signal(sem["lv"].at[k, 0], inc=1, device_id=to_z(zed(-step)), device_id_type=MESH)
        pl.semaphore_signal(sem["lv"].at[k, 1], inc=1, device_id=to_z(zed(step)), device_id_type=MESH)

    def told(k):
        pl.semaphore_wait(sem["lv"].at[k, 0], 1)
        pl.semaphore_wait(sem["lv"].at[k, 1], 1)

    tell(0, 2)

    for i in range(3):
        class_sends(i, v["S1"], v["Sc1"], v["X11"], v["X1c1"], 0)
    def cent_sends(C, k):
        for i in range(1, nx):
            send(C.at[x], C.at[x], sem["sc"].at[k], sem["rc"].at[k], to_x(xed(i)))

    cent_sends(v["C1"], 0)

    for b in range(npts // LANES):
        row = code1[0:1, b * LANES : (b + 1) * LANES].astype(F32)
        v["CT"][b * LANES : (b + 1) * LANES, :] = jnp.transpose(jnp.broadcast_to(row, (LANES, LANES)))

    told(0)
    tell(1, WIN)
    told(1)
    tell(2, 2 * WIN)
    far_sums(v["S1"], v["Sc1"], v["X11"], v["X1c1"], v["T1"], v["Tc1"], v["XM1"], v["XMc1"], v["X21"], v["X2c1"], 0)
    cent_sends(v["C2"], 1)
    wait(v["C1"].at[pl.ds(0, nx - 1)], sem["rc"].at[0])
    mins_one, psq_one = nearest(v["C1"], v["R1"])
    v["D0"][c, 0] = mins_one
    new_lo, new_hi, new_b = finish(v["T1"], v["Tc1"], v["X21"], v["X2c1"], v["C1"], 0)
    v["N1"][c, 2 * par + e, q, 0:g, :] = new_lo
    v["N1"][c, 2 * par + e, q, g : 2 * g, :] = new_hi
    v["N1"][c, 2 * par + e, q, 2 * g :, :] = new_b
    told(2)
    gather(v["N1"])
    wait(v["N1"].at[0], sem["rt"].at[0])

    kb = nq * g
    for cc in range(2):
        for k in range(WIN):
            base = (cc * WIN + k) * 2 * kb
            n = v["N1"][cc, k]
            v["L"][base : base + kb, 0:LANES] = n[:, 0:g, :].reshape(kb, LANES)
            v["L"][base + kb : base + 2 * kb, 0:LANES] = n[:, g : 2 * g, :].reshape(kb, LANES)
            b = n[:, 2 * g :, :].reshape(kb, LANES)
            v["L"][base : base + kb, LANES : 2 * LANES] = b
            v["L"][base + kb : base + 2 * kb, LANES : 2 * LANES] = pltpu.roll(b.astype(F32), HALF, 1).astype(BF16)

    @pl.loop(0, npts // blk)
    def _(i):
        sl = pl.ds(pl.multiple_of(i * blk, blk), blk)
        codes = v["CT"][sl, :]
        parts = []
        lane = iota((1, LANES), 1)
        for j in range(2 * nx * rows // LANES):
            r = lane + j * LANES
            cc = r // (WIN * 2 * kb)
            k = (r // (2 * kb)) & (WIN - 1)
            hl = (r // kb) & 1
            rq = (r // g) & (nq - 1)
            lab = rows * (2 * (2 * (k // 2) + hl) + cc) + g * (2 * rq + (k & 1)) + (r & (g - 1))
            parts.append(jnp.where(codes == lab.astype(F32), 1.0, 0.0).astype(BF16))
        oh = jnp.concatenate(parts, axis=1)
        looked = jnp.dot(oh, v["L"][...], preferred_element_type=F32)
        res = v["P"][sl, :].astype(F32) - looked
        v["W2"][sl, 0:LANES] = res[:, 0:LANES].astype(BF16)
        v["W2"][sl, LANES : 2 * LANES] = jnp.where(hm_b, res[:, LANES:], 1.0).astype(BF16)

    @pl.loop(0, WIN)
    def _(i):
        class_sums(i, code2, v["W2"], v["S2"], v["Sc2"])

        @pl.when(i < 3)
        def _():
            class_sends(i, v["S2"], v["Sc2"], v["X12"], v["X1c2"], 1)

    for i in range(1, nx):
        t = xed(i)
        sl = pl.ds(pl.multiple_of(chip * t, chip), chip)
        send(v["W2"].at[sl, :], v["RR"].at[x], sem["srr"], sem["rrr"], to_x(t))
    sl = pl.ds(pl.multiple_of(chip * x, chip), chip)
    mine = pltpu.make_async_copy(v["W2"].at[sl, :], v["RR"].at[x], sem["ld"].at[5])
    mine.start()
    far_sums(v["S2"], v["Sc2"], v["X12"], v["X1c2"], v["T2"], v["Tc2"], v["XM2"], v["XMc2"], v["X22"], v["X2c2"], 1)
    out_sends(v["N1"], v["OA1"], v["OB1"])

    mine.wait()
    wait(v["RR"].at[pl.ds(0, nx - 1)], sem["rrr"])
    for xx in range(nx):
        ta = xx + (xx + 1) // 2
        v["R2"][:, ta * LANES : (ta + 1) * LANES] = v["RR"][xx, :, 0:LANES]
    left_own = iota((chip, LANES), 1) < HALF
    for y in range(nx // 2):
        tb = 1 + 3 * y
        v["R2"][:, tb * LANES : (tb + 1) * LANES] = jnp.where(
            left_own,
            v["RR"][2 * y, :, LANES:].astype(F32),
            v["RR"][2 * y + 1, :, LANES:].astype(F32),
        ).astype(BF16)
    wait(v["C2"].at[pl.ds(0, nx - 1)], sem["rc"].at[1])
    mins_two, psq_two = nearest(v["C2"], v["R2"])
    v["D0"][c, 1] = mins_two
    send(v["D0"].at[c], v["D0"].at[c], sem["sd"].at[0], sem["rd"].at[0], sib)
    wait(v["D0"].at[0], sem["rd"].at[0])
    lane = iota((1, LANES), 1)
    tot_one = jnp.sum(jnp.minimum(v["D0"][0, 0], v["D0"][1, 0]), axis=1, keepdims=True) + psq_one
    tot_two = jnp.sum(jnp.minimum(v["D0"][0, 1], v["D0"][1, 1]), axis=1, keepdims=True) + psq_two
    v["D1"][x] = jnp.where(lane == 0, tot_one, jnp.where(lane == 1, tot_two, 0.0))
    for i in range(1, nx):
        send(v["D1"].at[x], v["D1"].at[x], sem["sd"].at[1], sem["rd"].at[1], to_x(xed(i)))

    new_lo, new_hi, new_b = finish(v["T2"], v["Tc2"], v["X22"], v["X2c2"], v["C2"], 1)
    v["NC"][0:g, :] = new_lo
    v["NC"][g : 2 * g, :] = new_b
    v["NC"][2 * g :, :] = new_hi
    role = x // 2 == par
    for hl in range(2):
        t = 2 * par + hl
        src = v["NC"].at[pl.ds(g * hl, 2 * g), :]

        @pl.when(t != x)
        def _():
            send(src, v["Y"].at[x], sem["sy"], sem["ry"], to_x(t))

        @pl.when(t == x)
        def _():
            pltpu.make_async_copy(src, v["Y"].at[x], sem["ly"]).start()

    wait(v["D1"].at[pl.ds(0, nx - 1)], sem["rd"].at[1])
    tot = v["D1"][0]
    for i in range(1, nx):
        tot = tot + v["D1"][i]
    v["D2"][cl, q] = tot
    for o in range(1, nq):
        send(v["D2"].at[cl, q], v["D2"].at[cl, q], sem["sd"].at[2], sem["rd"].at[2], to_z(zed(WIN * o)))

    out_rows(v["OA1"], v["OB1"], v["NW"])
    put_one = pltpu.make_async_copy(v["NW"], new1, sem["ld"].at[6])
    put_one.start()

    def pass_dist():
        wait(v["D2"].at[0, pl.ds(0, nq - 1)], sem["rd"].at[2])
        for i in range(3):
            send(v["D2"].at[cl], v["D2"].at[cl], sem["sd"].at[3], sem["rd"].at[3], to_z(zed(s * NEAR[i])))

    @pl.when(role)
    def _():
        wait(v["Y"].at[pl.ds(0, nx - 1)], sem["ry"])
        wait(v["Y"].at[0], sem["ly"])
        mine = 2 * q + e
        for y in range(nx // 2):
            two = []
            for xx in (2 * y, 2 * y + 1):
                top = v["Y"][xx, 0:g, :].astype(F32)
                low = v["Y"][xx, g : 2 * g, :].astype(F32)
                ta = xx + (xx + 1) // 2
                v["O"][mine, :, ta * LANES : (ta + 1) * LANES] = jnp.where(h == 1, low, top).astype(BF16)
                two.append(jnp.where(h == 1, pltpu.roll(top, HALF, 1), low))
            tb = 1 + 3 * y
            v["O"][mine, :, tb * LANES : (tb + 1) * LANES] = jnp.where(left, two[0], two[1]).astype(BF16)
        gather_rows(v["O"])
        pass_dist()
        wait(v["O"].at[pl.ds(0, nq)], sem["rl"].at[1, 2])

    @pl.when(jnp.logical_not(role))
    def _():
        pass_dist()
        wait(v["O"].at[pl.ds(0, nq)], sem["rl"].at[1, 0])
        wait(v["O"].at[pl.ds(0, nq)], sem["rl"].at[1, 1])

    put_two = pltpu.make_async_copy(v["O"], new2, sem["ld"].at[7])
    put_two.start()

    wait(v["D2"].at[pl.ds(0, 3)], sem["rd"].at[3])
    tot = v["D2"][0, 0]
    for i in range(1, nz):
        tot = tot + v["D2"][i // nq, i % nq]
    dist[...] = tot / jnp.float32(npts * nz * pts.shape[1])

    for k in range(2):
        wait(v["X11"], sem["s1"].at[k])
        wait(v["X1c1"], sem["s1c"].at[k])
        wait(v["X11"].at[0, pl.ds(0, nq - 1)], sem["s2"].at[k])
        wait(v["X1c1"].at[0, pl.ds(0, nq - 1)], sem["s2c"].at[k])
        wait(v["C1"].at[pl.ds(0, nx - 1)], sem["sc"].at[k])
    wait(v["N1"].at[0, 0, pl.ds(0, nq - 1)], sem["sf"].at[0])
    wait(v["N1"].at[0, pl.ds(0, 3)], sem["sl"].at[0])
    wait(v["OA1"].at[pl.ds(0, nx - 1)], sem["so"].at[0])
    wait(v["OB1"].at[pl.ds(0, nx - 1)], sem["so"].at[1])
    wait(v["N1"].at[0], sem["st"].at[0])
    wait(v["RR"].at[pl.ds(0, nx - 1)], sem["srr"])
    wait(v["D0"].at[0], sem["sd"].at[0])
    wait(v["D1"].at[pl.ds(0, nx - 1)], sem["sd"].at[1])
    wait(v["D2"].at[0, pl.ds(0, nq - 1)], sem["sd"].at[2])
    wait(v["D2"].at[pl.ds(0, 3)], sem["sd"].at[3])

    @pl.when(role)
    def _():
        wait(v["O"].at[pl.ds(0, nq - 1)], sem["sf"].at[1])
        wait(v["X11"], sem["sl"].at[1])
        wait(v["Y"].at[0], sem["sy"])

    @pl.when(jnp.logical_not(role))
    def _():
        wait(v["Y"].at[pl.ds(0, 2)], sem["sy"])

    put_one.wait()
    put_two.wait()


def solution(mesh):
    nz = mesh.shape["pts"]
    nx = mesh.shape["cb"] // 2
    nq = nz // WIN

    def local(points, code_one, code_two, cent_one, cent_two):
        npts, width = points.shape
        rows = cent_one.shape[0]
        chip = npts // nx
        g = 2 * rows // nz
        ch = 3 * g
        vm = pltpu.VMEM
        v = {
            "P": vm((npts, 2 * LANES), BF16),
            "W": vm((npts, 2 * LANES), BF16),
            "W2": vm((npts, 2 * LANES), BF16),
            "CT": vm((npts, LANES), F32),
            "L": vm((2 * nx * rows, 2 * LANES), BF16),
            "R1": vm((chip, width), BF16),
            "R2": vm((chip, width), BF16),
            "RR": vm((nx, chip, 2 * LANES), BF16),
            "D0": vm((2, 2, 1, chip), F32),
            "D1": vm((nx, 1, LANES), F32),
            "D2": vm((WIN, nq, 1, LANES), F32),
        }
        v["N1"] = vm((2, WIN, nq, ch, LANES), BF16)
        v["OA1"] = vm((nx, 2, nq, g, LANES), BF16)
        v["OB1"] = vm((nx, 2, nq, g, LANES), BF16)
        v["NW"] = vm((rows, width), BF16)
        v["NC"] = vm((ch, LANES), BF16)
        v["Y"] = vm((nx, 2 * g, LANES), BF16)
        v["O"] = vm((2 * nq, g, width), BF16)
        for k in ("1", "2"):
            v["C" + k] = vm((nx, rows, width), BF16)
            v["S" + k] = vm((WIN, nq, ch, LANES), F32)
            v["Sc" + k] = vm((WIN, nq, 1, LANES), F32)
            v["X1" + k] = vm((3, nq, ch, LANES), F32)
            v["X1c" + k] = vm((3, nq, 1, LANES), F32)
            v["T" + k] = vm((nq, ch, LANES), F32)
            v["Tc" + k] = vm((nq, 1, LANES), F32)
            v["XM" + k] = vm((3, ch, LANES), F32)
            v["X2" + k] = vm((4, ch, LANES), F32)
            v["X2c" + k] = vm((4, 1, LANES), F32)
            v["XMc" + k] = vm((3, 1, LANES), F32)
        dma = pltpu.SemaphoreType.DMA
        sem = {
            "ld": dma((8,)),
            "s1": dma((2,)), "r1": dma((2, nq)), "s1c": dma((2,)), "r1c": dma((2,)),
            "rm": dma((2, 3)), "rmc": dma((2, 3)), "lv": pltpu.SemaphoreType.REGULAR((3, 2)), "s2": dma((2,)), "r2": dma((2,)), "s2c": dma((2,)), "r2c": dma((2,)),
            "sf": dma((2,)), "rf": dma((2, nq - 1)), "sl": dma((2,)), "rl": dma((2, 3)),
            "st": dma((1,)), "rt": dma((1,)),
            "so": dma((2,)), "ro": dma((2,)), "lo": dma((2,)),
            "sy": dma(()), "ry": dma(()), "ly": dma(()),
            "sc": dma((2,)), "rc": dma((2,)),
            "srr": dma(()), "rrr": dma(()),
            "sd": dma((4,)), "rd": dma((4,)),
        }
        hbm = pl.BlockSpec(memory_space=pl.ANY)
        vmem = pl.BlockSpec(memory_space=pltpu.VMEM)
        far = pl.BlockSpec(memory_space=pltpu.HBM)
        new_one, new_two, dist = pl.pallas_call(
            functools.partial(kernel, nz, nx),
            out_shape=(
                jax.ShapeDtypeStruct((rows, width), BF16),
                jax.ShapeDtypeStruct((2 * nq, g, width), BF16),
                jax.ShapeDtypeStruct((1, LANES), F32),
            ),
            in_specs=[far, vmem, vmem, far, far],
            out_specs=(hbm, hbm, vmem),
            scratch_shapes=[v, sem],
            compiler_params=pltpu.CompilerParams(
                collective_id=0, has_side_effects=True, vmem_limit_bytes=53 * 1024 * 1024
            ),
        )(points, code_one.reshape(1, npts), code_two.reshape(1, npts), cent_one, cent_two)
        return new_one, new_two.reshape(rows, width), dist[0, :2]

    cents = P(("groups", "cb"), None)
    return jax.shard_map(
        local,
        mesh=mesh,
        in_specs=(P(("groups", "pts"), None), P(("groups", "pts")), P(("groups", "pts")), cents, cents),
        out_specs=(cents, cents, P("groups")),
        check_vma=False,
    )
```

```python
import functools

import jax
import jax.numpy as jnp
from jax import lax
from jax.experimental import pallas as pl
from jax.experimental.pallas import tpu as pltpu
from jax.sharding import PartitionSpec as P

MESH = pl.DeviceIdType.MESH
F32 = jnp.float32
BF16 = jnp.bfloat16
LANES = 128
HALF = 64
WIN = 4
NEAR = (-2, -1, 1)


TREE = (4, 3, -3, 2, -2, 1, -1)


def iota(shape, dim):
    return lax.broadcasted_iota(jnp.int32, shape, dim)


def kernel(nz, nx, pts, code1, code2, cent1, cent2, new1, new2, dist, v, sem):
    z = lax.axis_index("pts")
    cb = lax.axis_index("cb")
    x = cb // 2
    c = cb - 2 * x
    h = x - 2 * (x // 2)
    q = z // WIN
    cl = z - WIN * q
    par = cl - 2 * (cl // 2)
    e = cl // 2
    nq = nz // WIN
    s = 1 - 2 * c
    rows = cent1.shape[0]
    npts = pts.shape[0]
    chip = npts // nx
    g = 2 * rows // nz

    def qm(d):
        return lax.rem(q + d * s + 2 * nq, nq)

    def zq(d):
        return lax.rem(z + WIN * d * s + 2 * nz, nz)

    def zed(step):
        return lax.rem(z + step + nz, nz)

    def to_z(t):
        return {"pts": t}

    def to_x(t):
        return {"cb": 2 * t + c}

    sib = {"cb": 2 * x + 1 - c}

    def send(src, dst, ss, rs, where):
        pltpu.make_async_remote_copy(
            src_ref=src, dst_ref=dst, send_sem=ss, recv_sem=rs, device_id=where, device_id_type=MESH
        ).start()

    def wait(ref, sm):
        pltpu.make_async_copy(ref, ref, sm).wait()

    def xed(i):
        return lax.rem(x + i, nx)

    barrier = pltpu.get_barrier_semaphore()
    for step in (-2, -1, 1, 2):
        pl.semaphore_signal(barrier, inc=1, device_id=to_z(zed(step)), device_id_type=MESH)
    for i in range(1, nx):
        pl.semaphore_signal(barrier, inc=1, device_id=to_x(xed(i)), device_id_type=MESH)
    pl.semaphore_signal(barrier, inc=1, device_id=sib, device_id_type=MESH)

    tile_a = x + (x + 1) // 2
    tile_b = 1 + 3 * (x // 2)
    col_a = pl.ds(pl.multiple_of(tile_a * LANES, LANES), LANES)
    col_b = pl.ds(pl.multiple_of(tile_b * LANES, LANES), LANES)
    loads = [
        pltpu.make_async_copy(pts.at[:, col_a], v["P"].at[:, 0:LANES], sem["ld"].at[0]),
        pltpu.make_async_copy(pts.at[:, col_b], v["P"].at[:, LANES : 2 * LANES], sem["ld"].at[1]),
        pltpu.make_async_copy(cent1, v["C1"].at[x], sem["ld"].at[2]),
        pltpu.make_async_copy(cent2, v["C2"].at[x], sem["ld"].at[3]),
        pltpu.make_async_copy(pts.at[pl.ds(pl.multiple_of(x * chip, chip), chip), :], v["R1"], sem["ld"].at[4]),
    ]
    for ld in loads:
        ld.start()
    loads[0].wait()
    loads[1].wait()

    blk = 256
    hm_b = iota((blk, LANES), 1) // HALF == h
    hm_g = iota((g, LANES), 1) // HALF == h

    @pl.loop(0, npts // blk)
    def _(i):
        sl = pl.ds(pl.multiple_of(i * blk, blk), blk)
        v["W"][sl, 0:LANES] = v["P"][sl, 0:LANES]
        b = v["P"][sl, LANES : 2 * LANES].astype(F32)
        v["W"][sl, LANES : 2 * LANES] = jnp.where(hm_b, b, 1.0).astype(BF16)

    m16 = (iota((nq, g, LANES), 2) & (g - 1)) == iota((nq, g, LANES), 1)

    def class_of(i):
        t = zed(s * (i - 2 + (i // 2) * (5 - 2 * i)))
        return t, t // WIN, lax.rem(t, WIN)

    def class_sums(i, code, w, S, Sc):
        _, _, ct = class_of(i)
        pt = lax.rem(ct, 2)
        et = ct // 2
        n = 2 * nq * g
        r = iota((n, 1), 0)
        hl = r // (nq * g)
        rq = (r // g) & (nq - 1)
        lab = rows * (2 * (2 * pt + hl) + c) + g * (2 * rq + et) + (r & (g - 1))
        oh = jnp.where(lab == code[...], 1.0, 0.0).astype(BF16)
        out = jnp.dot(oh, w[...], preferred_element_type=F32)
        lo, hi = out[: nq * g], out[nq * g :]
        S[ct, :, 0:g, :] = lo[:, :LANES].reshape(nq, g, LANES)
        S[ct, :, g : 2 * g, :] = hi[:, :LANES].reshape(nq, g, LANES)
        lb = lo[:, LANES:]
        hb = pltpu.roll(hi[:, LANES:], HALF, 1)
        hm = iota(lb.shape, 1) // HALF == h
        S[ct, :, 2 * g :, :] = jnp.where(hm, lb, hb).reshape(nq, g, LANES)
        cnt = jnp.where(hm, hb, lb).reshape(nq, g, LANES)
        Sc[ct] = jnp.sum(jnp.where(m16, cnt, 0.0), axis=1, keepdims=True)

    def class_sends(i, S, Sc, X1, X1c, k):
        t, qt, ct = class_of(i)
        send(Sc.at[ct], X1c.at[i], sem["s1c"].at[k], sem["r1c"].at[k], to_z(t))
        for d in TREE + (0,):
            qd = lax.rem(qt + d * s + 2 * nq, nq)
            send(S.at[ct, qd], X1.at[i, qd], sem["s1"].at[k], sem["r1"].at[k, qd], to_z(t))

    def far_sums(S, Sc, X1, X1c, T, Tc, XM, XMc, X2, X2c, k, beside):
        wait(X1c, sem["r1c"].at[k])
        for d in TREE + (0,):
            qd = qm(d)
            wait(X1.at[:, 0], sem["r1"].at[k, qd])
            t = S[cl, qd] + X1[0, qd] + X1[1, qd] + X1[2, qd]
            n = Sc[cl, qd] + X1c[0, qd] + X1c[1, qd] + X1c[2, qd]
            for m in {2: (0, 1), -2: (2,)}.get(d, ()):
                wait(XM.at[m], sem["rm"].at[k, m])
                wait(XMc.at[m], sem["rmc"].at[k, m])
                t = t + XM[m]
                n = n + XMc[m]
            T[qd] = t
            Tc[qd] = n
            if d in (4, 3, -3):
                m = (4, 3, -3).index(d)
                to = to_z(zq((2, 1, -1)[m]))
                send(T.at[qd], XM.at[m], sem["s2"].at[k], sem["rm"].at[k, m], to)
                send(Tc.at[qd], XMc.at[m], sem["s2c"].at[k], sem["rmc"].at[k, m], to)
                if d == -3:
                    beside()
            elif d != 0:
                m = (1, -1, 2, -2).index(d)
                send(T.at[qd], X2.at[m], sem["s2"].at[k], sem["r2"].at[k], to_z(zq(d)))
                send(Tc.at[qd], X2c.at[m], sem["s2c"].at[k], sem["r2c"].at[k], to_z(zq(d)))

    def finish(T, Tc, X2, X2c, C, k):
        wait(X2c, sem["r2c"].at[k])
        cnt = Tc[q] + X2c[0] + X2c[1] + X2c[2] + X2c[3]
        wait(X2, sem["r2"].at[k])
        tot = T[q] + X2[0] + X2[1] + X2[2] + X2[3]
        full = jnp.broadcast_to(cnt, (g, LANES))
        diag = (iota((g, LANES), 1) & (HALF - 1)) == iota((g, LANES), 0)
        lo_n = jnp.sum(jnp.where(diag & jnp.logical_not(hm_g), full, 0.0), axis=1, keepdims=True) + 1.0
        hi_n = jnp.sum(jnp.where(diag & hm_g, full, 0.0), axis=1, keepdims=True) + 1.0
        sl = pl.ds(pl.multiple_of(g * (z // 2), g), g)
        at_lo = 2 * par
        at_hi = 2 * par + 1
        a_lo = C[at_lo, sl, col_a].astype(F32)
        a_hi = C[at_hi, sl, col_a].astype(F32)
        b_lo = C[at_lo, sl, col_b].astype(F32)
        b_hi = pltpu.roll(C[at_hi, sl, col_b].astype(F32), HALF, 1)
        new_lo = ((tot[0:g] + a_lo) / lo_n).astype(BF16)
        new_hi = ((tot[g : 2 * g] + a_hi) / hi_n).astype(BF16)
        new_b = ((tot[2 * g :] + jnp.where(hm_g, b_lo, b_hi)) / jnp.where(hm_g, lo_n, hi_n)).astype(BF16)
        return new_lo, new_hi, new_b

    def cidx(t):
        ct = lax.rem(t, WIN)
        return 2 * lax.rem(ct, 2) + ct // 2

    def far_gather(at, k, near_sends):
        slots = (1, -1, 2, -2, 3, -3, 4)

        def far_send(ref, d, to):
            send(ref, ref, sem["sf"].at[k], sem["rf"].at[k, slots.index(d)], to_z(zq(to)))

        for d in slots[5::-1]:
            far_send(at(q), d, d)
        near_sends(q)
        for d in slots:
            qs = qm(-d)
            wait(at(qs), sem["rf"].at[k, slots.index(d)])
            if d == 2:
                far_send(at(qs), 4, 2)
            near_sends(qs)

    def gather(N):
        ci = 2 * par + e

        def near_sends(qs):
            for i in range(3):
                send(N.at[c, ci, qs], N.at[c, ci, qs], sem["sl"].at[0], sem["rl"].at[0, i], to_z(zed(s * NEAR[i])))

        far_gather(lambda qs: N.at[c, ci, qs], 0, near_sends)
        send(N.at[c, ci], N.at[c, ci], sem["st"].at[0], sem["rt"].at[0], sib)
        for i in (2, 1, 0):
            cs = cidx(zed(-s * NEAR[i]))
            wait(N.at[c, cs], sem["rl"].at[0, i])
            send(N.at[c, cs], N.at[c, cs], sem["st"].at[0], sem["rt"].at[0], sib)

    def gather_rows(O):
        def near_sends(qs):
            at = O.at[2 * qs + e]
            for i, step in enumerate((1, -1, 2 * s)):
                send(at, at, sem["sl"].at[1], sem["rl"].at[1, i], to_z(zed(step)))

        far_gather(lambda qs: O.at[2 * qs + e], 1, near_sends)

    def out_parts(N, t):
        pair = pl.ds(2 * (t // 2), 2)
        rs = pl.ds(pl.multiple_of(g * lax.rem(t, 2), g), g)
        return N.at[c, pair, :, rs, :], N.at[c, pair, :, pl.ds(2 * g, g), :]

    def out_sends(N, OA, OB):
        for i in range(1, nx):
            t = xed(i)
            a, b = out_parts(N, t)
            send(a, OA.at[x], sem["so"].at[0], sem["ro"].at[0], to_x(t))
            send(b, OB.at[x], sem["so"].at[1], sem["ro"].at[1], to_x(t))
        a, b = out_parts(N, x)
        pltpu.make_async_copy(a, OA.at[x], sem["lo"].at[0]).start()
        pltpu.make_async_copy(b, OB.at[x], sem["lo"].at[1]).start()

    left = iota((g, LANES), 1) < HALF

    def out_rows(OA, OB, out):
        wait(OA.at[0], sem["lo"].at[0])
        wait(OB.at[0], sem["lo"].at[1])
        wait(OA.at[pl.ds(0, nx - 1)], sem["ro"].at[0])
        wait(OB.at[pl.ds(0, nx - 1)], sem["ro"].at[1])
        for ee in range(2):
            for qq in range(nq):
                r0 = g * (2 * qq + ee)
                for xx in range(nx):
                    ta = xx + (xx + 1) // 2
                    out[r0 : r0 + g, ta * LANES : (ta + 1) * LANES] = OA[xx, ee, qq]
                for y in range(nx // 2):
                    two = []
                    for xx in (2 * y, 2 * y + 1):
                        b = OB[xx, ee, qq].astype(F32)
                        two.append(jnp.where(h == 1, pltpu.roll(b, HALF, 1), b))
                    tb = 1 + 3 * y
                    out[r0 : r0 + g, tb * LANES : (tb + 1) * LANES] = jnp.where(left, two[0], two[1]).astype(BF16)

    def nearest(C, R):
        def body(k, m):
            ck = C[k]
            cross = lax.dot_general(ck, R[...], (((1,), (1,)), ((), ())), preferred_element_type=F32)
            cf = ck.astype(F32)
            csq = jnp.sum(cf * cf, axis=1, keepdims=True)
            d = csq - 2.0 * cross
            return jnp.minimum(m, jnp.min(d.reshape(rows // 8, 8, chip), axis=0))

        m = lax.fori_loop(0, nx, body, jnp.full((8, chip), jnp.inf, F32))
        r = R[...].astype(F32)
        psq = jnp.sum(jnp.sum(r * r, axis=0, keepdims=True), axis=1, keepdims=True)
        return jnp.min(m, axis=0, keepdims=True), psq

    @pl.loop(0, WIN)
    def _(i):
        class_sums(i, code1, v["W"], v["S1"], v["Sc1"])

    loads[2].wait()
    loads[3].wait()
    loads[4].wait()
    pl.semaphore_wait(barrier, 4 + (nx - 1) + 1)

    def tell(k, step):
        pl.semaphore_signal(sem["lv"].at[k, 0], inc=1, device_id=to_z(zed(-step)), device_id_type=MESH)
        pl.semaphore_signal(sem["lv"].at[k, 1], inc=1, device_id=to_z(zed(step)), device_id_type=MESH)

    def told(k):
        pl.semaphore_wait(sem["lv"].at[k, 0], 1)
        pl.semaphore_wait(sem["lv"].at[k, 1], 1)

    tell(0, 2)

    for i in range(3):
        class_sends(i, v["S1"], v["Sc1"], v["X11"], v["X1c1"], 0)
    right, left_x, over = xed(1), xed(nx - 1), xed(2)
    half = (pl.ds(0, rows // 2), pl.ds(rows // 2, rows // 2))

    def cent_pass(C, k):
        for side, (src, to) in enumerate(((left_x, right), (right, left_x))):
            wait(C.at[src], sem["rc"].at[k, side])
            send(C.at[src, half[side]], C.at[src, half[side]], sem["scf"].at[k], sem["rcf"].at[k], to_x(to))

    for k, C in enumerate((v["C1"], v["C2"])):
        send(C.at[x], C.at[x], sem["sc"].at[k], sem["rc"].at[k, 0], to_x(right))
        send(C.at[x], C.at[x], sem["sc"].at[k], sem["rc"].at[k, 1], to_x(left_x))

    for b in range(npts // LANES):
        row = code1[0:1, b * LANES : (b + 1) * LANES].astype(F32)
        v["CT"][b * LANES : (b + 1) * LANES, :] = jnp.transpose(jnp.broadcast_to(row, (LANES, LANES)))

    told(0)
    tell(1, WIN)
    told(1)
    tell(2, 2 * WIN)
    far_sums(v["S1"], v["Sc1"], v["X11"], v["X1c1"], v["T1"], v["Tc1"], v["XM1"], v["XMc1"], v["X21"], v["X2c1"], 0, lambda: cent_pass(v["C1"], 0))
    cent_pass(v["C2"], 1)
    wait(v["C1"].at[0], sem["rcf"].at[0])
    mins_one, psq_one = nearest(v["C1"], v["R1"])
    v["D0"][c, 0] = mins_one
    new_lo, new_hi, new_b = finish(v["T1"], v["Tc1"], v["X21"], v["X2c1"], v["C1"], 0)
    v["N1"][c, 2 * par + e, q, 0:g, :] = new_lo
    v["N1"][c, 2 * par + e, q, g : 2 * g, :] = new_hi
    v["N1"][c, 2 * par + e, q, 2 * g :, :] = new_b
    told(2)
    gather(v["N1"])
    wait(v["N1"].at[0], sem["rt"].at[0])

    kb = nq * g
    for cc in range(2):
        for k in range(WIN):
            base = (cc * WIN + k) * 2 * kb
            n = v["N1"][cc, k]
            v["L"][base : base + kb, 0:LANES] = n[:, 0:g, :].reshape(kb, LANES)
            v["L"][base + kb : base + 2 * kb, 0:LANES] = n[:, g : 2 * g, :].reshape(kb, LANES)
            b = n[:, 2 * g :, :].reshape(kb, LANES)
            v["L"][base : base + kb, LANES : 2 * LANES] = b
            v["L"][base + kb : base + 2 * kb, LANES : 2 * LANES] = pltpu.roll(b.astype(F32), HALF, 1).astype(BF16)

    @pl.loop(0, npts // blk)
    def _(i):
        sl = pl.ds(pl.multiple_of(i * blk, blk), blk)
        codes = v["CT"][sl, :]
        parts = []
        lane = iota((1, LANES), 1)
        for j in range(2 * nx * rows // LANES):
            r = lane + j * LANES
            cc = r // (WIN * 2 * kb)
            k = (r // (2 * kb)) & (WIN - 1)
            hl = (r // kb) & 1
            rq = (r // g) & (nq - 1)
            lab = rows * (2 * (2 * (k // 2) + hl) + cc) + g * (2 * rq + (k & 1)) + (r & (g - 1))
            parts.append(jnp.where(codes == lab.astype(F32), 1.0, 0.0).astype(BF16))
        oh = jnp.concatenate(parts, axis=1)
        looked = jnp.dot(oh, v["L"][...], preferred_element_type=F32)
        res = v["P"][sl, :].astype(F32) - looked
        v["W2"][sl, 0:LANES] = res[:, 0:LANES].astype(BF16)
        v["W2"][sl, LANES : 2 * LANES] = jnp.where(hm_b, res[:, LANES:], 1.0).astype(BF16)

    @pl.loop(0, WIN)
    def _(i):
        class_sums(i, code2, v["W2"], v["S2"], v["Sc2"])

        @pl.when(i < 3)
        def _():
            class_sends(i, v["S2"], v["Sc2"], v["X12"], v["X1c2"], 1)

    hc = chip // 2

    def pts_of(t, part):
        return pl.ds(pl.multiple_of(chip * t + hc * part, hc), hc)

    for side, to in enumerate((right, left_x)):
        send(v["W2"].at[pts_of(over, side), :], v["FW"].at[side], sem["sfw"], sem["rfw"].at[side], to_x(to))
    for to in (right, left_x):
        sl = pl.ds(pl.multiple_of(chip * to, chip), chip)
        send(v["W2"].at[sl, :], v["RR"].at[x], sem["srr"], sem["rrr"], to_x(to))

    def rows_pass():
        for side, (src, to) in enumerate(((left_x, right), (right, left_x))):
            wait(v["FW"].at[side], sem["rfw"].at[side])
            send(v["FW"].at[side], v["RR"].at[src, pl.ds(hc * side, hc)], sem["sff"], sem["rrf"], to_x(to))

    sl = pl.ds(pl.multiple_of(chip * x, chip), chip)
    mine = pltpu.make_async_copy(v["W2"].at[sl, :], v["RR"].at[x], sem["ld"].at[5])
    mine.start()
    far_sums(v["S2"], v["Sc2"], v["X12"], v["X1c2"], v["T2"], v["Tc2"], v["XM2"], v["XMc2"], v["X22"], v["X2c2"], 1, rows_pass)

    mine.wait()
    wait(v["RR"].at[pl.ds(0, 2)], sem["rrr"])
    wait(v["RR"].at[0], sem["rrf"])
    for xx in range(nx):
        ta = xx + (xx + 1) // 2
        v["R2"][:, ta * LANES : (ta + 1) * LANES] = v["RR"][xx, :, 0:LANES]
    left_own = iota((chip, LANES), 1) < HALF
    for y in range(nx // 2):
        tb = 1 + 3 * y
        v["R2"][:, tb * LANES : (tb + 1) * LANES] = jnp.where(
            left_own,
            v["RR"][2 * y, :, LANES:].astype(F32),
            v["RR"][2 * y + 1, :, LANES:].astype(F32),
        ).astype(BF16)
    wait(v["C2"].at[0], sem["rcf"].at[1])
    mins_two, psq_two = nearest(v["C2"], v["R2"])
    v["D0"][c, 1] = mins_two
    send(v["D0"].at[c], v["D0"].at[c], sem["sd"].at[0], sem["rd"].at[0], sib)
    wait(v["D0"].at[0], sem["rd"].at[0])
    lane = iota((1, LANES), 1)
    tot_one = jnp.sum(jnp.minimum(v["D0"][0, 0], v["D0"][1, 0]), axis=1, keepdims=True) + psq_one
    tot_two = jnp.sum(jnp.minimum(v["D0"][0, 1], v["D0"][1, 1]), axis=1, keepdims=True) + psq_two
    v["D1"][x] = jnp.where(lane == 0, tot_one, jnp.where(lane == 1, tot_two, 0.0))
    for i in range(1, nx):
        send(v["D1"].at[x], v["D1"].at[x], sem["sd"].at[1], sem["rd"].at[1], to_x(xed(i)))

    new_lo, new_hi, new_b = finish(v["T2"], v["Tc2"], v["X22"], v["X2c2"], v["C2"], 1)
    v["NC"][0:g, :] = new_lo
    v["NC"][g : 2 * g, :] = new_b
    v["NC"][2 * g :, :] = new_hi
    role = x // 2 == par
    for hl in range(2):
        t = 2 * par + hl
        src = v["NC"].at[pl.ds(g * hl, 2 * g), :]

        @pl.when(t != x)
        def _():
            send(src, v["Y"].at[x], sem["sy"], sem["ry"], to_x(t))

        @pl.when(t == x)
        def _():
            pltpu.make_async_copy(src, v["Y"].at[x], sem["ly"]).start()

    wait(v["D1"].at[pl.ds(0, nx - 1)], sem["rd"].at[1])
    tot = v["D1"][0]
    for i in range(1, nx):
        tot = tot + v["D1"][i]
    v["D2"][cl, q] = tot
    for o in range(1, nq):
        send(v["D2"].at[cl, q], v["D2"].at[cl, q], sem["sd"].at[2], sem["rd"].at[2], to_z(zed(WIN * o)))

    out_sends(v["N1"], v["OA1"], v["OB1"])

    def pass_dist():
        wait(v["D2"].at[0, pl.ds(0, nq - 1)], sem["rd"].at[2])
        for i in range(3):
            send(v["D2"].at[cl], v["D2"].at[cl], sem["sd"].at[3], sem["rd"].at[3], to_z(zed(s * NEAR[i])))

    @pl.when(role)
    def _():
        wait(v["Y"].at[pl.ds(0, nx - 1)], sem["ry"])
        wait(v["Y"].at[0], sem["ly"])
        mine = 2 * q + e
        for y in range(nx // 2):
            two = []
            for xx in (2 * y, 2 * y + 1):
                top = v["Y"][xx, 0:g, :].astype(F32)
                low = v["Y"][xx, g : 2 * g, :].astype(F32)
                ta = xx + (xx + 1) // 2
                v["O"][mine, :, ta * LANES : (ta + 1) * LANES] = jnp.where(h == 1, low, top).astype(BF16)
                two.append(jnp.where(h == 1, pltpu.roll(top, HALF, 1), low))
            tb = 1 + 3 * y
            v["O"][mine, :, tb * LANES : (tb + 1) * LANES] = jnp.where(left, two[0], two[1]).astype(BF16)
        gather_rows(v["O"])
        pass_dist()
        wait(v["O"].at[pl.ds(0, nq)], sem["rl"].at[1, 2])

    @pl.when(jnp.logical_not(role))
    def _():
        pass_dist()
        wait(v["O"].at[pl.ds(0, nq)], sem["rl"].at[1, 0])
        wait(v["O"].at[pl.ds(0, nq)], sem["rl"].at[1, 1])

    out_rows(v["OA1"], v["OB1"], v["NW"])
    put_one = pltpu.make_async_copy(v["NW"], new1, sem["ld"].at[6])
    put_one.start()
    put_two = pltpu.make_async_copy(v["O"], new2, sem["ld"].at[7])
    put_two.start()

    wait(v["D2"].at[pl.ds(0, 3)], sem["rd"].at[3])
    tot = v["D2"][0, 0]
    for i in range(1, nz):
        tot = tot + v["D2"][i // nq, i % nq]
    dist[...] = tot / jnp.float32(npts * nz * pts.shape[1])

    for k in range(2):
        wait(v["X11"], sem["s1"].at[k])
        wait(v["X1c1"], sem["s1c"].at[k])
        wait(v["X11"].at[0, pl.ds(0, nq - 1)], sem["s2"].at[k])
        wait(v["X1c1"].at[0, pl.ds(0, nq - 1)], sem["s2c"].at[k])
        wait(v["C1"].at[pl.ds(0, 2)], sem["sc"].at[k])
        wait(v["C1"].at[0], sem["scf"].at[k])
    wait(v["N1"].at[0, 0, pl.ds(0, nq - 1)], sem["sf"].at[0])
    wait(v["N1"].at[0, pl.ds(0, 3)], sem["sl"].at[0])
    wait(v["OA1"].at[pl.ds(0, nx - 1)], sem["so"].at[0])
    wait(v["OB1"].at[pl.ds(0, nx - 1)], sem["so"].at[1])
    wait(v["N1"].at[0], sem["st"].at[0])
    wait(v["RR"].at[pl.ds(0, 2)], sem["srr"])
    wait(v["FW"], sem["sfw"])
    wait(v["FW"], sem["sff"])
    wait(v["D0"].at[0], sem["sd"].at[0])
    wait(v["D1"].at[pl.ds(0, nx - 1)], sem["sd"].at[1])
    wait(v["D2"].at[0, pl.ds(0, nq - 1)], sem["sd"].at[2])
    wait(v["D2"].at[pl.ds(0, 3)], sem["sd"].at[3])

    @pl.when(role)
    def _():
        wait(v["O"].at[pl.ds(0, nq - 1)], sem["sf"].at[1])
        wait(v["X11"], sem["sl"].at[1])
        wait(v["Y"].at[0], sem["sy"])

    @pl.when(jnp.logical_not(role))
    def _():
        wait(v["Y"].at[pl.ds(0, 2)], sem["sy"])

    put_one.wait()
    put_two.wait()


def solution(mesh):
    nz = mesh.shape["pts"]
    nx = mesh.shape["cb"] // 2
    nq = nz // WIN

    def local(points, code_one, code_two, cent_one, cent_two):
        npts, width = points.shape
        rows = cent_one.shape[0]
        chip = npts // nx
        g = 2 * rows // nz
        ch = 3 * g
        vm = pltpu.VMEM
        v = {
            "P": vm((npts, 2 * LANES), BF16),
            "W": vm((npts, 2 * LANES), BF16),
            "W2": vm((npts, 2 * LANES), BF16),
            "CT": vm((npts, LANES), F32),
            "L": vm((2 * nx * rows, 2 * LANES), BF16),
            "R1": vm((chip, width), BF16),
            "R2": vm((chip, width), BF16),
            "FW": vm((2, chip // 2, 2 * LANES), BF16),
            "RR": vm((nx, chip, 2 * LANES), BF16),
            "D0": vm((2, 2, 1, chip), F32),
            "D1": vm((nx, 1, LANES), F32),
            "D2": vm((WIN, nq, 1, LANES), F32),
        }
        v["N1"] = vm((2, WIN, nq, ch, LANES), BF16)
        v["OA1"] = vm((nx, 2, nq, g, LANES), BF16)
        v["OB1"] = vm((nx, 2, nq, g, LANES), BF16)
        v["NW"] = vm((rows, width), BF16)
        v["NC"] = vm((ch, LANES), BF16)
        v["Y"] = vm((nx, 2 * g, LANES), BF16)
        v["O"] = vm((2 * nq, g, width), BF16)
        for k in ("1", "2"):
            v["C" + k] = vm((nx, rows, width), BF16)
            v["S" + k] = vm((WIN, nq, ch, LANES), F32)
            v["Sc" + k] = vm((WIN, nq, 1, LANES), F32)
            v["X1" + k] = vm((3, nq, ch, LANES), F32)
            v["X1c" + k] = vm((3, nq, 1, LANES), F32)
            v["T" + k] = vm((nq, ch, LANES), F32)
            v["Tc" + k] = vm((nq, 1, LANES), F32)
            v["XM" + k] = vm((3, ch, LANES), F32)
            v["X2" + k] = vm((4, ch, LANES), F32)
            v["X2c" + k] = vm((4, 1, LANES), F32)
            v["XMc" + k] = vm((3, 1, LANES), F32)
        dma = pltpu.SemaphoreType.DMA
        sem = {
            "ld": dma((8,)),
            "s1": dma((2,)), "r1": dma((2, nq)), "s1c": dma((2,)), "r1c": dma((2,)),
            "rm": dma((2, 3)), "rmc": dma((2, 3)), "lv": pltpu.SemaphoreType.REGULAR((3, 2)), "s2": dma((2,)), "r2": dma((2,)), "s2c": dma((2,)), "r2c": dma((2,)),
            "sf": dma((2,)), "rf": dma((2, nq - 1)), "sl": dma((2,)), "rl": dma((2, 3)),
            "st": dma((1,)), "rt": dma((1,)),
            "so": dma((2,)), "ro": dma((2,)), "lo": dma((2,)),
            "sy": dma(()), "ry": dma(()), "ly": dma(()),
            "sc": dma((2,)), "rc": dma((2, 2)), "scf": dma((2,)), "rcf": dma((2,)),
            "sfw": dma(()), "rfw": dma((2,)), "sff": dma(()), "rrf": dma(()),
            "srr": dma(()), "rrr": dma(()),
            "sd": dma((4,)), "rd": dma((4,)),
        }
        hbm = pl.BlockSpec(memory_space=pl.ANY)
        vmem = pl.BlockSpec(memory_space=pltpu.VMEM)
        far = pl.BlockSpec(memory_space=pltpu.HBM)
        new_one, new_two, dist = pl.pallas_call(
            functools.partial(kernel, nz, nx),
            out_shape=(
                jax.ShapeDtypeStruct((rows, width), BF16),
                jax.ShapeDtypeStruct((2 * nq, g, width), BF16),
                jax.ShapeDtypeStruct((1, LANES), F32),
            ),
            in_specs=[far, vmem, vmem, far, far],
            out_specs=(hbm, hbm, vmem),
            scratch_shapes=[v, sem],
            compiler_params=pltpu.CompilerParams(
                collective_id=0, has_side_effects=True, vmem_limit_bytes=53 * 1024 * 1024
            ),
        )(points, code_one.reshape(1, npts), code_two.reshape(1, npts), cent_one, cent_two)
        return new_one, new_two.reshape(rows, width), dist[0, :2]

    cents = P(("groups", "cb"), None)
    return jax.shard_map(
        local,
        mesh=mesh,
        in_specs=(P(("groups", "pts"), None), P(("groups", "pts")), P(("groups", "pts")), cents, cents),
        out_specs=(cents, cents, P("groups")),
        check_vma=False,
    )
```

```python
import functools

import jax
import jax.numpy as jnp
from jax import lax
from jax.experimental import pallas as pl
from jax.experimental.pallas import tpu as pltpu
from jax.sharding import PartitionSpec as P

MESH = pl.DeviceIdType.MESH
F32 = jnp.float32
BF16 = jnp.bfloat16
LANES = 128
HALF = 64
WIN = 4
NEAR = (-2, -1, 1)


TREE = (4, 3, -3, 2, -2, 1, -1)


def iota(shape, dim):
    return lax.broadcasted_iota(jnp.int32, shape, dim)


def kernel(nz, nx, pts, code1, code2, cent1, cent2, new1, new2, dist, v, sem):
    z = lax.axis_index("pts")
    cb = lax.axis_index("cb")
    x = cb // 2
    c = cb - 2 * x
    h = x - 2 * (x // 2)
    q = z // WIN
    cl = z - WIN * q
    par = cl - 2 * (cl // 2)
    e = cl // 2
    nq = nz // WIN
    s = 1 - 2 * c
    rows = cent1.shape[0]
    npts = pts.shape[0]
    chip = npts // nx
    g = 2 * rows // nz

    def qm(d):
        return lax.rem(q + d * s + 2 * nq, nq)

    def zq(d):
        return lax.rem(z + WIN * d * s + 2 * nz, nz)

    def zed(step):
        return lax.rem(z + step + nz, nz)

    def to_z(t):
        return {"pts": t}

    def to_x(t):
        return {"cb": 2 * t + c}

    sib = {"cb": 2 * x + 1 - c}

    def send(src, dst, ss, rs, where):
        pltpu.make_async_remote_copy(
            src_ref=src, dst_ref=dst, send_sem=ss, recv_sem=rs, device_id=where, device_id_type=MESH
        ).start()

    def wait(ref, sm):
        pltpu.make_async_copy(ref, ref, sm).wait()

    def xed(i):
        return lax.rem(x + i, nx)

    barrier = pltpu.get_barrier_semaphore()
    for step in (-2, -1, 1, 2):
        pl.semaphore_signal(barrier, inc=1, device_id=to_z(zed(step)), device_id_type=MESH)
    for i in range(1, nx):
        pl.semaphore_signal(barrier, inc=1, device_id=to_x(xed(i)), device_id_type=MESH)
    pl.semaphore_signal(barrier, inc=1, device_id=sib, device_id_type=MESH)

    tile_a = x + (x + 1) // 2
    tile_b = 1 + 3 * (x // 2)
    col_a = pl.ds(pl.multiple_of(tile_a * LANES, LANES), LANES)
    col_b = pl.ds(pl.multiple_of(tile_b * LANES, LANES), LANES)
    loads = [
        pltpu.make_async_copy(pts.at[:, col_a], v["P"].at[:, 0:LANES], sem["ld"].at[0]),
        pltpu.make_async_copy(pts.at[:, col_b], v["P"].at[:, LANES : 2 * LANES], sem["ld"].at[1]),
        pltpu.make_async_copy(cent1, v["C1"].at[x], sem["ld"].at[2]),
        pltpu.make_async_copy(cent2, v["C2"].at[x], sem["ld"].at[3]),
        pltpu.make_async_copy(pts.at[pl.ds(pl.multiple_of(x * chip, chip), chip), :], v["R1"], sem["ld"].at[4]),
    ]
    for ld in loads:
        ld.start()
    loads[0].wait()
    loads[1].wait()

    blk = 256
    hm_b = iota((blk, LANES), 1) // HALF == h
    hm_g = iota((g, LANES), 1) // HALF == h

    @pl.loop(0, npts // blk)
    def _(i):
        sl = pl.ds(pl.multiple_of(i * blk, blk), blk)
        v["W"][sl, 0:LANES] = v["P"][sl, 0:LANES]
        b = v["P"][sl, LANES : 2 * LANES].astype(F32)
        v["W"][sl, LANES : 2 * LANES] = jnp.where(hm_b, b, 1.0).astype(BF16)

    m16 = (iota((nq, g, LANES), 2) & (g - 1)) == iota((nq, g, LANES), 1)

    def class_of(i):
        t = zed(s * (i - 2 + (i // 2) * (5 - 2 * i)))
        return t, t // WIN, lax.rem(t, WIN)

    def class_sums(i, code, w, S, Sc):
        _, _, ct = class_of(i)
        pt = lax.rem(ct, 2)
        et = ct // 2
        n = 2 * nq * g
        r = iota((n, 1), 0)
        hl = r // (nq * g)
        rq = (r // g) & (nq - 1)
        lab = rows * (2 * (2 * pt + hl) + c) + g * (2 * rq + et) + (r & (g - 1))
        oh = jnp.where(lab == code[...], 1.0, 0.0).astype(BF16)
        out = jnp.dot(oh, w[...], preferred_element_type=F32)
        lo, hi = out[: nq * g], out[nq * g :]
        S[ct, :, 0:g, :] = lo[:, :LANES].reshape(nq, g, LANES)
        S[ct, :, g : 2 * g, :] = hi[:, :LANES].reshape(nq, g, LANES)
        lb = lo[:, LANES:]
        hb = pltpu.roll(hi[:, LANES:], HALF, 1)
        hm = iota(lb.shape, 1) // HALF == h
        S[ct, :, 2 * g :, :] = jnp.where(hm, lb, hb).reshape(nq, g, LANES)
        cnt = jnp.where(hm, hb, lb).reshape(nq, g, LANES)
        Sc[ct] = jnp.sum(jnp.where(m16, cnt, 0.0), axis=1, keepdims=True)

    def class_sends(i, S, Sc, X1, X1c, k):
        t, qt, ct = class_of(i)
        send(Sc.at[ct], X1c.at[i], sem["s1c"].at[k], sem["r1c"].at[k], to_z(t))
        for d in TREE + (0,):
            qd = lax.rem(qt + d * s + 2 * nq, nq)
            send(S.at[ct, qd], X1.at[i, qd], sem["s1"].at[k], sem["r1"].at[k, qd], to_z(t))

    def far_sums(S, Sc, X1, X1c, T, Tc, XM, XMc, X2, X2c, k, beside):
        wait(X1c, sem["r1c"].at[k])
        for d in TREE + (0,):
            qd = qm(d)
            wait(X1.at[:, 0], sem["r1"].at[k, qd])
            t = S[cl, qd] + X1[0, qd] + X1[1, qd] + X1[2, qd]
            n = Sc[cl, qd] + X1c[0, qd] + X1c[1, qd] + X1c[2, qd]
            for m in {2: (0, 1), -2: (2,)}.get(d, ()):
                wait(XM.at[m], sem["rm"].at[k, m])
                wait(XMc.at[m], sem["rmc"].at[k, m])
                t = t + XM[m]
                n = n + XMc[m]
            T[qd] = t
            Tc[qd] = n
            if d in (4, 3, -3):
                m = (4, 3, -3).index(d)
                to = to_z(zq((2, 1, -1)[m]))
                send(T.at[qd], XM.at[m], sem["s2"].at[k], sem["rm"].at[k, m], to)
                send(Tc.at[qd], XMc.at[m], sem["s2c"].at[k], sem["rmc"].at[k, m], to)
                if d == -3:
                    beside()
            elif d != 0:
                m = (1, -1, 2, -2).index(d)
                send(T.at[qd], X2.at[m], sem["s2"].at[k], sem["r2"].at[k], to_z(zq(d)))
                send(Tc.at[qd], X2c.at[m], sem["s2c"].at[k], sem["r2c"].at[k], to_z(zq(d)))

    def finish(T, Tc, X2, X2c, C, k):
        wait(X2c, sem["r2c"].at[k])
        cnt = Tc[q] + X2c[0] + X2c[1] + X2c[2] + X2c[3]
        wait(X2, sem["r2"].at[k])
        tot = T[q] + X2[0] + X2[1] + X2[2] + X2[3]
        full = jnp.broadcast_to(cnt, (g, LANES))
        diag = (iota((g, LANES), 1) & (HALF - 1)) == iota((g, LANES), 0)
        lo_n = jnp.sum(jnp.where(diag & jnp.logical_not(hm_g), full, 0.0), axis=1, keepdims=True) + 1.0
        hi_n = jnp.sum(jnp.where(diag & hm_g, full, 0.0), axis=1, keepdims=True) + 1.0
        sl = pl.ds(pl.multiple_of(g * (z // 2), g), g)
        at_lo = 2 * par
        at_hi = 2 * par + 1
        a_lo = C[at_lo, sl, col_a].astype(F32)
        a_hi = C[at_hi, sl, col_a].astype(F32)
        b_lo = C[at_lo, sl, col_b].astype(F32)
        b_hi = pltpu.roll(C[at_hi, sl, col_b].astype(F32), HALF, 1)
        new_lo = ((tot[0:g] + a_lo) / lo_n).astype(BF16)
        new_hi = ((tot[g : 2 * g] + a_hi) / hi_n).astype(BF16)
        new_b = ((tot[2 * g :] + jnp.where(hm_g, b_lo, b_hi)) / jnp.where(hm_g, lo_n, hi_n)).astype(BF16)
        return new_lo, new_hi, new_b

    def cidx(t):
        ct = lax.rem(t, WIN)
        return 2 * lax.rem(ct, 2) + ct // 2

    def far_gather(at, k, near_sends):
        slots = (1, -1, 2, -2, 3, -3, 4)

        def far_send(ref, d, to):
            send(ref, ref, sem["sf"].at[k], sem["rf"].at[k, slots.index(d)], to_z(zq(to)))

        for d in slots[5::-1]:
            far_send(at(q), d, d)
        near_sends(q)
        for d in slots:
            qs = qm(-d)
            wait(at(qs), sem["rf"].at[k, slots.index(d)])
            if d == 2:
                far_send(at(qs), 4, 2)
            near_sends(qs)

    def gather(N):
        ci = 2 * par + e

        def near_sends(qs):
            for i in range(3):
                send(N.at[c, ci, qs], N.at[c, ci, qs], sem["sl"].at[0], sem["rl"].at[0, i], to_z(zed(s * NEAR[i])))

        far_gather(lambda qs: N.at[c, ci, qs], 0, near_sends)
        send(N.at[c, ci], N.at[c, ci], sem["st"].at[0], sem["rt"].at[0], sib)
        for i in (2, 1, 0):
            cs = cidx(zed(-s * NEAR[i]))
            wait(N.at[c, cs], sem["rl"].at[0, i])
            send(N.at[c, cs], N.at[c, cs], sem["st"].at[0], sem["rt"].at[0], sib)

    def gather_rows(O):
        def near_sends(qs):
            at = O.at[2 * qs + e]
            for i, step in enumerate((1, -1, 2 * s)):
                send(at, at, sem["sl"].at[1], sem["rl"].at[1, i], to_z(zed(step)))

        far_gather(lambda qs: O.at[2 * qs + e], 1, near_sends)

    def out_parts(N, t):
        pair = pl.ds(2 * (t // 2), 2)
        rs = pl.ds(pl.multiple_of(g * lax.rem(t, 2), g), g)
        return N.at[c, pair, :, rs, :], N.at[c, pair, :, pl.ds(2 * g, g), :]

    def out_sends(N, OA, OB):
        for i in range(1, nx):
            t = xed(i)
            a, b = out_parts(N, t)
            send(a, OA.at[x], sem["so"].at[0], sem["ro"].at[0], to_x(t))
            send(b, OB.at[x], sem["so"].at[1], sem["ro"].at[1], to_x(t))
        a, b = out_parts(N, x)
        pltpu.make_async_copy(a, OA.at[x], sem["lo"].at[0]).start()
        pltpu.make_async_copy(b, OB.at[x], sem["lo"].at[1]).start()

    left = iota((g, LANES), 1) < HALF

    def out_rows(OA, OB, out):
        wait(OA.at[0], sem["lo"].at[0])
        wait(OB.at[0], sem["lo"].at[1])
        wait(OA.at[pl.ds(0, nx - 1)], sem["ro"].at[0])
        wait(OB.at[pl.ds(0, nx - 1)], sem["ro"].at[1])
        for ee in range(2):
            for qq in range(nq):
                r0 = g * (2 * qq + ee)
                for xx in range(nx):
                    ta = xx + (xx + 1) // 2
                    out[r0 : r0 + g, ta * LANES : (ta + 1) * LANES] = OA[xx, ee, qq]
                for y in range(nx // 2):
                    two = []
                    for xx in (2 * y, 2 * y + 1):
                        b = OB[xx, ee, qq].astype(F32)
                        two.append(jnp.where(h == 1, pltpu.roll(b, HALF, 1), b))
                    tb = 1 + 3 * y
                    out[r0 : r0 + g, tb * LANES : (tb + 1) * LANES] = jnp.where(left, two[0], two[1]).astype(BF16)

    def nearest(C, R):
        def body(k, m):
            ck = C[k]
            cross = lax.dot_general(ck, R[...], (((1,), (1,)), ((), ())), preferred_element_type=F32)
            cf = ck.astype(F32)
            csq = jnp.sum(cf * cf, axis=1, keepdims=True)
            d = csq - 2.0 * cross
            return jnp.minimum(m, jnp.min(d.reshape(rows // 8, 8, chip), axis=0))

        m = lax.fori_loop(0, nx, body, jnp.full((8, chip), jnp.inf, F32))
        r = R[...].astype(F32)
        psq = jnp.sum(jnp.sum(r * r, axis=0, keepdims=True), axis=1, keepdims=True)
        return jnp.min(m, axis=0, keepdims=True), psq

    @pl.loop(0, WIN)
    def _(i):
        class_sums(i, code1, v["W"], v["S1"], v["Sc1"])

    loads[2].wait()
    loads[3].wait()
    loads[4].wait()
    pl.semaphore_wait(barrier, 4 + (nx - 1) + 1)

    def tell(k, step):
        pl.semaphore_signal(sem["lv"].at[k, 0], inc=1, device_id=to_z(zed(-step)), device_id_type=MESH)
        pl.semaphore_signal(sem["lv"].at[k, 1], inc=1, device_id=to_z(zed(step)), device_id_type=MESH)

    def told(k):
        pl.semaphore_wait(sem["lv"].at[k, 0], 1)
        pl.semaphore_wait(sem["lv"].at[k, 1], 1)

    tell(0, 2)

    for i in range(3):
        class_sends(i, v["S1"], v["Sc1"], v["X11"], v["X1c1"], 0)
    right, left_x, over = xed(1), xed(nx - 1), xed(2)
    half = (pl.ds(0, rows // 2), pl.ds(rows // 2, rows // 2))

    def cent_pass(C, k):
        for side, (src, to) in enumerate(((left_x, right), (right, left_x))):
            wait(C.at[src], sem["rc"].at[k, side])
            send(C.at[src, half[side]], C.at[src, half[side]], sem["scf"].at[k], sem["rcf"].at[k], to_x(to))

    for k, C in enumerate((v["C1"], v["C2"])):
        send(C.at[x], C.at[x], sem["sc"].at[k], sem["rc"].at[k, 0], to_x(right))
        send(C.at[x], C.at[x], sem["sc"].at[k], sem["rc"].at[k, 1], to_x(left_x))

    for b in range(npts // LANES):
        row = code1[0:1, b * LANES : (b + 1) * LANES].astype(F32)
        v["CT"][b * LANES : (b + 1) * LANES, :] = jnp.transpose(jnp.broadcast_to(row, (LANES, LANES)))

    told(0)
    tell(1, WIN)
    told(1)
    tell(2, 2 * WIN)
    far_sums(v["S1"], v["Sc1"], v["X11"], v["X1c1"], v["T1"], v["Tc1"], v["XM1"], v["XMc1"], v["X21"], v["X2c1"], 0, lambda: cent_pass(v["C1"], 0))
    wait(v["C1"].at[0], sem["rcf"].at[0])
    mins_one, psq_one = nearest(v["C1"], v["R1"])
    v["D0"][c, 0] = mins_one
    new_lo, new_hi, new_b = finish(v["T1"], v["Tc1"], v["X21"], v["X2c1"], v["C1"], 0)
    v["N1"][c, 2 * par + e, q, 0:g, :] = new_lo
    v["N1"][c, 2 * par + e, q, g : 2 * g, :] = new_hi
    v["N1"][c, 2 * par + e, q, 2 * g :, :] = new_b
    told(2)
    gather(v["N1"])
    cent_pass(v["C2"], 1)
    kb = nq * g
    for part in range(2):
        if part == 1:
            wait(v["N1"].at[0], sem["rt"].at[0])
        cc = c if part == 0 else 1 - c
        for k in range(WIN):
            base = k * 2 * kb
            n = v["N1"][cc, k]
            v["L"][part, base : base + kb, 0:LANES] = n[:, 0:g, :].reshape(kb, LANES)
            v["L"][part, base + kb : base + 2 * kb, 0:LANES] = n[:, g : 2 * g, :].reshape(kb, LANES)
            b = n[:, 2 * g :, :].reshape(kb, LANES)
            v["L"][part, base : base + kb, LANES : 2 * LANES] = b
            v["L"][part, base + kb : base + 2 * kb, LANES : 2 * LANES] = pltpu.roll(b.astype(F32), HALF, 1).astype(BF16)

        @pl.loop(0, npts // blk)
        def _(i):
            sl = pl.ds(pl.multiple_of(i * blk, blk), blk)
            codes = v["CT"][sl, :]
            parts = []
            lane = iota((1, LANES), 1)
            for j in range(nx * rows // LANES):
                r = lane + j * LANES
                k = r // (2 * kb)
                hl = (r // kb) & 1
                rq = (r // g) & (nq - 1)
                lab = rows * (2 * (2 * (k // 2) + hl) + cc) + g * (2 * rq + (k & 1)) + (r & (g - 1))
                parts.append(jnp.where(codes == lab.astype(F32), 1.0, 0.0).astype(BF16))
            oh = jnp.concatenate(parts, axis=1)
            looked = jnp.dot(oh, v["L"][part], preferred_element_type=F32)
            if part == 0:
                v["ACC"][sl, :] = looked
            else:
                res = v["P"][sl, :].astype(F32) - (v["ACC"][sl, :] + looked)
                v["W2"][sl, 0:LANES] = res[:, 0:LANES].astype(BF16)
                v["W2"][sl, LANES : 2 * LANES] = jnp.where(hm_b, res[:, LANES:], 1.0).astype(BF16)

    @pl.loop(0, WIN)
    def _(i):
        class_sums(i, code2, v["W2"], v["S2"], v["Sc2"])

        @pl.when(i < 3)
        def _():
            class_sends(i, v["S2"], v["Sc2"], v["X12"], v["X1c2"], 1)

    hc = chip // 2

    def pts_of(t, part):
        return pl.ds(pl.multiple_of(chip * t + hc * part, hc), hc)

    for side, to in enumerate((right, left_x)):
        send(v["W2"].at[pts_of(over, side), :], v["FW"].at[side], sem["sfw"], sem["rfw"].at[side], to_x(to))
    for to in (right, left_x):
        sl = pl.ds(pl.multiple_of(chip * to, chip), chip)
        send(v["W2"].at[sl, :], v["RR"].at[x], sem["srr"], sem["rrr"], to_x(to))

    def rows_pass():
        for side, (src, to) in enumerate(((left_x, right), (right, left_x))):
            wait(v["FW"].at[side], sem["rfw"].at[side])
            send(v["FW"].at[side], v["RR"].at[src, pl.ds(hc * side, hc)], sem["sff"], sem["rrf"], to_x(to))

    sl = pl.ds(pl.multiple_of(chip * x, chip), chip)
    mine = pltpu.make_async_copy(v["W2"].at[sl, :], v["RR"].at[x], sem["ld"].at[5])
    mine.start()
    far_sums(v["S2"], v["Sc2"], v["X12"], v["X1c2"], v["T2"], v["Tc2"], v["XM2"], v["XMc2"], v["X22"], v["X2c2"], 1, rows_pass)
    out_sends(v["N1"], v["OA1"], v["OB1"])

    mine.wait()
    wait(v["RR"].at[pl.ds(0, 2)], sem["rrr"])
    wait(v["RR"].at[0], sem["rrf"])
    for xx in range(nx):
        ta = xx + (xx + 1) // 2
        v["R2"][:, ta * LANES : (ta + 1) * LANES] = v["RR"][xx, :, 0:LANES]
    left_own = iota((chip, LANES), 1) < HALF
    for y in range(nx // 2):
        tb = 1 + 3 * y
        v["R2"][:, tb * LANES : (tb + 1) * LANES] = jnp.where(
            left_own,
            v["RR"][2 * y, :, LANES:].astype(F32),
            v["RR"][2 * y + 1, :, LANES:].astype(F32),
        ).astype(BF16)
    wait(v["C2"].at[0], sem["rcf"].at[1])
    mins_two, psq_two = nearest(v["C2"], v["R2"])
    v["D0"][c, 1] = mins_two
    send(v["D0"].at[c], v["D0"].at[c], sem["sd"].at[0], sem["rd"].at[0], sib)
    wait(v["D0"].at[0], sem["rd"].at[0])
    lane = iota((1, LANES), 1)
    tot_one = jnp.sum(jnp.minimum(v["D0"][0, 0], v["D0"][1, 0]), axis=1, keepdims=True) + psq_one
    tot_two = jnp.sum(jnp.minimum(v["D0"][0, 1], v["D0"][1, 1]), axis=1, keepdims=True) + psq_two
    v["D1"][x] = jnp.where(lane == 0, tot_one, jnp.where(lane == 1, tot_two, 0.0))
    for i in range(1, nx):
        send(v["D1"].at[x], v["D1"].at[x], sem["sd"].at[1], sem["rd"].at[1], to_x(xed(i)))

    new_lo, new_hi, new_b = finish(v["T2"], v["Tc2"], v["X22"], v["X2c2"], v["C2"], 1)
    v["NC"][0:g, :] = new_lo
    v["NC"][g : 2 * g, :] = new_b
    v["NC"][2 * g :, :] = new_hi
    role = x // 2 == par
    for hl in range(2):
        t = 2 * par + hl
        src = v["NC"].at[pl.ds(g * hl, 2 * g), :]

        @pl.when(t != x)
        def _():
            send(src, v["Y"].at[x], sem["sy"], sem["ry"], to_x(t))

        @pl.when(t == x)
        def _():
            pltpu.make_async_copy(src, v["Y"].at[x], sem["ly"]).start()

    wait(v["D1"].at[pl.ds(0, nx - 1)], sem["rd"].at[1])
    tot = v["D1"][0]
    for i in range(1, nx):
        tot = tot + v["D1"][i]
    v["D2"][cl, q] = tot
    for o in range(1, nq):
        send(v["D2"].at[cl, q], v["D2"].at[cl, q], sem["sd"].at[2], sem["rd"].at[2], to_z(zed(WIN * o)))

    out_rows(v["OA1"], v["OB1"], v["NW"])
    put_one = pltpu.make_async_copy(v["NW"], new1, sem["ld"].at[6])
    put_one.start()

    def pass_dist():
        wait(v["D2"].at[0, pl.ds(0, nq - 1)], sem["rd"].at[2])
        for i in range(3):
            send(v["D2"].at[cl], v["D2"].at[cl], sem["sd"].at[3], sem["rd"].at[3], to_z(zed(s * NEAR[i])))

    @pl.when(role)
    def _():
        wait(v["Y"].at[pl.ds(0, nx - 1)], sem["ry"])
        wait(v["Y"].at[0], sem["ly"])
        mine = 2 * q + e
        for y in range(nx // 2):
            two = []
            for xx in (2 * y, 2 * y + 1):
                top = v["Y"][xx, 0:g, :].astype(F32)
                low = v["Y"][xx, g : 2 * g, :].astype(F32)
                ta = xx + (xx + 1) // 2
                v["O"][mine, :, ta * LANES : (ta + 1) * LANES] = jnp.where(h == 1, low, top).astype(BF16)
                two.append(jnp.where(h == 1, pltpu.roll(top, HALF, 1), low))
            tb = 1 + 3 * y
            v["O"][mine, :, tb * LANES : (tb + 1) * LANES] = jnp.where(left, two[0], two[1]).astype(BF16)
        gather_rows(v["O"])
        pass_dist()
        wait(v["O"].at[pl.ds(0, nq)], sem["rl"].at[1, 2])

    @pl.when(jnp.logical_not(role))
    def _():
        pass_dist()
        wait(v["O"].at[pl.ds(0, nq)], sem["rl"].at[1, 0])
        wait(v["O"].at[pl.ds(0, nq)], sem["rl"].at[1, 1])

    put_two = pltpu.make_async_copy(v["O"], new2, sem["ld"].at[7])
    put_two.start()

    wait(v["D2"].at[pl.ds(0, 3)], sem["rd"].at[3])
    tot = v["D2"][0, 0]
    for i in range(1, nz):
        tot = tot + v["D2"][i // nq, i % nq]
    dist[...] = tot / jnp.float32(npts * nz * pts.shape[1])

    for k in range(2):
        wait(v["X11"], sem["s1"].at[k])
        wait(v["X1c1"], sem["s1c"].at[k])
        wait(v["X11"].at[0, pl.ds(0, nq - 1)], sem["s2"].at[k])
        wait(v["X1c1"].at[0, pl.ds(0, nq - 1)], sem["s2c"].at[k])
        wait(v["C1"].at[pl.ds(0, 2)], sem["sc"].at[k])
        wait(v["C1"].at[0], sem["scf"].at[k])
    wait(v["N1"].at[0, 0, pl.ds(0, nq - 1)], sem["sf"].at[0])
    wait(v["N1"].at[0, pl.ds(0, 3)], sem["sl"].at[0])
    wait(v["OA1"].at[pl.ds(0, nx - 1)], sem["so"].at[0])
    wait(v["OB1"].at[pl.ds(0, nx - 1)], sem["so"].at[1])
    wait(v["N1"].at[0], sem["st"].at[0])
    wait(v["RR"].at[pl.ds(0, 2)], sem["srr"])
    wait(v["FW"], sem["sfw"])
    wait(v["FW"], sem["sff"])
    wait(v["D0"].at[0], sem["sd"].at[0])
    wait(v["D1"].at[pl.ds(0, nx - 1)], sem["sd"].at[1])
    wait(v["D2"].at[0, pl.ds(0, nq - 1)], sem["sd"].at[2])
    wait(v["D2"].at[pl.ds(0, 3)], sem["sd"].at[3])

    @pl.when(role)
    def _():
        wait(v["O"].at[pl.ds(0, nq - 1)], sem["sf"].at[1])
        wait(v["X11"], sem["sl"].at[1])
        wait(v["Y"].at[0], sem["sy"])

    @pl.when(jnp.logical_not(role))
    def _():
        wait(v["Y"].at[pl.ds(0, 2)], sem["sy"])

    put_one.wait()
    put_two.wait()


def solution(mesh):
    nz = mesh.shape["pts"]
    nx = mesh.shape["cb"] // 2
    nq = nz // WIN

    def local(points, code_one, code_two, cent_one, cent_two):
        npts, width = points.shape
        rows = cent_one.shape[0]
        chip = npts // nx
        g = 2 * rows // nz
        ch = 3 * g
        vm = pltpu.VMEM
        v = {
            "P": vm((npts, 2 * LANES), BF16),
            "W": vm((npts, 2 * LANES), BF16),
            "W2": vm((npts, 2 * LANES), BF16),
            "CT": vm((npts, LANES), F32),
            "L": vm((2, nx * rows, 2 * LANES), BF16),
            "ACC": vm((npts, 2 * LANES), F32),
            "R1": vm((chip, width), BF16),
            "R2": vm((chip, width), BF16),
            "FW": vm((2, chip // 2, 2 * LANES), BF16),
            "RR": vm((nx, chip, 2 * LANES), BF16),
            "D0": vm((2, 2, 1, chip), F32),
            "D1": vm((nx, 1, LANES), F32),
            "D2": vm((WIN, nq, 1, LANES), F32),
        }
        v["N1"] = vm((2, WIN, nq, ch, LANES), BF16)
        v["OA1"] = vm((nx, 2, nq, g, LANES), BF16)
        v["OB1"] = vm((nx, 2, nq, g, LANES), BF16)
        v["NW"] = vm((rows, width), BF16)
        v["NC"] = vm((ch, LANES), BF16)
        v["Y"] = vm((nx, 2 * g, LANES), BF16)
        v["O"] = vm((2 * nq, g, width), BF16)
        for k in ("1", "2"):
            v["C" + k] = vm((nx, rows, width), BF16)
            v["S" + k] = vm((WIN, nq, ch, LANES), F32)
            v["Sc" + k] = vm((WIN, nq, 1, LANES), F32)
            v["X1" + k] = vm((3, nq, ch, LANES), F32)
            v["X1c" + k] = vm((3, nq, 1, LANES), F32)
            v["T" + k] = vm((nq, ch, LANES), F32)
            v["Tc" + k] = vm((nq, 1, LANES), F32)
            v["XM" + k] = vm((3, ch, LANES), F32)
            v["X2" + k] = vm((4, ch, LANES), F32)
            v["X2c" + k] = vm((4, 1, LANES), F32)
            v["XMc" + k] = vm((3, 1, LANES), F32)
        dma = pltpu.SemaphoreType.DMA
        sem = {
            "ld": dma((8,)),
            "s1": dma((2,)), "r1": dma((2, nq)), "s1c": dma((2,)), "r1c": dma((2,)),
            "rm": dma((2, 3)), "rmc": dma((2, 3)), "lv": pltpu.SemaphoreType.REGULAR((3, 2)), "s2": dma((2,)), "r2": dma((2,)), "s2c": dma((2,)), "r2c": dma((2,)),
            "sf": dma((2,)), "rf": dma((2, nq - 1)), "sl": dma((2,)), "rl": dma((2, 3)),
            "st": dma((1,)), "rt": dma((1,)),
            "so": dma((2,)), "ro": dma((2,)), "lo": dma((2,)),
            "sy": dma(()), "ry": dma(()), "ly": dma(()),
            "sc": dma((2,)), "rc": dma((2, 2)), "scf": dma((2,)), "rcf": dma((2,)),
            "sfw": dma(()), "rfw": dma((2,)), "sff": dma(()), "rrf": dma(()),
            "srr": dma(()), "rrr": dma(()),
            "sd": dma((4,)), "rd": dma((4,)),
        }
        hbm = pl.BlockSpec(memory_space=pl.ANY)
        vmem = pl.BlockSpec(memory_space=pltpu.VMEM)
        far = pl.BlockSpec(memory_space=pltpu.HBM)
        new_one, new_two, dist = pl.pallas_call(
            functools.partial(kernel, nz, nx),
            out_shape=(
                jax.ShapeDtypeStruct((rows, width), BF16),
                jax.ShapeDtypeStruct((2 * nq, g, width), BF16),
                jax.ShapeDtypeStruct((1, LANES), F32),
            ),
            in_specs=[far, vmem, vmem, far, far],
            out_specs=(hbm, hbm, vmem),
            scratch_shapes=[v, sem],
            compiler_params=pltpu.CompilerParams(
                collective_id=0, has_side_effects=True, vmem_limit_bytes=53 * 1024 * 1024
            ),
        )(points, code_one.reshape(1, npts), code_two.reshape(1, npts), cent_one, cent_two)
        return new_one, new_two.reshape(rows, width), dist[0, :2]

    cents = P(("groups", "cb"), None)
    return jax.shard_map(
        local,
        mesh=mesh,
        in_specs=(P(("groups", "pts"), None), P(("groups", "pts")), P(("groups", "pts")), cents, cents),
        out_specs=(cents, cents, P("groups")),
        check_vma=False,
    )
```

```python
import functools

import jax
import jax.numpy as jnp
from jax import lax
from jax.experimental import pallas as pl
from jax.experimental.pallas import tpu as pltpu
from jax.sharding import PartitionSpec as P

MESH = pl.DeviceIdType.MESH
F32 = jnp.float32
BF16 = jnp.bfloat16
LANES = 128
HALF = 64
WIN = 4
NEAR = (-2, -1, 1)


TREE = (4, 3, -3, 2, -2, 1, -1)


def iota(shape, dim):
    return lax.broadcasted_iota(jnp.int32, shape, dim)


def kernel(nz, nx, pts, code1, code2, cent1, cent2, new1, new2, dist, v, sem):
    z = lax.axis_index("pts")
    cb = lax.axis_index("cb")
    x = cb // 2
    c = cb - 2 * x
    h = x - 2 * (x // 2)
    q = z // WIN
    cl = z - WIN * q
    par = cl - 2 * (cl // 2)
    e = cl // 2
    nq = nz // WIN
    s = 1 - 2 * c
    rows = cent1.shape[0]
    npts = pts.shape[0]
    chip = npts // nx
    g = 2 * rows // nz

    def qm(d):
        return lax.rem(q + d * s + 2 * nq, nq)

    def zq(d):
        return lax.rem(z + WIN * d * s + 2 * nz, nz)

    def zed(step):
        return lax.rem(z + step + nz, nz)

    def to_z(t):
        return {"pts": t}

    def to_x(t):
        return {"cb": 2 * t + c}

    sib = {"cb": 2 * x + 1 - c}

    def send(src, dst, ss, rs, where):
        pltpu.make_async_remote_copy(
            src_ref=src, dst_ref=dst, send_sem=ss, recv_sem=rs, device_id=where, device_id_type=MESH
        ).start()

    def wait(ref, sm):
        pltpu.make_async_copy(ref, ref, sm).wait()

    def xed(i):
        return lax.rem(x + i, nx)

    barrier = pltpu.get_barrier_semaphore()
    for step in (-2, -1, 1, 2):
        pl.semaphore_signal(barrier, inc=1, device_id=to_z(zed(step)), device_id_type=MESH)
    for i in range(1, nx):
        pl.semaphore_signal(barrier, inc=1, device_id=to_x(xed(i)), device_id_type=MESH)
    pl.semaphore_signal(barrier, inc=1, device_id=sib, device_id_type=MESH)

    tile_a = x + (x + 1) // 2
    tile_b = 1 + 3 * (x // 2)
    col_a = pl.ds(pl.multiple_of(tile_a * LANES, LANES), LANES)
    col_b = pl.ds(pl.multiple_of(tile_b * LANES, LANES), LANES)
    loads = [
        pltpu.make_async_copy(pts.at[:, col_a], v["P"].at[:, 0:LANES], sem["ld"].at[0]),
        pltpu.make_async_copy(pts.at[:, col_b], v["P"].at[:, LANES : 2 * LANES], sem["ld"].at[1]),
        pltpu.make_async_copy(cent1, v["C1"].at[x], sem["ld"].at[2]),
        pltpu.make_async_copy(cent2, v["C2"].at[x], sem["ld"].at[3]),
        pltpu.make_async_copy(pts.at[pl.ds(pl.multiple_of(x * chip, chip), chip), :], v["R1"], sem["ld"].at[4]),
    ]
    for ld in loads:
        ld.start()
    loads[0].wait()
    loads[1].wait()

    blk = 256
    hm_b = iota((blk, LANES), 1) // HALF == h
    hm_g = iota((g, LANES), 1) // HALF == h

    @pl.loop(0, npts // blk)
    def _(i):
        sl = pl.ds(pl.multiple_of(i * blk, blk), blk)
        v["W"][sl, 0:LANES] = v["P"][sl, 0:LANES]
        b = v["P"][sl, LANES : 2 * LANES].astype(F32)
        v["W"][sl, LANES : 2 * LANES] = jnp.where(hm_b, b, 1.0).astype(BF16)

    m16 = (iota((nq, g, LANES), 2) & (g - 1)) == iota((nq, g, LANES), 1)

    def class_of(i):
        t = zed(s * (i - 2 + (i // 2) * (5 - 2 * i)))
        return t, t // WIN, lax.rem(t, WIN)

    def class_sums(i, code, w, S, Sc):
        _, _, ct = class_of(i)
        pt = lax.rem(ct, 2)
        et = ct // 2
        n = 2 * nq * g
        r = iota((n, 1), 0)
        hl = r // (nq * g)
        rq = (r // g) & (nq - 1)
        lab = rows * (2 * (2 * pt + hl) + c) + g * (2 * rq + et) + (r & (g - 1))
        oh = jnp.where(lab == code[...], 1.0, 0.0).astype(BF16)
        out = jnp.dot(oh, w[...], preferred_element_type=F32)
        lo, hi = out[: nq * g], out[nq * g :]
        S[ct, :, 0:g, :] = lo[:, :LANES].reshape(nq, g, LANES)
        S[ct, :, g : 2 * g, :] = hi[:, :LANES].reshape(nq, g, LANES)
        lb = lo[:, LANES:]
        hb = pltpu.roll(hi[:, LANES:], HALF, 1)
        hm = iota(lb.shape, 1) // HALF == h
        S[ct, :, 2 * g :, :] = jnp.where(hm, lb, hb).reshape(nq, g, LANES)
        cnt = jnp.where(hm, hb, lb).reshape(nq, g, LANES)
        Sc[ct] = jnp.sum(jnp.where(m16, cnt, 0.0), axis=1, keepdims=True)

    def class_sends(i, S, Sc, X1, X1c, k):
        t, qt, ct = class_of(i)
        send(Sc.at[ct], X1c.at[i], sem["s1c"].at[k], sem["r1c"].at[k], to_z(t))
        for d in TREE + (0,):
            qd = lax.rem(qt + d * s + 2 * nq, nq)
            send(S.at[ct, qd], X1.at[i, qd], sem["s1"].at[k], sem["r1"].at[k, qd], to_z(t))

    def far_sums(S, Sc, X1, X1c, T, Tc, XM, XMc, X2, X2c, k):
        wait(X1c, sem["r1c"].at[k])
        for d in TREE + (0,):
            qd = qm(d)
            wait(X1.at[:, 0], sem["r1"].at[k, qd])
            t = S[cl, qd] + X1[0, qd] + X1[1, qd] + X1[2, qd]
            n = Sc[cl, qd] + X1c[0, qd] + X1c[1, qd] + X1c[2, qd]
            for m in {2: (0, 1), -2: (2,)}.get(d, ()):
                wait(XM.at[m], sem["rm"].at[k, m])
                wait(XMc.at[m], sem["rmc"].at[k, m])
                t = t + XM[m]
                n = n + XMc[m]
            T[qd] = t
            Tc[qd] = n
            if d in (4, 3, -3):
                m = (4, 3, -3).index(d)
                to = to_z(zq((2, 1, -1)[m]))
                send(T.at[qd], XM.at[m], sem["s2"].at[k], sem["rm"].at[k, m], to)
                send(Tc.at[qd], XMc.at[m], sem["s2c"].at[k], sem["rmc"].at[k, m], to)
            elif d != 0:
                m = (1, -1, 2, -2).index(d)
                send(T.at[qd], X2.at[m], sem["s2"].at[k], sem["r2"].at[k], to_z(zq(d)))
                send(Tc.at[qd], X2c.at[m], sem["s2c"].at[k], sem["r2c"].at[k], to_z(zq(d)))

    def finish(T, Tc, X2, X2c, C, k):
        wait(X2c, sem["r2c"].at[k])
        cnt = Tc[q] + X2c[0] + X2c[1] + X2c[2] + X2c[3]
        wait(X2, sem["r2"].at[k])
        tot = T[q] + X2[0] + X2[1] + X2[2] + X2[3]
        full = jnp.broadcast_to(cnt, (g, LANES))
        diag = (iota((g, LANES), 1) & (HALF - 1)) == iota((g, LANES), 0)
        lo_n = jnp.sum(jnp.where(diag & jnp.logical_not(hm_g), full, 0.0), axis=1, keepdims=True) + 1.0
        hi_n = jnp.sum(jnp.where(diag & hm_g, full, 0.0), axis=1, keepdims=True) + 1.0
        sl = pl.ds(pl.multiple_of(g * (z // 2), g), g)
        at_lo = 2 * par
        at_hi = 2 * par + 1
        a_lo = C[at_lo, sl, col_a].astype(F32)
        a_hi = C[at_hi, sl, col_a].astype(F32)
        b_lo = C[at_lo, sl, col_b].astype(F32)
        b_hi = pltpu.roll(C[at_hi, sl, col_b].astype(F32), HALF, 1)
        new_lo = ((tot[0:g] + a_lo) / lo_n).astype(BF16)
        new_hi = ((tot[g : 2 * g] + a_hi) / hi_n).astype(BF16)
        new_b = ((tot[2 * g :] + jnp.where(hm_g, b_lo, b_hi)) / jnp.where(hm_g, lo_n, hi_n)).astype(BF16)
        return new_lo, new_hi, new_b

    def cidx(t):
        ct = lax.rem(t, WIN)
        return 2 * lax.rem(ct, 2) + ct // 2

    def far_gather(at, k, near_sends):
        slots = (1, -1, 2, -2, 3, -3, 4)

        def far_send(ref, d, to):
            send(ref, ref, sem["sf"].at[k], sem["rf"].at[k, slots.index(d)], to_z(zq(to)))

        for d in slots[5::-1]:
            far_send(at(q), d, d)
        near_sends(q)
        for d in slots:
            qs = qm(-d)
            wait(at(qs), sem["rf"].at[k, slots.index(d)])
            if d == 2:
                far_send(at(qs), 4, 2)
            near_sends(qs)

    def gather(N):
        ci = 2 * par + e

        def near_sends(qs):
            for i in range(3):
                send(N.at[c, ci, qs], N.at[c, ci, qs], sem["sl"].at[0], sem["rl"].at[0, i], to_z(zed(s * NEAR[i])))

        far_gather(lambda qs: N.at[c, ci, qs], 0, near_sends)
        send(N.at[c, ci], N.at[c, ci], sem["st"].at[0], sem["rt"].at[0], sib)
        for i in (2, 1, 0):
            cs = cidx(zed(-s * NEAR[i]))
            wait(N.at[c, cs], sem["rl"].at[0, i])
            send(N.at[c, cs], N.at[c, cs], sem["st"].at[0], sem["rt"].at[0], sib)

    def gather_rows(O):
        def near_sends(qs):
            at = O.at[2 * qs + e]
            for i, step in enumerate((1, -1, 2 * s)):
                send(at, at, sem["sl"].at[1], sem["rl"].at[1, i], to_z(zed(step)))

        far_gather(lambda qs: O.at[2 * qs + e], 1, near_sends)

    def out_parts(N, t):
        pair = pl.ds(2 * (t // 2), 2)
        rs = pl.ds(pl.multiple_of(g * lax.rem(t, 2), g), g)
        return N.at[c, pair, :, rs, :], N.at[c, pair, :, pl.ds(2 * g, g), :]

    def out_sends(N, OA, OB):
        for i in range(1, nx):
            t = xed(i)
            a, b = out_parts(N, t)
            send(a, OA.at[x], sem["so"].at[0], sem["ro"].at[0], to_x(t))
            send(b, OB.at[x], sem["so"].at[1], sem["ro"].at[1], to_x(t))
        a, b = out_parts(N, x)
        pltpu.make_async_copy(a, OA.at[x], sem["lo"].at[0]).start()
        pltpu.make_async_copy(b, OB.at[x], sem["lo"].at[1]).start()

    left = iota((g, LANES), 1) < HALF

    def out_rows(OA, OB, out):
        wait(OA.at[0], sem["lo"].at[0])
        wait(OB.at[0], sem["lo"].at[1])
        wait(OA.at[pl.ds(0, nx - 1)], sem["ro"].at[0])
        wait(OB.at[pl.ds(0, nx - 1)], sem["ro"].at[1])
        for ee in range(2):
            for qq in range(nq):
                r0 = g * (2 * qq + ee)
                for xx in range(nx):
                    ta = xx + (xx + 1) // 2
                    out[r0 : r0 + g, ta * LANES : (ta + 1) * LANES] = OA[xx, ee, qq]
                for y in range(nx // 2):
                    two = []
                    for xx in (2 * y, 2 * y + 1):
                        b = OB[xx, ee, qq].astype(F32)
                        two.append(jnp.where(h == 1, pltpu.roll(b, HALF, 1), b))
                    tb = 1 + 3 * y
                    out[r0 : r0 + g, tb * LANES : (tb + 1) * LANES] = jnp.where(left, two[0], two[1]).astype(BF16)

    def nearest(C, R):
        def body(k, m):
            ck = C[k]
            cross = lax.dot_general(ck, R[...], (((1,), (1,)), ((), ())), preferred_element_type=F32)
            cf = ck.astype(F32)
            csq = jnp.sum(cf * cf, axis=1, keepdims=True)
            d = csq - 2.0 * cross
            return jnp.minimum(m, jnp.min(d.reshape(rows // 8, 8, chip), axis=0))

        m = lax.fori_loop(0, nx, body, jnp.full((8, chip), jnp.inf, F32))
        r = R[...].astype(F32)
        psq = jnp.sum(jnp.sum(r * r, axis=0, keepdims=True), axis=1, keepdims=True)
        return jnp.min(m, axis=0, keepdims=True), psq

    @pl.loop(0, WIN)
    def _(i):
        class_sums(i, code1, v["W"], v["S1"], v["Sc1"])

    loads[2].wait()
    loads[3].wait()
    loads[4].wait()
    pl.semaphore_wait(barrier, 4 + (nx - 1) + 1)

    def tell(k, step):
        pl.semaphore_signal(sem["lv"].at[k, 0], inc=1, device_id=to_z(zed(-step)), device_id_type=MESH)
        pl.semaphore_signal(sem["lv"].at[k, 1], inc=1, device_id=to_z(zed(step)), device_id_type=MESH)

    def told(k):
        pl.semaphore_wait(sem["lv"].at[k, 0], 1)
        pl.semaphore_wait(sem["lv"].at[k, 1], 1)

    tell(0, 2)

    for i in range(3):
        class_sends(i, v["S1"], v["Sc1"], v["X11"], v["X1c1"], 0)
    def cent_sends(C, k):
        for i in range(1, nx):
            send(C.at[x], C.at[x], sem["sc"].at[k], sem["rc"].at[k], to_x(xed(i)))

    right, left_x = xed(1), xed(nx - 1)
    half = (pl.ds(0, rows // 2), pl.ds(rows // 2, rows // 2))

    def cent_near():
        C = v["C2"]
        send(C.at[x], C.at[x], sem["sc"].at[1], sem["rcn"].at[0], to_x(right))
        send(C.at[x], C.at[x], sem["sc"].at[1], sem["rcn"].at[1], to_x(left_x))

    def cent_pass():
        C = v["C2"]
        for side, (src, to) in enumerate(((left_x, right), (right, left_x))):
            wait(C.at[src], sem["rcn"].at[side])
            send(C.at[src, half[side]], C.at[src, half[side]], sem["scf"], sem["rc"].at[1], to_x(to))

    cent_sends(v["C1"], 0)

    for b in range(npts // LANES):
        row = code1[0:1, b * LANES : (b + 1) * LANES].astype(F32)
        v["CT"][b * LANES : (b + 1) * LANES, :] = jnp.transpose(jnp.broadcast_to(row, (LANES, LANES)))

    told(0)
    tell(1, WIN)
    told(1)
    tell(2, 2 * WIN)
    far_sums(v["S1"], v["Sc1"], v["X11"], v["X1c1"], v["T1"], v["Tc1"], v["XM1"], v["XMc1"], v["X21"], v["X2c1"], 0)
    wait(v["C1"].at[pl.ds(0, nx - 1)], sem["rc"].at[0])
    mins_one, psq_one = nearest(v["C1"], v["R1"])
    v["D0"][c, 0] = mins_one
    new_lo, new_hi, new_b = finish(v["T1"], v["Tc1"], v["X21"], v["X2c1"], v["C1"], 0)
    v["N1"][c, 2 * par + e, q, 0:g, :] = new_lo
    v["N1"][c, 2 * par + e, q, g : 2 * g, :] = new_hi
    v["N1"][c, 2 * par + e, q, 2 * g :, :] = new_b
    told(2)
    gather(v["N1"])
    cent_near()
    wait(v["N1"].at[0], sem["rt"].at[0])

    kb = nq * g
    for cc in range(2):
        for k in range(WIN):
            base = (cc * WIN + k) * 2 * kb
            n = v["N1"][cc, k]
            v["L"][base : base + kb, 0:LANES] = n[:, 0:g, :].reshape(kb, LANES)
            v["L"][base + kb : base + 2 * kb, 0:LANES] = n[:, g : 2 * g, :].reshape(kb, LANES)
            b = n[:, 2 * g :, :].reshape(kb, LANES)
            v["L"][base : base + kb, LANES : 2 * LANES] = b
            v["L"][base + kb : base + 2 * kb, LANES : 2 * LANES] = pltpu.roll(b.astype(F32), HALF, 1).astype(BF16)

    @pl.loop(0, npts // blk)
    def _(i):
        sl = pl.ds(pl.multiple_of(i * blk, blk), blk)
        codes = v["CT"][sl, :]
        parts = []
        lane = iota((1, LANES), 1)
        for j in range(2 * nx * rows // LANES):
            r = lane + j * LANES
            cc = r // (WIN * 2 * kb)
            k = (r // (2 * kb)) & (WIN - 1)
            hl = (r // kb) & 1
            rq = (r // g) & (nq - 1)
            lab = rows * (2 * (2 * (k // 2) + hl) + cc) + g * (2 * rq + (k & 1)) + (r & (g - 1))
            parts.append(jnp.where(codes == lab.astype(F32), 1.0, 0.0).astype(BF16))
        oh = jnp.concatenate(parts, axis=1)
        looked = jnp.dot(oh, v["L"][...], preferred_element_type=F32)
        res = v["P"][sl, :].astype(F32) - looked
        v["W2"][sl, 0:LANES] = res[:, 0:LANES].astype(BF16)
        v["W2"][sl, LANES : 2 * LANES] = jnp.where(hm_b, res[:, LANES:], 1.0).astype(BF16)

    @pl.loop(0, WIN)
    def _(i):
        class_sums(i, code2, v["W2"], v["S2"], v["Sc2"])

        @pl.when(i < 3)
        def _():
            class_sends(i, v["S2"], v["Sc2"], v["X12"], v["X1c2"], 1)

    for i in range(1, nx):
        t = xed(i)
        sl = pl.ds(pl.multiple_of(chip * t, chip), chip)
        send(v["W2"].at[sl, :], v["RR"].at[x], sem["srr"], sem["rrr"], to_x(t))
    sl = pl.ds(pl.multiple_of(chip * x, chip), chip)
    mine = pltpu.make_async_copy(v["W2"].at[sl, :], v["RR"].at[x], sem["ld"].at[5])
    mine.start()
    far_sums(v["S2"], v["Sc2"], v["X12"], v["X1c2"], v["T2"], v["Tc2"], v["XM2"], v["XMc2"], v["X22"], v["X2c2"], 1)
    cent_pass()
    out_sends(v["N1"], v["OA1"], v["OB1"])

    mine.wait()
    wait(v["RR"].at[pl.ds(0, nx - 1)], sem["rrr"])
    for xx in range(nx):
        ta = xx + (xx + 1) // 2
        v["R2"][:, ta * LANES : (ta + 1) * LANES] = v["RR"][xx, :, 0:LANES]
    left_own = iota((chip, LANES), 1) < HALF
    for y in range(nx // 2):
        tb = 1 + 3 * y
        v["R2"][:, tb * LANES : (tb + 1) * LANES] = jnp.where(
            left_own,
            v["RR"][2 * y, :, LANES:].astype(F32),
            v["RR"][2 * y + 1, :, LANES:].astype(F32),
        ).astype(BF16)
    wait(v["C2"].at[0], sem["rc"].at[1])
    mins_two, psq_two = nearest(v["C2"], v["R2"])
    v["D0"][c, 1] = mins_two
    send(v["D0"].at[c], v["D0"].at[c], sem["sd"].at[0], sem["rd"].at[0], sib)
    wait(v["D0"].at[0], sem["rd"].at[0])
    lane = iota((1, LANES), 1)
    tot_one = jnp.sum(jnp.minimum(v["D0"][0, 0], v["D0"][1, 0]), axis=1, keepdims=True) + psq_one
    tot_two = jnp.sum(jnp.minimum(v["D0"][0, 1], v["D0"][1, 1]), axis=1, keepdims=True) + psq_two
    v["D1"][x] = jnp.where(lane == 0, tot_one, jnp.where(lane == 1, tot_two, 0.0))
    for i in range(1, nx):
        send(v["D1"].at[x], v["D1"].at[x], sem["sd"].at[1], sem["rd"].at[1], to_x(xed(i)))

    new_lo, new_hi, new_b = finish(v["T2"], v["Tc2"], v["X22"], v["X2c2"], v["C2"], 1)
    v["NC"][0:g, :] = new_lo
    v["NC"][g : 2 * g, :] = new_b
    v["NC"][2 * g :, :] = new_hi
    role = x // 2 == par
    for hl in range(2):
        t = 2 * par + hl
        src = v["NC"].at[pl.ds(g * hl, 2 * g), :]

        @pl.when(t != x)
        def _():
            send(src, v["Y"].at[x], sem["sy"], sem["ry"], to_x(t))

        @pl.when(t == x)
        def _():
            pltpu.make_async_copy(src, v["Y"].at[x], sem["ly"]).start()

    wait(v["D1"].at[pl.ds(0, nx - 1)], sem["rd"].at[1])
    tot = v["D1"][0]
    for i in range(1, nx):
        tot = tot + v["D1"][i]
    v["D2"][cl, q] = tot
    for o in range(1, nq):
        send(v["D2"].at[cl, q], v["D2"].at[cl, q], sem["sd"].at[2], sem["rd"].at[2], to_z(zed(WIN * o)))

    out_rows(v["OA1"], v["OB1"], v["NW"])
    put_one = pltpu.make_async_copy(v["NW"], new1, sem["ld"].at[6])
    put_one.start()

    def pass_dist():
        wait(v["D2"].at[0, pl.ds(0, nq - 1)], sem["rd"].at[2])
        for i in range(3):
            send(v["D2"].at[cl], v["D2"].at[cl], sem["sd"].at[3], sem["rd"].at[3], to_z(zed(s * NEAR[i])))

    @pl.when(role)
    def _():
        wait(v["Y"].at[pl.ds(0, nx - 1)], sem["ry"])
        wait(v["Y"].at[0], sem["ly"])
        mine = 2 * q + e
        for y in range(nx // 2):
            two = []
            for xx in (2 * y, 2 * y + 1):
                top = v["Y"][xx, 0:g, :].astype(F32)
                low = v["Y"][xx, g : 2 * g, :].astype(F32)
                ta = xx + (xx + 1) // 2
                v["O"][mine, :, ta * LANES : (ta + 1) * LANES] = jnp.where(h == 1, low, top).astype(BF16)
                two.append(jnp.where(h == 1, pltpu.roll(top, HALF, 1), low))
            tb = 1 + 3 * y
            v["O"][mine, :, tb * LANES : (tb + 1) * LANES] = jnp.where(left, two[0], two[1]).astype(BF16)
        gather_rows(v["O"])
        pass_dist()
        wait(v["O"].at[pl.ds(0, nq)], sem["rl"].at[1, 2])

    @pl.when(jnp.logical_not(role))
    def _():
        pass_dist()
        wait(v["O"].at[pl.ds(0, nq)], sem["rl"].at[1, 0])
        wait(v["O"].at[pl.ds(0, nq)], sem["rl"].at[1, 1])

    put_two = pltpu.make_async_copy(v["O"], new2, sem["ld"].at[7])
    put_two.start()

    wait(v["D2"].at[pl.ds(0, 3)], sem["rd"].at[3])
    tot = v["D2"][0, 0]
    for i in range(1, nz):
        tot = tot + v["D2"][i // nq, i % nq]
    dist[...] = tot / jnp.float32(npts * nz * pts.shape[1])

    for k in range(2):
        wait(v["X11"], sem["s1"].at[k])
        wait(v["X1c1"], sem["s1c"].at[k])
        wait(v["X11"].at[0, pl.ds(0, nq - 1)], sem["s2"].at[k])
        wait(v["X1c1"].at[0, pl.ds(0, nq - 1)], sem["s2c"].at[k])
        wait(v["C1"].at[pl.ds(0, nx - 1 - k)], sem["sc"].at[k])
    wait(v["N1"].at[0, 0, pl.ds(0, nq - 1)], sem["sf"].at[0])
    wait(v["N1"].at[0, pl.ds(0, 3)], sem["sl"].at[0])
    wait(v["OA1"].at[pl.ds(0, nx - 1)], sem["so"].at[0])
    wait(v["OB1"].at[pl.ds(0, nx - 1)], sem["so"].at[1])
    wait(v["N1"].at[0], sem["st"].at[0])
    wait(v["RR"].at[pl.ds(0, nx - 1)], sem["srr"])
    wait(v["D0"].at[0], sem["sd"].at[0])
    wait(v["D1"].at[pl.ds(0, nx - 1)], sem["sd"].at[1])
    wait(v["D2"].at[0, pl.ds(0, nq - 1)], sem["sd"].at[2])
    wait(v["D2"].at[pl.ds(0, 3)], sem["sd"].at[3])

    @pl.when(role)
    def _():
        wait(v["O"].at[pl.ds(0, nq - 1)], sem["sf"].at[1])
        wait(v["X11"], sem["sl"].at[1])
        wait(v["Y"].at[0], sem["sy"])

    @pl.when(jnp.logical_not(role))
    def _():
        wait(v["Y"].at[pl.ds(0, 2)], sem["sy"])

    wait(v["C1"].at[0], sem["scf"])
    put_one.wait()
    put_two.wait()


def solution(mesh):
    nz = mesh.shape["pts"]
    nx = mesh.shape["cb"] // 2
    nq = nz // WIN

    def local(points, code_one, code_two, cent_one, cent_two):
        npts, width = points.shape
        rows = cent_one.shape[0]
        chip = npts // nx
        g = 2 * rows // nz
        ch = 3 * g
        vm = pltpu.VMEM
        v = {
            "P": vm((npts, 2 * LANES), BF16),
            "W": vm((npts, 2 * LANES), BF16),
            "W2": vm((npts, 2 * LANES), BF16),
            "CT": vm((npts, LANES), F32),
            "L": vm((2 * nx * rows, 2 * LANES), BF16),
            "R1": vm((chip, width), BF16),
            "R2": vm((chip, width), BF16),
            "RR": vm((nx, chip, 2 * LANES), BF16),
            "D0": vm((2, 2, 1, chip), F32),
            "D1": vm((nx, 1, LANES), F32),
            "D2": vm((WIN, nq, 1, LANES), F32),
        }
        v["N1"] = vm((2, WIN, nq, ch, LANES), BF16)
        v["OA1"] = vm((nx, 2, nq, g, LANES), BF16)
        v["OB1"] = vm((nx, 2, nq, g, LANES), BF16)
        v["NW"] = vm((rows, width), BF16)
        v["NC"] = vm((ch, LANES), BF16)
        v["Y"] = vm((nx, 2 * g, LANES), BF16)
        v["O"] = vm((2 * nq, g, width), BF16)
        for k in ("1", "2"):
            v["C" + k] = vm((nx, rows, width), BF16)
            v["S" + k] = vm((WIN, nq, ch, LANES), F32)
            v["Sc" + k] = vm((WIN, nq, 1, LANES), F32)
            v["X1" + k] = vm((3, nq, ch, LANES), F32)
            v["X1c" + k] = vm((3, nq, 1, LANES), F32)
            v["T" + k] = vm((nq, ch, LANES), F32)
            v["Tc" + k] = vm((nq, 1, LANES), F32)
            v["XM" + k] = vm((3, ch, LANES), F32)
            v["X2" + k] = vm((4, ch, LANES), F32)
            v["X2c" + k] = vm((4, 1, LANES), F32)
            v["XMc" + k] = vm((3, 1, LANES), F32)
        dma = pltpu.SemaphoreType.DMA
        sem = {
            "ld": dma((8,)),
            "s1": dma((2,)), "r1": dma((2, nq)), "s1c": dma((2,)), "r1c": dma((2,)),
            "rm": dma((2, 3)), "rmc": dma((2, 3)), "lv": pltpu.SemaphoreType.REGULAR((3, 2)), "s2": dma((2,)), "r2": dma((2,)), "s2c": dma((2,)), "r2c": dma((2,)),
            "sf": dma((2,)), "rf": dma((2, nq - 1)), "sl": dma((2,)), "rl": dma((2, 3)),
            "st": dma((1,)), "rt": dma((1,)),
            "so": dma((2,)), "ro": dma((2,)), "lo": dma((2,)),
            "sy": dma(()), "ry": dma(()), "ly": dma(()),
            "sc": dma((2,)), "rcn": dma((2,)), "scf": dma(()), "rc": dma((2,)),
            "srr": dma(()), "rrr": dma(()),
            "sd": dma((4,)), "rd": dma((4,)),
        }
        hbm = pl.BlockSpec(memory_space=pl.ANY)
        vmem = pl.BlockSpec(memory_space=pltpu.VMEM)
        far = pl.BlockSpec(memory_space=pltpu.HBM)
        new_one, new_two, dist = pl.pallas_call(
            functools.partial(kernel, nz, nx),
            out_shape=(
                jax.ShapeDtypeStruct((rows, width), BF16),
                jax.ShapeDtypeStruct((2 * nq, g, width), BF16),
                jax.ShapeDtypeStruct((1, LANES), F32),
            ),
            in_specs=[far, vmem, vmem, far, far],
            out_specs=(hbm, hbm, vmem),
            scratch_shapes=[v, sem],
            compiler_params=pltpu.CompilerParams(
                collective_id=0, has_side_effects=True, vmem_limit_bytes=53 * 1024 * 1024
            ),
        )(points, code_one.reshape(1, npts), code_two.reshape(1, npts), cent_one, cent_two)
        return new_one, new_two.reshape(rows, width), dist[0, :2]

    cents = P(("groups", "cb"), None)
    return jax.shard_map(
        local,
        mesh=mesh,
        in_specs=(P(("groups", "pts"), None), P(("groups", "pts")), P(("groups", "pts")), cents, cents),
        out_specs=(cents, cents, P("groups")),
        check_vma=False,
    )
```
